1024 devices in a mesh: gx: 8 (over z_hi, core), gy: 4 (over x), gz: 32 (over z_lo, y).
Axes of the slice: x: 4, y: 4, z: 32 (z_hi: 4, z_lo: 8; z = z_hi * 8 + z_lo), core: 2. Of those that a mesh axis runs over, the one named last changes fastest.
Arguments:
- euler_state: float32 [5, 32, 32, 4096], P(None, 'gx', 'gy', 'gz'), as said below
- gravity_state: float32 [4, 32, 32, 4096], P(None, 'gx', 'gy', 'gz'), may hold values from -6 to 6
Outputs:
- section_rate: float32 [5, 32, 32, 4096], P(None, 'gx', 'gy', 'gz')
- gravity_next: float32 [4, 32, 32, 4096], P(None, 'gx', 'gy', 'gz')
- gravity_source: float32 [4, 32, 32, 4096], P(None, 'gx', 'gy', 'gz')
- residual_norm: float32 [], replicated
The draws below stay inside these ranges and needn't reach their ends.
Inputs may be any that keep to these rules, and one draw needn't show every extreme that they name: `euler_state`: each node's density lies between 0.7 and 3.9 and its pressure, for a ratio of specific heats of 1.4, between 0.7 and 71.
All inputs are finite; a program needn't handle non-finite values.
Results may differ from the reference program's by a relative error of at most 0.0003.
Values sent between devices are 32-bit elements; how exact they have to be, the bound alone decides.
No kernel may reach another device: no remote copies, remote signals or barrier semaphores. Data moves between devices by JAX's collectives and lax.ppermute only.
A program may use at most 32 MiB of HBM per device.

```python
import math
import jax
import jax.numpy as jnp
import numpy as np
from jax import lax

GRAV_VARS = 4
ITERS = 3
NXN = 32
NYN = 32
NZN = 4096


def draw_euler_state(key, part):
    subkeys = jax.random.split(jax.random.fold_in(key, 17), 5)
    grid_shape = (NXN, NYN, NZN)
    block_shape = (NXN // 4, NYN // 4, NZN // 4)
    log_rough = jax.random.uniform(subkeys[0], block_shape, jnp.float32, math.log(0.001), math.log(0.3))
    roughness = jnp.exp(log_rough)
    roughness = jnp.repeat(jnp.repeat(jnp.repeat(roughness, 4, axis=0), 4, axis=1), 4, axis=2)
    height = lax.broadcasted_iota(jnp.int32, grid_shape, 2).astype(jnp.float32) / NZN
    across = lax.broadcasted_iota(jnp.int32, grid_shape, 0).astype(jnp.float32) / NXN
    wiggle_rho = jax.random.uniform(subkeys[1], grid_shape, jnp.float32, -1.0, 1.0)
    wiggle_pres = jax.random.uniform(subkeys[2], grid_shape, jnp.float32, -1.0, 1.0)
    base_rho = 1.0 + height + across
    velocity = 0.3 * jax.random.uniform(subkeys[3], (3,) + grid_shape, jnp.float32, -1.0, 1.0)
    hot_block = jax.random.randint(subkeys[4], (3,), 0, jnp.array(block_shape, dtype=jnp.int32))
    block_x = lax.broadcasted_iota(jnp.int32, grid_shape, 0) // 4
    block_y = lax.broadcasted_iota(jnp.int32, grid_shape, 1) // 4
    block_z = lax.broadcasted_iota(jnp.int32, grid_shape, 2) // 4
    is_hot = (block_x == hot_block[0]) & (block_y == hot_block[1]) & (block_z == hot_block[2])
    density = base_rho * (1.0 + roughness * wiggle_rho)
    pressure = (1.0 + 8.0 * height) * (1.0 + roughness * wiggle_pres) * jnp.where(is_hot, 6.0, 1.0)
    energy = pressure / 0.4 + 0.5 * density * jnp.sum(velocity * velocity, axis=0)
    return jnp.concatenate([density[None], density[None] * velocity, energy[None]], axis=0)


def levels(own_key, extent, shards, smallest, top_value):
    loudness, own = 1.0, jax.random.fold_in(own_key, 6)
    for axis_at, blocks in shards:
        draws = jnp.exp(jax.random.uniform(jax.random.fold_in(own, axis_at), (blocks,), jnp.float32, smallest / len(shards), top_value / len(shards)))
        loudness = loudness * jnp.repeat(draws, extent[axis_at] // blocks).reshape([-1 if axis == axis_at else 1 for axis in range(len(extent))])
    return loudness


def gaussian(stream_key, extent, width, most, shards=(), held_as=jnp.bfloat16):
    level = levels(stream_key, extent, shards, -0.22, 0.18) if shards else 1.0
    result = jax.random.normal(stream_key, extent, jnp.float32) * width * level
    return jnp.minimum(jnp.maximum(result, -most), most).astype(held_as)


def setup_inputs(seed: int = 0) -> dict:
    splits = jax.random.split(jax.random.key(seed), 3)
    return {
        "euler_state": draw_euler_state(jax.random.fold_in(splits[2], 71), 0),
        "gravity_state": gaussian(splits[1], (GRAV_VARS, NXN, NYN, NZN), 1.0, 6.0, ((1, 8), (2, 4), (3, 32)), jnp.float32),
    }


gamma_gas = 1.4
elem_width = 1.0
cfl_euler = 0.5
alpha_most = 0.5
indicator_level = 0.5 * 10.0 ** (-1.8 * 4.0 ** 0.25)
indicator_slope = math.log((1.0 - 0.0001) / 0.0001) / indicator_level
coupling = 10.0
relax_time = 1.0
grav_speed = 1.0
pseudo_step = 0.3 * elem_width / 7.0

def lgl_tables():
    points = np.array([-1.0, -1.0 / math.sqrt(5.0), 1.0 / math.sqrt(5.0), 1.0])
    weights = np.array([1.0, 5.0, 5.0, 1.0]) / 6.0
    barycentric = np.array([1.0 / np.prod([points[node_a] - points[node_b] for node_b in range(4) if node_b != node_a]) for node_a in range(4)])
    derivative = np.zeros((4, 4))
    for node_a in range(4):
        for node_b in range(4):
            if node_b != node_a:
                derivative[node_a, node_b] = barycentric[node_b] / barycentric[node_a] / (points[node_a] - points[node_b])
        derivative[node_a, node_a] = -np.sum(derivative[node_a])
    legendre = np.stack([np.ones(4), points, 0.5 * (3.0 * points ** 2 - 1.0), 0.5 * (5.0 * points ** 3 - 3.0 * points)], axis=1)
    legendre = legendre * np.sqrt((2.0 * np.arange(4) + 1.0) / 2.0)
    gram = np.sum(weights[:, None] * legendre * legendre, axis=0)
    modal_map = (legendre * weights[:, None]).T / gram[:, None]
    return (weights, derivative, modal_map)

def diagonal_of(derivative):
    return [derivative[node_at, node_at] for node_at in range(4)]

def along(values, length, axis_pos, array_rank):
    shape_list = [1] * array_rank
    shape_list[axis_pos] = length
    return jnp.asarray(np.tile(np.asarray([float(item) for item in values]), length // 4).reshape(shape_list))

def log_mean(left, right):
    ratio_sq = ((left - right) / (left + right)) ** 2
    is_close = ratio_sq < 0.0001
    series = (left + right) / (2.0 + ratio_sq * (2.0 / 3.0 + ratio_sq * (2.0 / 5.0 + ratio_sq * 2.0 / 7.0)))
    top_part = jnp.where(is_close, 1.0, right - left)
    low_part = jnp.where(is_close, 1.0, jnp.log(right / left))
    return jnp.where(is_close, series, top_part / low_part)

def describe(conserved, direction):
    density = conserved[0]
    velocity = conserved[1:4] / density
    pressure = (gamma_gas - 1.0) * (conserved[4] - 0.5 * lax.optimization_barrier(jnp.sum(conserved[1:4] * velocity, axis=0)))
    normal_vel = velocity[direction]
    momentum_flux = [conserved[1 + comp] * normal_vel + (pressure if comp == direction else 0.0) for comp in range(3)]
    energy_flux = (conserved[4] + pressure) * normal_vel
    sound = jnp.sqrt(gamma_gas * pressure / density)
    return jnp.stack([conserved[0], conserved[1], conserved[2], conserved[3], conserved[4], velocity[0], velocity[1], velocity[2], pressure, conserved[1 + direction]] + momentum_flux + [energy_flux, jnp.abs(normal_vel) + sound])

def euler_interface(left, right):
    speed = jnp.maximum(left[14], right[14])
    return 0.5 * (left[9:14] + right[9:14]) - 0.5 * speed * (right[0:5] - left[0:5])

def two_point(left, right, direction):
    rho_mean = log_mean(left[0], right[0])
    inv_mean = left[8] * right[8] / log_mean(left[0] * right[8], right[0] * left[8])
    vel_avg = 0.5 * (left[5:8] + right[5:8])
    pres_avg = 0.5 * (left[8] + right[8])
    vel_product = 0.5 * lax.optimization_barrier(jnp.sum(left[5:8] * right[5:8], axis=0))
    mass_flux = rho_mean * vel_avg[direction]
    momentum = [mass_flux * vel_avg[comp] + (pres_avg if comp == direction else 0.0) for comp in range(3)]
    energy = mass_flux * (vel_product + inv_mean / (gamma_gas - 1.0)) + 0.5 * (left[8] * right[5 + direction] + right[8] * left[5 + direction])
    return jnp.stack([mass_flux] + momentum + [energy])

def euler_direction(described, low_desc, high_desc, direction):
    weights, derivative, modal_map = lgl_tables()
    axis_pos = direction + 1
    length = described.shape[axis_pos]
    array_rank = described.ndim
    prev_desc = jnp.concatenate([low_desc, lax.slice_in_dim(described, 0, length - 1, axis=axis_pos)], axis=axis_pos)
    face_flux = euler_interface(prev_desc, described)
    last_face = euler_interface(lax.slice_in_dim(described, length - 1, length, axis=axis_pos), high_desc)
    next_faces = jnp.concatenate([lax.slice_in_dim(face_flux, 1, length, axis=axis_pos), last_face], axis=axis_pos)
    own_flux = described[9:14]
    volume = along([2.0 * item for item in diagonal_of(derivative)], length, axis_pos, array_rank) * own_flux
    for offset in range(1, 4):
        partner = jnp.roll(described, -offset, axis=axis_pos)
        pair_flux = two_point(described, partner, direction)
        upward = [2.0 * derivative[node_at, node_at + offset] if node_at + offset < 4 else 0.0 for node_at in range(4)]
        downward = [2.0 * derivative[node_at, node_at - offset] if node_at - offset >= 0 else 0.0 for node_at in range(4)]
        volume = volume + along(upward, length, axis_pos, array_rank) * pair_flux + along(downward, length, axis_pos, array_rank) * jnp.roll(pair_flux, offset, axis=axis_pos)
    first_coef = along([-1.0 / weights[0], 0.0, 0.0, 0.0], length, axis_pos, array_rank)
    last_coef = along([0.0, 0.0, 0.0, 1.0 / weights[3]], length, axis_pos, array_rank)
    dg_part = volume + first_coef * (face_flux - own_flux) + last_coef * (next_faces - own_flux)
    fv_part = along(1.0 / weights, length, axis_pos, array_rank) * (next_faces - face_flux)
    return (dg_part, fv_part)

def section_rate_from(euler_state, gravity_state, low_states, high_states, alpha):
    dg_total = 0.0
    fv_total = 0.0
    speed_total = 0.0
    for direction in range(3):
        described = describe(euler_state, direction)
        dg_part, fv_part = euler_direction(described, describe(low_states[direction], direction), describe(high_states[direction], direction), direction)
        dg_total = dg_total + dg_part
        fv_total = fv_total + fv_part
        speed_total = speed_total + described[14]
    grav_grad = gravity_state[1:4]
    source = jnp.concatenate([jnp.zeros_like(euler_state[0:1]), -euler_state[0:1] * grav_grad, -lax.optimization_barrier(jnp.sum(euler_state[1:4] * grav_grad, axis=0, keepdims=True))], axis=0)
    rate = -(2.0 / elem_width) * ((1.0 - alpha) * dg_total + alpha * fv_total) + source
    return (rate, speed_total)

def gravity_flux(gravity, direction):
    zero_field = jnp.zeros_like(gravity[0])
    parts = [-gravity[1 + direction]]
    for comp in range(3):
        parts.append(-gravity[0] / relax_time if comp == direction else zero_field)
    return jnp.stack(parts)

def gravity_interface(left, right, direction):
    return 0.5 * (gravity_flux(left, direction) + gravity_flux(right, direction)) - 0.5 * grav_speed * (right - left)

def gravity_direction(gravity, first_face, end_face, direction):
    weights, derivative, modal_map = lgl_tables()
    axis_pos = direction + 1
    length = gravity.shape[axis_pos]
    array_rank = gravity.ndim
    own_flux = gravity_flux(gravity, direction)
    inner = gravity_interface(jnp.roll(gravity, 1, axis=axis_pos), gravity, direction)
    face_flux = jnp.concatenate([first_face, lax.slice_in_dim(inner, 1, length, axis=axis_pos)], axis=axis_pos)
    next_faces = jnp.concatenate([lax.slice_in_dim(face_flux, 1, length, axis=axis_pos), end_face], axis=axis_pos)
    volume = along(diagonal_of(derivative), length, axis_pos, array_rank) * own_flux
    for offset in range(1, 4):
        upward = [derivative[node_at, node_at + offset] if node_at + offset < 4 else 0.0 for node_at in range(4)]
        downward = [derivative[node_at, node_at - offset] if node_at - offset >= 0 else 0.0 for node_at in range(4)]
        volume = volume + along(upward, length, axis_pos, array_rank) * jnp.roll(own_flux, -offset, axis=axis_pos) + along(downward, length, axis_pos, array_rank) * jnp.roll(own_flux, offset, axis=axis_pos)
    first_coef = along([-1.0 / weights[0], 0.0, 0.0, 0.0], length, axis_pos, array_rank)
    last_coef = along([0.0, 0.0, 0.0, 1.0 / weights[3]], length, axis_pos, array_rank)
    return volume + first_coef * (face_flux - own_flux) + last_coef * (next_faces - own_flux)

def gravity_rate(gravity, first_faces, end_faces, density, density_mean):
    total = 0.0
    for direction in range(3):
        total = total + gravity_direction(gravity, first_faces[direction], end_faces[direction], direction)
    rate = -(2.0 / elem_width) * total
    rate_phi = rate[0:1] - coupling * (density[None] - density_mean)
    rate_grad = rate[1:4] - gravity[1:4] / relax_time
    return jnp.concatenate([rate_phi, rate_grad], axis=0)

def node_weights(grid_shape):
    weights, derivative, modal_map = lgl_tables()
    return along(weights, grid_shape[0], 0, 3) * along(weights, grid_shape[1], 1, 3) * along(weights, grid_shape[2], 2, 3)

def element_alpha(euler_state):
    weights, derivative, modal_map = lgl_tables()
    density = euler_state[0]
    velocity = euler_state[1:4] / density
    pressure = (gamma_gas - 1.0) * (euler_state[4] - 0.5 * lax.optimization_barrier(jnp.sum(euler_state[1:4] * velocity, axis=0)))
    product = density * pressure
    size_x, size_y, size_z = product.shape
    blocks = product.reshape(size_x // 4, 4, size_y // 4, 4, size_z // 4, 4)
    modal_arr = jnp.asarray(modal_map)
    coeffs = jnp.einsum('ai,bj,ck,xiyjzk->xaybzc', modal_arr, modal_arr, modal_arr, blocks, precision=lax.Precision.HIGHEST)
    energy = coeffs * coeffs
    low_index = np.array([1.0, 1.0, 1.0, 0.0])
    low_mask = jnp.asarray(low_index.reshape(1, 4, 1, 1, 1, 1) * low_index.reshape(1, 1, 1, 4, 1, 1) * low_index.reshape(1, 1, 1, 1, 1, 4))
    total = lax.optimization_barrier(jnp.sum(energy, axis=(1, 3, 5)))
    high_energy = lax.optimization_barrier(jnp.sum(energy * (1.0 - low_mask), axis=(1, 3, 5)))
    high_share = high_energy / total
    alpha = alpha_most / (1.0 + jnp.exp(-indicator_slope * (high_share - indicator_level)))
    return jnp.repeat(jnp.repeat(jnp.repeat(alpha, 4, axis=0), 4, axis=1), 4, axis=2)

def reference(euler_state, gravity_state):
    low_states = []
    high_states = []
    for direction in range(3):
        length = euler_state.shape[direction + 1]
        low_states.append(lax.slice_in_dim(euler_state, length - 1, length, axis=direction + 1))
        high_states.append(lax.slice_in_dim(euler_state, 0, 1, axis=direction + 1))
    alpha = element_alpha(euler_state)
    rate, speed_total = section_rate_from(euler_state, gravity_state, low_states, high_states, alpha)
    time_step = cfl_euler * elem_width / (7.0 * jnp.max(speed_total))
    state_next = euler_state + time_step * rate
    grid_shape = euler_state.shape[1:]
    weight_grid = node_weights(grid_shape)
    weight_total = 8.0 * (grid_shape[0] // 4) * (grid_shape[1] // 4) * (grid_shape[2] // 4)
    density_mean = jnp.sum(weight_grid * state_next[0]) / weight_total
    gravity = gravity_state
    rate_grav = jnp.zeros_like(gravity_state)
    for iteration in range(ITERS):
        first_faces = []
        end_faces = []
        for direction in range(3):
            length = gravity.shape[direction + 1]
            first_plane = lax.slice_in_dim(gravity, 0, 1, axis=direction + 1)
            last_plane = lax.slice_in_dim(gravity, length - 1, length, axis=direction + 1)
            first_faces.append(gravity_interface(last_plane, first_plane, direction))
            end_faces.append(gravity_interface(last_plane, first_plane, direction))
        rate_grav = gravity_rate(gravity, first_faces, end_faces, state_next[0], density_mean)
        gravity = gravity + pseudo_step * rate_grav
    residual_norm = jnp.sqrt(jnp.sum(weight_grid * rate_grav[0] * rate_grav[0]) / weight_total)
    grav_grad = gravity[1:4]
    gravity_source = jnp.concatenate([-state_next[0:1] * grav_grad, -lax.optimization_barrier(jnp.sum(state_next[1:4] * grav_grad, axis=0, keepdims=True))], axis=0)
    return (rate, gravity, gravity_source, residual_norm)
```

```python
import functools
import math

import jax
import jax.numpy as jnp
import numpy as np
from jax import lax
from jax.experimental import pallas as pl
from jax.experimental.pallas import tpu as pltpu
from jax.sharding import Mesh
from jax.sharding import PartitionSpec as P

ITERS = 3
GX = ("gx_0", "gx_1")
GZ = ("gz_0", "gz_1")

gamma_gas = 1.4
elem_width = 1.0
cfl_euler = 0.5
alpha_most = 0.5
indicator_level = 0.5 * 10.0 ** (-1.8 * 4.0**0.25)
indicator_slope = math.log((1.0 - 0.0001) / 0.0001) / indicator_level
coupling = 10.0
pseudo_step = 0.3 * elem_width / 7.0
rho_offset = 2.3

NX, NY, NZ = (4, 8, 128)
F32 = jnp.float32


def lgl_tables():
    points = np.array([-1.0, -1.0 / math.sqrt(5.0), 1.0 / math.sqrt(5.0), 1.0])
    weights = np.array([1.0, 5.0, 5.0, 1.0]) / 6.0
    barycentric = np.array(
        [1.0 / np.prod([points[a] - points[b] for b in range(4) if b != a]) for a in range(4)]
    )
    derivative = np.zeros((4, 4))
    for a in range(4):
        for b in range(4):
            if b != a:
                derivative[a, b] = barycentric[b] / barycentric[a] / (points[a] - points[b])
        derivative[a, a] = -np.sum(derivative[a])
    legendre = np.stack(
        [np.ones(4), points, 0.5 * (3.0 * points**2 - 1.0), 0.5 * (5.0 * points**3 - 3.0 * points)],
        axis=1,
    )
    legendre = legendre * np.sqrt((2.0 * np.arange(4) + 1.0) / 2.0)
    gram = np.sum(weights[:, None] * legendre * legendre, axis=0)
    modal_map = (legendre * weights[:, None]).T / gram[:, None]
    return (weights, derivative, modal_map)


WEIGHTS, DERIV, MODAL = lgl_tables()


class Line:
    def __init__(self, dim):
        self.dim = dim
        self.length = (NY, NZ)[dim]
        self.at = lax.broadcasted_iota(jnp.int32, (NY, NZ), dim)
        self.node = self.at % 4
        self.lowest = self.at == 0
        self.highest = self.at == self.length - 1
        self.is0 = self.node == 0
        self.is3 = self.node == 3

    def by_node(self, values):
        v = [float(item) for item in values]
        if v[1] == v[2] and v[0] == v[3]:
            return jnp.where(self.is0 | self.is3, v[0], v[1]).astype(F32)
        return jnp.where(
            self.node < 2,
            jnp.where(self.is0, v[0], v[1]),
            jnp.where(self.is3, v[3], v[2]),
        ).astype(F32)

    def roll(self, value, by):
        return pltpu.roll(value, by % self.length, self.dim)

    def cyc(self, value, k):
        return jnp.where(self.node < 4 - k, self.roll(value, -k), self.roll(value, 4 - k))

    def coef(self, matrix, k, scale=1.0):
        return self.by_node([scale * matrix[i, (i + k) % 4] for i in range(4)])

    def element_sum(self, value):
        value = value + self.cyc(value, 2)
        return value + self.cyc(value, 1)


def quad(at):
    return [at[x] for x in range(NX)]


def load(ref):
    return [[ref[c, x] for x in range(NX)] for c in range(ref.shape[0])]


def pack(comps, outs):
    xf, xl, yf, yl, zf, zl = outs
    lane = lax.broadcasted_iota(jnp.int32, (NY, NZ), 1)
    first = jnp.zeros((NY, NZ), F32)
    last = jnp.zeros((NY, NZ), F32)
    for c, comp in enumerate(comps):
        xf[c] = comp[0]
        xl[c] = comp[NX - 1]
        for x in range(NX):
            yf[c, pl.ds(x, 1), :] = comp[x][0:1, :]
            yl[c, pl.ds(x, 1), :] = comp[x][NY - 1 : NY, :]
            k = c * NX + x
            here = lane == k
            first = jnp.where(here, pltpu.roll(comp[x], k, 1) if k else comp[x], first)
            last = jnp.where(here, pltpu.roll(comp[x], k + 1, 1), last)
    zf[...] = first
    zl[...] = last


class Halo:
    def __init__(self, refs):
        self.xlo, self.xhi, self.ylo, self.yhi = refs[:4]
        self.zlo, self.zhi = (refs[4][...], refs[5][...])

    def low(self, dim, c, x):
        if dim == 0:
            return jnp.broadcast_to(self.ylo[c, pl.ds(x, 1), :], (NY, NZ))
        k = c * NX + x
        return pltpu.roll(self.zlo, (NZ - k) % NZ, 1) if k else self.zlo

    def high(self, dim, c, x):
        if dim == 0:
            return jnp.broadcast_to(self.yhi[c, pl.ds(x, 1), :], (NY, NZ))
        k = c * NX + x
        return pltpu.roll(self.zhi, NZ - 1 - k, 1)


def message_shapes(n):
    return [
        jax.ShapeDtypeStruct((n, NY, NZ), F32),
        jax.ShapeDtypeStruct((n, NY, NZ), F32),
        jax.ShapeDtypeStruct((n, NX, NZ), F32),
        jax.ShapeDtypeStruct((n, NX, NZ), F32),
        jax.ShapeDtypeStruct((NY, NZ), F32),
        jax.ShapeDtypeStruct((NY, NZ), F32),
    ]


def log_mean(left, right):
    total = left + right
    gap = right - left
    slope = gap / total
    ratio_sq = slope * slope
    is_close = ratio_sq < 0.0001
    series = 2.0 + ratio_sq * (2.0 / 3.0 + ratio_sq * (2.0 / 5.0 + ratio_sq * (2.0 / 7.0)))
    top = jnp.where(is_close, total, gap)
    low = jnp.where(is_close, series, jnp.log(right / left))
    return top / low


def two_point(left, right, d):
    rho_mean = log_mean(left[0], right[0])
    inv_mean = left[4] * right[4] / log_mean(left[0] * right[4], right[0] * left[4])
    vel = [0.5 * (left[1 + i] + right[1 + i]) for i in range(3)]
    product = left[1] * right[1] + left[2] * right[2] + left[3] * right[3]
    mass = rho_mean * vel[d]
    flux = [mass] + [mass * vel[i] for i in range(3)]
    flux[1 + d] = flux[1 + d] + 0.5 * (left[4] + right[4])
    energy = mass * (0.5 * product + inv_mean * (1.0 / (gamma_gas - 1.0))) + 0.5 * (
        left[4] * right[1 + d] + right[4] * left[1 + d]
    )
    return flux + [energy]


def primitive(u):
    inv = 1.0 / u[0]
    vel = [u[1 + i] * inv for i in range(3)]
    kinetic = u[1] * vel[0] + u[2] * vel[1] + u[3] * vel[2]
    pressure = (gamma_gas - 1.0) * (u[4] - 0.5 * kinetic)
    return (vel, pressure, jnp.sqrt(gamma_gas * pressure * inv))


def face_data(u, d, known=None):
    vel, pressure, sound = known or primitive(u)
    normal = vel[d]
    flux = [u[1 + d]] + [u[1 + i] * normal for i in range(3)] + [(u[4] + pressure) * normal]
    flux[1 + d] = flux[1 + d] + pressure
    return (u, flux, jnp.abs(normal) + sound)


def interface(left, right):
    speed = jnp.maximum(left[2], right[2])
    return [
        0.5 * ((left[1][c] + right[1][c]) - speed * (right[0][c] - left[0][c])) for c in range(5)
    ]


def volume_kernel(u_ref, vol_ref, alpha_ref, fast_ref):
    y, z = (Line(0), Line(1))
    u = load(u_ref)
    known = [primitive([u[c][x] for c in range(5)]) for x in range(NX)]
    nodes = [[u[0][x]] + known[x][0] + [known[x][1]] for x in range(NX)]
    speed = [
        jnp.abs(known[x][0][0]) + jnp.abs(known[x][0][1]) + jnp.abs(known[x][0][2]) + 3.0 * known[x][2]
        for x in range(NX)
    ]
    fast_ref[...] = jnp.maximum(jnp.maximum(speed[0], speed[1]), jnp.maximum(speed[2], speed[3]))

    product = [u[0][x] * known[x][1] for x in range(NX)]
    coeffs = [sum(float(MODAL[a, i]) * product[i] for i in range(4)) for a in range(4)]
    for line in (y, z):
        modal = [line.coef(MODAL, k) for k in range(4)]
        coeffs = [
            modal[0] * value + sum(modal[k] * line.cyc(value, k) for k in range(1, 4))
            for value in coeffs
        ]
    energy = [value * value for value in coeffs]
    total = (energy[0] + energy[1]) + (energy[2] + energy[3])
    low = (energy[0] + energy[1]) + energy[2]
    high = energy[3] + jnp.where(y.is3 | z.is3, low, 0.0)
    share = z.element_sum(y.element_sum(high)) / z.element_sum(y.element_sum(total))
    alpha = alpha_most / (1.0 + jnp.exp(-indicator_slope * (share - indicator_level)))
    alpha_ref[...] = alpha

    volume = [[None] * NX for _ in range(5)]
    for i in range(NX):
        for j in range(i + 1, NX):
            flux = two_point(nodes[i], nodes[j], 0)
            for c in range(5):
                for at, other in ((i, j), (j, i)):
                    term = (2.0 * DERIV[at, other]).astype(np.float32) * flux[c]
                    volume[c][at] = term if volume[c][at] is None else volume[c][at] + term
    for d, line in ((1, y), (2, z)):
        up, across, down = [line.coef(DERIV, k, 2.0) for k in (1, 2, 3)]
        for x in range(NX):
            near = two_point(nodes[x], [line.cyc(a, 1) for a in nodes[x]], d)
            far = two_point(nodes[x], [line.cyc(a, 2) for a in nodes[x]], d)
            for c in range(5):
                volume[c][x] = volume[c][x] + (
                    up * near[c] + down * line.cyc(near[c], 3) + across * far[c]
                )
    keep = 1.0 - alpha
    for c in range(5):
        for x in range(NX):
            vol_ref[c, x] = keep * volume[c][x]


def gravity_parts(field, halo, base, y, z):
    total = [[0.0] * NX for _ in range(4)]
    have = [c for c in range(4) if field[c] is not None]
    where = {c: base + i for i, c in enumerate(have)}

    def diff(c, x):
        return field[c][x]

    for c, partner in ((0, 1), (1, 0)):
        if field[partner] is not None:
            for i in range(NX):
                terms = [float(2.0 * DERIV[i, j]) * field[partner][j] for j in range(NX) if DERIV[i, j] != 0.0]
                total[c][i] = total[c][i] + sum(terms[1:], terms[0])
    jumps = {}
    for c in have:
        jumps[c] = (halo.xlo[where[c]] - field[c][0], halo.xhi[where[c]] - field[c][NX - 1])
        for side, x in ((0, 0), (1, NX - 1)):
            total[c][x] = total[c][x] + 6.0 * jumps[c][side]
    for c, partner in ((0, 1), (1, 0)):
        if partner in jumps:
            total[c][0] = total[c][0] - 6.0 * jumps[partner][0]
            total[c][NX - 1] = total[c][NX - 1] + 6.0 * jumps[partner][1]
    for d, line in ((1, y), (2, z)):
        comp = 1 + d
        diag = line.coef(DERIV, 0, 2.0)
        coefs = [line.coef(DERIV, k, 2.0) for k in range(1, 4)]
        sign = line.by_node([-6.0, 0.0, 0.0, 6.0])
        for x in range(NX):
            for c, partner in ((0, comp), (comp, 0)):
                if field[partner] is not None:
                    value = field[partner][x]
                    term = diag * value
                    for k in range(1, 4):
                        term = term + coefs[k - 1] * line.cyc(value, k)
                    total[c][x] = total[c][x] + term
            gaps = {}
            for c in have:
                value = field[c][x]
                prev = jnp.where(line.lowest, halo.low(line.dim, where[c], x), line.roll(value, 1))
                after = jnp.where(line.highest, halo.high(line.dim, where[c], x), line.roll(value, -1))
                beside = jnp.where(line.is0, prev, jnp.where(line.is3, after, value))
                gaps[c] = beside - value
                total[c][x] = total[c][x] + 6.0 * gaps[c]
            for c, partner in ((0, comp), (comp, 0)):
                if partner in gaps:
                    total[c][x] = total[c][x] + sign * gaps[partner]
    return total


def advance(field, halo, base, y, z, source):
    total = gravity_parts(field, halo, base, y, z)
    phi_rate = [total[0][x] - coupling * source[x] for x in range(NX)]
    new = [[None] * NX for _ in range(4)]
    for x in range(NX):
        change = pseudo_step * phi_rate[x]
        new[0][x] = change if field[0] is None else field[0][x] + change
        for c in range(1, 4):
            if field[c] is None:
                new[c][x] = pseudo_step * total[c][x]
            else:
                new[c][x] = field[c][x] + pseudo_step * (total[c][x] - field[c][x])
    return (new, phi_rate)


def pack_kernel(u_ref, g_ref, *outs):
    pack(load(u_ref) + load(g_ref), outs)


def face_kernel(u_ref, g_ref, vol_ref, alpha_ref, *refs):
    halo = Halo(refs[:6])
    rate_ref, field_ref = refs[6:8]
    outs = refs[8:]
    y, z = (Line(0), Line(1))
    u = load(u_ref)
    g = load(g_ref)
    alpha = alpha_ref[...]
    keep = 1.0 - alpha
    known = [primitive([u[c][x] for c in range(5)]) for x in range(NX)]
    total = load(vol_ref)

    own = [face_data([u[c][x] for c in range(5)], 0, known[x]) for x in range(NX)]
    below = face_data([halo.xlo[c] for c in range(5)], 0)
    above = face_data([halo.xhi[c] for c in range(5)], 0)
    chain = [below] + own + [above]
    faces = [interface(chain[i], chain[i + 1]) for i in range(NX + 1)]
    for x in range(NX):
        inner = alpha * float(1.0 / WEIGHTS[x])
        edge = inner + keep * 6.0
        low_coef = edge if x == 0 else inner
        high_coef = edge if x == NX - 1 else inner
        for c in range(5):
            total[c][x] = total[c][x] + (high_coef * faces[x + 1][c] - low_coef * faces[x][c])
    for d, line in ((1, y), (2, z)):
        inner = alpha * line.by_node(1.0 / WEIGHTS)
        low_coef = inner + keep * line.by_node([6.0, 0.0, 0.0, 0.0])
        high_coef = inner + keep * line.by_node([0.0, 0.0, 0.0, 6.0])
        for x in range(NX):
            mine = face_data([u[c][x] for c in range(5)], d, known[x])
            prev = face_data(
                [
                    jnp.where(line.lowest, halo.low(line.dim, c, x), line.roll(u[c][x], 1))
                    for c in range(5)
                ],
                d,
            )
            after = face_data(
                [jnp.where(line.highest, halo.high(line.dim, c, x), u[c][x]) for c in range(5)], d
            )
            face = interface(prev, mine)
            end = interface(mine, after)
            for c in range(5):
                following = jnp.where(line.highest, end[c], line.roll(face[c], -1))
                total[c][x] = total[c][x] + (high_coef * following - low_coef * face[c])
    rate = [[-2.0 * total[c][x] for x in range(NX)] for c in range(5)]
    for x in range(NX):
        for i in range(3):
            rate[1 + i][x] = rate[1 + i][x] - u[0][x] * g[1 + i][x]
        rate[4][x] = rate[4][x] - (
            u[1][x] * g[1][x] + u[2][x] * g[2][x] + u[3][x] * g[3][x]
        )
        for c in range(5):
            rate_ref[c, x] = rate[c][x]

    source = [u[0][x] - rho_offset for x in range(NX)]
    new, _ = advance(g, halo, 5, y, z, source)
    slope = [(-pseudo_step * coupling) * rate[0][x] for x in range(NX)]
    comps = new + [slope]
    for c in range(5):
        for x in range(NX):
            field_ref[c, x] = comps[c][x]
    pack(comps, outs)


def middle_kernel(u_ref, rate_ref, field_ref, *refs):
    halo = Halo(refs[:6])
    next_ref = refs[6]
    outs = refs[7:]
    y, z = (Line(0), Line(1))
    field = load(field_ref)
    new, _ = advance(field[:4], halo, 0, y, z, [u_ref[0, x] - rho_offset for x in range(NX)])
    slope, _ = advance([field[4], None, None, None], halo, 4, y, z, [rate_ref[0, x] for x in range(NX)])
    comps = new + slope
    for c in range(8):
        for x in range(NX):
            next_ref[c, x] = comps[c][x]
    pack(comps, outs)


def last_kernel(u_ref, rate_ref, field_ref, fast_ref, *refs):
    halo = Halo(refs[:6])
    next_ref, stat_ref = refs[6:]
    y, z = (Line(0), Line(1))
    field = load(field_ref)
    source = [u_ref[0, x] - rho_offset for x in range(NX)]
    new, base_rate = advance(field[:4], halo, 0, y, z, source)
    slope, slope_rate = advance(field[4:], halo, 4, y, z, [rate_ref[0, x] for x in range(NX)])
    comps = new + slope
    for c in range(8):
        for x in range(NX):
            next_ref[c, x] = comps[c][x]
    weight = y.by_node(WEIGHTS) * z.by_node(WEIGHTS)

    def total(values):
        by_x = [float(WEIGHTS[x]) * values[x] for x in range(NX)]
        return jnp.sum(((by_x[0] + by_x[1]) + (by_x[2] + by_x[3])) * weight)

    stats = [
        jnp.max(fast_ref[...]),
        total([a * a for a in base_rate]),
        total([a * b for a, b in zip(base_rate, slope_rate)]),
        total([b * b for b in slope_rate]),
        total(base_rate),
        total(slope_rate),
        total(source),
    ]
    lane = lax.broadcasted_iota(jnp.int32, (1, NZ), 1)
    out = jnp.zeros((1, NZ), F32)
    for i, value in enumerate(stats):
        out = jnp.where(lane == i, value, out)
    stat_ref[...] = out


def finish_kernel(weight_total, u_ref, rate_ref, field_ref, stat_ref, grav_ref, source_ref, norm_ref):
    stat = stat_ref[...]
    part = [stat[:, i : i + 1] for i in range(7)]
    step = cfl_euler * elem_width / (7.0 * part[0])
    mean = part[6] * (1.0 / weight_total)
    shift = coupling * mean
    squares = (
        part[1]
        + step * (2.0 * part[2] + step * part[3])
        + shift * (2.0 * (part[4] + step * part[5]) + shift * weight_total)
    )
    norm_ref[...] = jnp.sqrt(jnp.maximum(squares, 0.0) * (1.0 / weight_total))
    raised = (ITERS * pseudo_step) * shift
    for x in range(NX):
        phi = field_ref[0, x] + step * field_ref[4, x] + raised
        grad = [field_ref[c, x] + step * field_ref[4 + c, x] for c in range(1, 4)]
        grav_ref[0, x] = phi
        for c in range(3):
            grav_ref[1 + c, x] = grad[c]
        rho = u_ref[0, x] + step * rate_ref[0, x]
        work = 0.0
        for c in range(3):
            source_ref[c, x] = -rho * grad[c]
            work = work + (u_ref[1 + c, x] + step * rate_ref[1 + c, x]) * grad[c]
        source_ref[3, x] = -work


def call(kernel, out_shape, flops):
    return pl.pallas_call(
        kernel,
        out_shape=out_shape,
        name=getattr(kernel, "__name__", "finish_kernel"),
        cost_estimate=pl.CostEstimate(flops=flops, bytes_accessed=400000, transcendentals=0),
    )


def exchange(messages):
    received = []
    for axis, first, last in zip((GX, "gy", GZ), messages[0::2], messages[1::2]):
        size = lax.axis_size(axis)
        up = [(i, (i + 1) % size) for i in range(size)]
        received.append(lax.ppermute(last, axis, up))
        received.append(lax.ppermute(first, axis, [(b, a) for a, b in up]))
    return received


def combine(a, b):
    lane = lax.broadcasted_iota(jnp.int32, (1, NZ), 1)
    return jnp.where(lane == 0, jnp.maximum(a, b), a + b)


def swap(stat, axis, mask):
    size = lax.axis_size(axis)
    return combine(stat, lax.ppermute(stat, axis, [(i, i ^ mask) for i in range(size)]))


def slots(stat, axis):
    size = lax.axis_size(axis)
    row = lax.broadcasted_iota(jnp.int32, (size, NZ), 0)
    lane = lax.broadcasted_iota(jnp.int32, (1, NZ), 1)
    every = lax.psum(jnp.where(row == lax.axis_index(axis), stat, 0.0), axis)
    return jnp.where(
        lane == 0, jnp.max(every, axis=0, keepdims=True), jnp.sum(every, axis=0, keepdims=True)
    )


def over_all(stat):
    for axis in ("gx_1", "gy", "gz_1"):
        stat = slots(stat, axis)
    for mask in (1, 2, 4):
        stat = swap(stat, "gz_0", mask)
    return slots(stat, "gx_0")


def shape(*dims):
    return jax.ShapeDtypeStruct(dims, F32)


def local(u, g):
    weight_total = float(
        8.0
        * (u.shape[1] // 4 * lax.axis_size(GX))
        * (u.shape[2] // 4 * lax.axis_size("gy"))
        * (u.shape[3] // 4 * lax.axis_size(GZ))
    )
    full = (NX, NY, NZ)
    messages = call(pack_kernel, message_shapes(9), 10**5)(u, g)
    received = exchange(messages)
    vol, alpha, fast = call(
        volume_kernel, [shape(5, *full), shape(NY, NZ), shape(NY, NZ)], 10**7
    )(u)
    rate, field, *messages = call(
        face_kernel, [shape(5, *full), shape(5, *full)] + message_shapes(5), 10**6
    )(u, g, vol, alpha, *received)
    received = exchange(messages)
    field, *messages = call(middle_kernel, [shape(8, *full)] + message_shapes(8), 10**6)(
        u, rate, field, *received
    )
    received = exchange(messages)
    field, stat = call(last_kernel, [shape(8, *full), shape(1, NZ)], 10**6)(
        u, rate, field, fast, *received
    )
    stat = over_all(stat)
    gravity, gravity_source, norm = call(
        functools.partial(finish_kernel, weight_total),
        [shape(4, *full), shape(4, *full), shape(1, 1)],
        10**5,
    )(u, rate, field, stat)
    return (rate, gravity, gravity_source, norm.reshape(()))


def solution(mesh):
    torus = Mesh(
        mesh.devices.reshape(4, 2, mesh.shape["gy"], 8, 4), ("gx_0", "gx_1", "gy", "gz_0", "gz_1")
    )
    placed = (P(None, GX, "gy", GZ), P(None, GX, "gy", GZ))
    return jax.shard_map(
        local,
        mesh=torus,
        in_specs=placed,
        out_specs=(P(None, GX, "gy", GZ), P(None, GX, "gy", GZ), P(None, GX, "gy", GZ), P()),
        check_vma=False,
    )
```

```python
import functools
import math

import jax
import jax.numpy as jnp
import numpy as np
from jax import lax
from jax.experimental import pallas as pl
from jax.experimental.pallas import tpu as pltpu
from jax.sharding import Mesh
from jax.sharding import PartitionSpec as P

ITERS = 3
GX = ("gx_0", "gx_1")
GZ = ("gz_0", "gz_1")

gamma_gas = 1.4
elem_width = 1.0
cfl_euler = 0.5
alpha_most = 0.5
indicator_level = 0.5 * 10.0 ** (-1.8 * 4.0**0.25)
indicator_slope = math.log((1.0 - 0.0001) / 0.0001) / indicator_level
coupling = 10.0
pseudo_step = 0.3 * elem_width / 7.0
rho_offset = 2.3

NX, NY, NZ = (4, 8, 128)
F32 = jnp.float32


def lgl_tables():
    points = np.array([-1.0, -1.0 / math.sqrt(5.0), 1.0 / math.sqrt(5.0), 1.0])
    weights = np.array([1.0, 5.0, 5.0, 1.0]) / 6.0
    barycentric = np.array(
        [1.0 / np.prod([points[a] - points[b] for b in range(4) if b != a]) for a in range(4)]
    )
    derivative = np.zeros((4, 4))
    for a in range(4):
        for b in range(4):
            if b != a:
                derivative[a, b] = barycentric[b] / barycentric[a] / (points[a] - points[b])
        derivative[a, a] = -np.sum(derivative[a])
    legendre = np.stack(
        [np.ones(4), points, 0.5 * (3.0 * points**2 - 1.0), 0.5 * (5.0 * points**3 - 3.0 * points)],
        axis=1,
    )
    legendre = legendre * np.sqrt((2.0 * np.arange(4) + 1.0) / 2.0)
    gram = np.sum(weights[:, None] * legendre * legendre, axis=0)
    modal_map = (legendre * weights[:, None]).T / gram[:, None]
    return (weights, derivative, modal_map)


WEIGHTS, DERIV, MODAL = lgl_tables()


class Line:
    def __init__(self, dim):
        self.dim = dim
        self.length = (NY, NZ)[dim]
        self.at = lax.broadcasted_iota(jnp.int32, (NY, NZ), dim)
        self.node = self.at % 4
        self.lowest = self.at == 0
        self.highest = self.at == self.length - 1
        self.is0 = self.node == 0
        self.is3 = self.node == 3

    def by_node(self, values):
        v = [float(item) for item in values]
        if v[1] == v[2] and v[0] == v[3]:
            return jnp.where(self.is0 | self.is3, v[0], v[1]).astype(F32)
        return jnp.where(
            self.node < 2,
            jnp.where(self.is0, v[0], v[1]),
            jnp.where(self.is3, v[3], v[2]),
        ).astype(F32)

    def roll(self, value, by):
        return pltpu.roll(value, by % self.length, self.dim)

    def cyc(self, value, k):
        return jnp.where(self.node < 4 - k, self.roll(value, -k), self.roll(value, 4 - k))

    def coef(self, matrix, k, scale=1.0):
        return self.by_node([scale * matrix[i, (i + k) % 4] for i in range(4)])

    def element_sum(self, value):
        value = value + self.cyc(value, 2)
        return value + self.cyc(value, 1)


def quad(at):
    return [at[x] for x in range(NX)]


def load(ref):
    return [[ref[c, x] for x in range(NX)] for c in range(ref.shape[0])]


def pack(comps, flags_ref, outs):
    even = [flags_ref[d] == 0 for d in range(3)]
    xp, xo, yp, yo, zp, zo = outs
    lane = lax.broadcasted_iota(jnp.int32, (NY, NZ), 1)
    first = jnp.zeros((NY, NZ), F32)
    last = jnp.zeros((NY, NZ), F32)
    for c, comp in enumerate(comps):
        xp[c] = jnp.where(even[0], comp[NX - 1], comp[0])
        xo[c] = jnp.where(even[0], comp[0], comp[NX - 1])
        for x in range(NX):
            low, high = (comp[x][0:1, :], comp[x][NY - 1 : NY, :])
            yp[c, pl.ds(x, 1), :] = jnp.where(even[1], high, low)
            yo[c, pl.ds(x, 1), :] = jnp.where(even[1], low, high)
            k = c * NX + x
            here = lane == k
            first = jnp.where(here, pltpu.roll(comp[x], k, 1) if k else comp[x], first)
            last = jnp.where(here, pltpu.roll(comp[x], k + 1, 1), last)
    zp[...] = jnp.where(even[2], last, first)
    zo[...] = jnp.where(even[2], first, last)


class Halo:
    def __init__(self, flags_ref, refs):
        self.even = [flags_ref[d] == 0 for d in range(3)]
        self.refs = refs
        zp, zo = (refs[4][...], refs[5][...])
        self.zlo = jnp.where(self.even[2], zo, zp)
        self.zhi = jnp.where(self.even[2], zp, zo)

    def x_low(self, c):
        return jnp.where(self.even[0], self.refs[1][c], self.refs[0][c])

    def x_high(self, c):
        return jnp.where(self.even[0], self.refs[0][c], self.refs[1][c])

    def row(self, c, x, pair, other):
        line = jnp.where(self.even[1], self.refs[pair][c, pl.ds(x, 1), :], self.refs[other][c, pl.ds(x, 1), :])
        return jnp.broadcast_to(line, (NY, NZ))

    def low(self, dim, c, x):
        if dim == 0:
            return self.row(c, x, 3, 2)
        k = c * NX + x
        return pltpu.roll(self.zlo, (NZ - k) % NZ, 1) if k else self.zlo

    def high(self, dim, c, x):
        if dim == 0:
            return self.row(c, x, 2, 3)
        k = c * NX + x
        return pltpu.roll(self.zhi, NZ - 1 - k, 1)


def message_shapes(n):
    return [shape(n, NY, NZ)] * 2 + [shape(n, NX, NZ)] * 2 + [shape(NY, NZ)] * 2


def log_mean(left, right):
    total = left + right
    gap = right - left
    slope = gap / total
    ratio_sq = slope * slope
    is_close = ratio_sq < 0.0001
    series = 2.0 + ratio_sq * (2.0 / 3.0 + ratio_sq * (2.0 / 5.0 + ratio_sq * (2.0 / 7.0)))
    top = jnp.where(is_close, total, gap)
    low = jnp.where(is_close, series, jnp.log(right / left))
    return top / low


def two_point(left, right, d):
    rho_mean = log_mean(left[0], right[0])
    inv_mean = left[4] * right[4] / log_mean(left[0] * right[4], right[0] * left[4])
    vel = [0.5 * (left[1 + i] + right[1 + i]) for i in range(3)]
    product = left[1] * right[1] + left[2] * right[2] + left[3] * right[3]
    mass = rho_mean * vel[d]
    flux = [mass] + [mass * vel[i] for i in range(3)]
    flux[1 + d] = flux[1 + d] + 0.5 * (left[4] + right[4])
    energy = mass * (0.5 * product + inv_mean * (1.0 / (gamma_gas - 1.0))) + 0.5 * (
        left[4] * right[1 + d] + right[4] * left[1 + d]
    )
    return flux + [energy]


def primitive(u):
    inv = 1.0 / u[0]
    vel = [u[1 + i] * inv for i in range(3)]
    kinetic = u[1] * vel[0] + u[2] * vel[1] + u[3] * vel[2]
    pressure = (gamma_gas - 1.0) * (u[4] - 0.5 * kinetic)
    return (vel, pressure, jnp.sqrt(gamma_gas * pressure * inv))


def face_data(u, d, known=None):
    vel, pressure, sound = known or primitive(u)
    normal = vel[d]
    flux = [u[1 + d]] + [u[1 + i] * normal for i in range(3)] + [(u[4] + pressure) * normal]
    flux[1 + d] = flux[1 + d] + pressure
    return (u, flux, jnp.abs(normal) + sound)


def interface(left, right):
    speed = jnp.maximum(left[2], right[2])
    return [
        0.5 * ((left[1][c] + right[1][c]) - speed * (right[0][c] - left[0][c])) for c in range(5)
    ]


def volume_kernel(u_ref, vol_ref, alpha_ref, fast_ref):
    y, z = (Line(0), Line(1))
    u = load(u_ref)
    known = [primitive([u[c][x] for c in range(5)]) for x in range(NX)]
    nodes = [[u[0][x]] + known[x][0] + [known[x][1]] for x in range(NX)]
    speed = [
        jnp.abs(known[x][0][0]) + jnp.abs(known[x][0][1]) + jnp.abs(known[x][0][2]) + 3.0 * known[x][2]
        for x in range(NX)
    ]
    fast_ref[...] = jnp.maximum(jnp.maximum(speed[0], speed[1]), jnp.maximum(speed[2], speed[3]))

    product = [u[0][x] * known[x][1] for x in range(NX)]
    coeffs = [sum(float(MODAL[a, i]) * product[i] for i in range(4)) for a in range(4)]
    for line in (y, z):
        modal = [line.coef(MODAL, k) for k in range(4)]
        coeffs = [
            modal[0] * value + sum(modal[k] * line.cyc(value, k) for k in range(1, 4))
            for value in coeffs
        ]
    energy = [value * value for value in coeffs]
    total = (energy[0] + energy[1]) + (energy[2] + energy[3])
    low = (energy[0] + energy[1]) + energy[2]
    high = energy[3] + jnp.where(y.is3 | z.is3, low, 0.0)
    share = z.element_sum(y.element_sum(high)) / z.element_sum(y.element_sum(total))
    alpha = alpha_most / (1.0 + jnp.exp(-indicator_slope * (share - indicator_level)))
    alpha_ref[...] = alpha

    volume = [[None] * NX for _ in range(5)]
    for i in range(NX):
        for j in range(i + 1, NX):
            flux = two_point(nodes[i], nodes[j], 0)
            for c in range(5):
                for at, other in ((i, j), (j, i)):
                    term = (2.0 * DERIV[at, other]).astype(np.float32) * flux[c]
                    volume[c][at] = term if volume[c][at] is None else volume[c][at] + term
    for d, line in ((1, y), (2, z)):
        up, across, down = [line.coef(DERIV, k, 2.0) for k in (1, 2, 3)]
        for x in range(NX):
            near = two_point(nodes[x], [line.cyc(a, 1) for a in nodes[x]], d)
            far = two_point(nodes[x], [line.cyc(a, 2) for a in nodes[x]], d)
            for c in range(5):
                volume[c][x] = volume[c][x] + (
                    up * near[c] + down * line.cyc(near[c], 3) + across * far[c]
                )
    keep = 1.0 - alpha
    for c in range(5):
        for x in range(NX):
            vol_ref[c, x] = keep * volume[c][x]


def gravity_parts(field, halo, base, y, z):
    total = [[0.0] * NX for _ in range(4)]
    have = [c for c in range(4) if field[c] is not None]
    where = {c: base + i for i, c in enumerate(have)}

    for c, partner in ((0, 1), (1, 0)):
        if field[partner] is not None:
            for i in range(NX):
                terms = [float(2.0 * DERIV[i, j]) * field[partner][j] for j in range(NX) if DERIV[i, j] != 0.0]
                total[c][i] = total[c][i] + sum(terms[1:], terms[0])
    jumps = {}
    for c in have:
        jumps[c] = (halo.x_low(where[c]) - field[c][0], halo.x_high(where[c]) - field[c][NX - 1])
        for side, x in ((0, 0), (1, NX - 1)):
            total[c][x] = total[c][x] + 6.0 * jumps[c][side]
    for c, partner in ((0, 1), (1, 0)):
        if partner in jumps:
            total[c][0] = total[c][0] - 6.0 * jumps[partner][0]
            total[c][NX - 1] = total[c][NX - 1] + 6.0 * jumps[partner][1]
    for d, line in ((1, y), (2, z)):
        comp = 1 + d
        diag = line.coef(DERIV, 0, 2.0)
        coefs = [line.coef(DERIV, k, 2.0) for k in range(1, 4)]
        sign = line.by_node([-6.0, 0.0, 0.0, 6.0])
        for x in range(NX):
            for c, partner in ((0, comp), (comp, 0)):
                if field[partner] is not None:
                    value = field[partner][x]
                    term = diag * value
                    for k in range(1, 4):
                        term = term + coefs[k - 1] * line.cyc(value, k)
                    total[c][x] = total[c][x] + term
            gaps = {}
            for c in have:
                value = field[c][x]
                prev = jnp.where(line.lowest, halo.low(line.dim, where[c], x), line.roll(value, 1))
                after = jnp.where(line.highest, halo.high(line.dim, where[c], x), line.roll(value, -1))
                beside = jnp.where(line.is0, prev, jnp.where(line.is3, after, value))
                gaps[c] = beside - value
                total[c][x] = total[c][x] + 6.0 * gaps[c]
            for c, partner in ((0, comp), (comp, 0)):
                if partner in gaps:
                    total[c][x] = total[c][x] + sign * gaps[partner]
    return total


def advance(field, halo, base, y, z, source):
    total = gravity_parts(field, halo, base, y, z)
    phi_rate = [total[0][x] - coupling * source[x] for x in range(NX)]
    new = [[None] * NX for _ in range(4)]
    for x in range(NX):
        change = pseudo_step * phi_rate[x]
        new[0][x] = change if field[0] is None else field[0][x] + change
        for c in range(1, 4):
            if field[c] is None:
                new[c][x] = pseudo_step * total[c][x]
            else:
                new[c][x] = field[c][x] + pseudo_step * (total[c][x] - field[c][x])
    return (new, phi_rate)


def pack_kernel(flags_ref, u_ref, g_ref, *outs):
    pack(load(u_ref) + load(g_ref), flags_ref, outs)


def face_kernel(flags_ref, u_ref, g_ref, vol_ref, alpha_ref, *refs):
    halo = Halo(flags_ref, refs[:6])
    rate_ref, field_ref = refs[6:8]
    outs = refs[8:]
    y, z = (Line(0), Line(1))
    u = load(u_ref)
    g = load(g_ref)
    alpha = alpha_ref[...]
    keep = 1.0 - alpha
    known = [primitive([u[c][x] for c in range(5)]) for x in range(NX)]
    total = load(vol_ref)

    own = [face_data([u[c][x] for c in range(5)], 0, known[x]) for x in range(NX)]
    below = face_data([halo.x_low(c) for c in range(5)], 0)
    above = face_data([halo.x_high(c) for c in range(5)], 0)
    chain = [below] + own + [above]
    faces = [interface(chain[i], chain[i + 1]) for i in range(NX + 1)]
    for x in range(NX):
        inner = alpha * float(1.0 / WEIGHTS[x])
        edge = inner + keep * 6.0
        low_coef = edge if x == 0 else inner
        high_coef = edge if x == NX - 1 else inner
        for c in range(5):
            total[c][x] = total[c][x] + (high_coef * faces[x + 1][c] - low_coef * faces[x][c])
    for d, line in ((1, y), (2, z)):
        inner = alpha * line.by_node(1.0 / WEIGHTS)
        low_coef = inner + keep * line.by_node([6.0, 0.0, 0.0, 0.0])
        high_coef = inner + keep * line.by_node([0.0, 0.0, 0.0, 6.0])
        for x in range(NX):
            mine = face_data([u[c][x] for c in range(5)], d, known[x])
            prev = face_data(
                [
                    jnp.where(line.lowest, halo.low(line.dim, c, x), line.roll(u[c][x], 1))
                    for c in range(5)
                ],
                d,
            )
            after = face_data(
                [jnp.where(line.highest, halo.high(line.dim, c, x), u[c][x]) for c in range(5)], d
            )
            face = interface(prev, mine)
            end = interface(mine, after)
            for c in range(5):
                following = jnp.where(line.highest, end[c], line.roll(face[c], -1))
                total[c][x] = total[c][x] + (high_coef * following - low_coef * face[c])
    rate = [[-2.0 * total[c][x] for x in range(NX)] for c in range(5)]
    for x in range(NX):
        for i in range(3):
            rate[1 + i][x] = rate[1 + i][x] - u[0][x] * g[1 + i][x]
        rate[4][x] = rate[4][x] - (
            u[1][x] * g[1][x] + u[2][x] * g[2][x] + u[3][x] * g[3][x]
        )
        for c in range(5):
            rate_ref[c, x] = rate[c][x]

    source = [u[0][x] - rho_offset for x in range(NX)]
    new, _ = advance(g, halo, 5, y, z, source)
    slope = [(-pseudo_step * coupling) * rate[0][x] for x in range(NX)]
    comps = new + [slope]
    for c in range(5):
        for x in range(NX):
            field_ref[c, x] = comps[c][x]
    pack(comps, flags_ref, outs)


def middle_kernel(flags_ref, u_ref, rate_ref, field_ref, *refs):
    halo = Halo(flags_ref, refs[:6])
    next_ref = refs[6]
    outs = refs[7:]
    y, z = (Line(0), Line(1))
    field = load(field_ref)
    new, _ = advance(field[:4], halo, 0, y, z, [u_ref[0, x] - rho_offset for x in range(NX)])
    slope, _ = advance([field[4], None, None, None], halo, 4, y, z, [rate_ref[0, x] for x in range(NX)])
    comps = new + slope
    for c in range(8):
        for x in range(NX):
            next_ref[c, x] = comps[c][x]
    pack(comps, flags_ref, outs)


def last_kernel(flags_ref, u_ref, rate_ref, field_ref, fast_ref, *refs):
    halo = Halo(flags_ref, refs[:6])
    next_ref, stat_ref = refs[6:]
    y, z = (Line(0), Line(1))
    field = load(field_ref)
    source = [u_ref[0, x] - rho_offset for x in range(NX)]
    new, base_rate = advance(field[:4], halo, 0, y, z, source)
    slope, slope_rate = advance(field[4:], halo, 4, y, z, [rate_ref[0, x] for x in range(NX)])
    comps = new + slope
    for c in range(8):
        for x in range(NX):
            next_ref[c, x] = comps[c][x]
    weight = y.by_node(WEIGHTS) * z.by_node(WEIGHTS)

    def total(values):
        by_x = [float(WEIGHTS[x]) * values[x] for x in range(NX)]
        return jnp.sum(((by_x[0] + by_x[1]) + (by_x[2] + by_x[3])) * weight)

    stats = [
        jnp.max(fast_ref[...]),
        total([a * a for a in base_rate]),
        total([a * b for a, b in zip(base_rate, slope_rate)]),
        total([b * b for b in slope_rate]),
        total(base_rate),
        total(slope_rate),
        total(source),
    ]
    lane = lax.broadcasted_iota(jnp.int32, (1, NZ), 1)
    out = jnp.zeros((1, NZ), F32)
    for i, value in enumerate(stats):
        out = jnp.where(lane == i, value, out)
    stat_ref[...] = out


def finish_kernel(weight_total, u_ref, rate_ref, field_ref, stat_ref, grav_ref, source_ref, norm_ref):
    stat = stat_ref[...]
    part = [stat[:, i : i + 1] for i in range(7)]
    step = cfl_euler * elem_width / (7.0 * part[0])
    mean = part[6] * (1.0 / weight_total)
    shift = coupling * mean
    squares = (
        part[1]
        + step * (2.0 * part[2] + step * part[3])
        + shift * (2.0 * (part[4] + step * part[5]) + shift * weight_total)
    )
    norm_ref[...] = jnp.sqrt(jnp.maximum(squares, 0.0) * (1.0 / weight_total))
    raised = (ITERS * pseudo_step) * shift
    for x in range(NX):
        phi = field_ref[0, x] + step * field_ref[4, x] + raised
        grad = [field_ref[c, x] + step * field_ref[4 + c, x] for c in range(1, 4)]
        grav_ref[0, x] = phi
        for c in range(3):
            grav_ref[1 + c, x] = grad[c]
        rho = u_ref[0, x] + step * rate_ref[0, x]
        work = 0.0
        for c in range(3):
            source_ref[c, x] = -rho * grad[c]
            work = work + (u_ref[1 + c, x] + step * rate_ref[1 + c, x]) * grad[c]
        source_ref[3, x] = -work


def call(kernel, out_shape, flops, flags=None):
    def run(*args):
        specs = [pl.BlockSpec(memory_space=pltpu.VMEM)] * len(args)
        args = [pltpu.with_memory_space_constraint(a, pltpu.VMEM) for a in args]
        if flags is not None:
            specs = [pl.BlockSpec(memory_space=pltpu.SMEM)] + specs
            args = [flags] + args
        return pl.pallas_call(
            kernel,
            in_specs=specs,
            out_specs=[pl.BlockSpec(memory_space=pltpu.VMEM)] * len(out_shape),
            out_shape=out_shape,
            name=getattr(kernel, "__name__", "finish_kernel"),
            cost_estimate=pl.CostEstimate(flops=flops, bytes_accessed=400000, transcendentals=0),
        )(*args)

    return run


def pair_of(i, size):
    return i ^ 1


def other_of(i, size):
    return (i + 1 if i % 2 else i - 1) % size


def exchange(messages):
    received = [None] * 6
    for i in (1, 5, 3, 2, 4, 0):
        axis = (GX, "gy", GZ)[i // 2]
        partner = (pair_of, other_of)[i % 2]
        size = lax.axis_size(axis)
        received[i] = lax.ppermute(messages[i], axis, [(a, partner(a, size)) for a in range(size)])
    return received


def slots(stat, axis):
    size = lax.axis_size(axis)
    row = lax.broadcasted_iota(jnp.int32, (size, NZ), 0)
    lane = lax.broadcasted_iota(jnp.int32, (1, NZ), 1)
    every = lax.psum(jnp.where(row == lax.axis_index(axis), stat, 0.0), axis)
    return jnp.where(
        lane == 0, jnp.max(every, axis=0, keepdims=True), jnp.sum(every, axis=0, keepdims=True)
    )


def spread(stat):
    names = ("gx_0", "gx_1", "gy", "gz_0", "gz_1")
    sizes = [lax.axis_size(name) for name in names]
    ring = sizes[0] * sizes[3]
    pairs = []
    for at in np.ndindex(*sizes):
        a, core, b, c, e = at
        place = (a * sizes[3] + c + core * sizes[4] + e - (sizes[3] // 2 - 1)) % ring
        to = (place // sizes[3], core, b, place % sizes[3], e)
        pairs.append(
            (int(np.ravel_multi_index(at, sizes)), int(np.ravel_multi_index(to, sizes)))
        )
    return lax.ppermute(stat, names, pairs)


def over_all(stat):
    for axis in ("gx_1", "gy", "gz_1"):
        stat = slots(stat, axis)
    stat = spread(stat)
    for axis in ("gx_1", "gz_1", "gx_0"):
        stat = slots(stat, axis)
    return stat


def shape(*dims):
    return pltpu.VMEM(dims, F32)


def local(u, g):
    weight_total = float(
        8.0
        * (u.shape[1] // 4 * lax.axis_size(GX))
        * (u.shape[2] // 4 * lax.axis_size("gy"))
        * (u.shape[3] // 4 * lax.axis_size(GZ))
    )
    full = (NX, NY, NZ)
    flags = jnp.stack([lax.axis_index(axis) & 1 for axis in ("gx_1", "gy", "gz_1")])
    messages = call(pack_kernel, message_shapes(9), 10**5, flags)(u, g)
    received = exchange(messages)
    vol, alpha, fast = call(
        volume_kernel, [shape(5, *full), shape(NY, NZ), shape(NY, NZ)], 10**7
    )(u)
    rate, field, *messages = call(
        face_kernel, [shape(5, *full), shape(5, *full)] + message_shapes(5), 10**6, flags
    )(u, g, vol, alpha, *received)
    received = exchange(messages)
    field, *messages = call(middle_kernel, [shape(8, *full)] + message_shapes(8), 10**6, flags)(
        u, rate, field, *received
    )
    received = exchange(messages)
    field, stat = call(last_kernel, [shape(8, *full), shape(1, NZ)], 10**6, flags)(
        u, rate, field, fast, *received
    )
    stat = over_all(stat)
    gravity, gravity_source, norm = call(
        functools.partial(finish_kernel, weight_total),
        [jax.ShapeDtypeStruct((4, *full), F32)] * 2 + [jax.ShapeDtypeStruct((1, 1), F32)],
        10**5,
    )(u, rate, field, stat)
    return (rate, gravity, gravity_source, norm.reshape(()))


def solution(mesh):
    torus = Mesh(
        mesh.devices.reshape(4, 2, mesh.shape["gy"], 8, 4), ("gx_0", "gx_1", "gy", "gz_0", "gz_1")
    )
    placed = (P(None, GX, "gy", GZ), P(None, GX, "gy", GZ))
    return jax.shard_map(
        local,
        mesh=torus,
        in_specs=placed,
        out_specs=(P(None, GX, "gy", GZ), P(None, GX, "gy", GZ), P(None, GX, "gy", GZ), P()),
        check_vma=False,
    )
```

```python
import functools
import math

import jax
import jax.numpy as jnp
import numpy as np
from jax import lax
from jax.experimental import pallas as pl
from jax.experimental.pallas import tpu as pltpu
from jax.sharding import Mesh
from jax.sharding import PartitionSpec as P


ITERS = 3
GX = ("gx_0", "gx_1")
GZ = ("gz_0", "gz_1")

gamma_gas = 1.4
elem_width = 1.0
cfl_euler = 0.5
alpha_most = 0.5
indicator_level = 0.5 * 10.0 ** (-1.8 * 4.0**0.25)
indicator_slope = math.log((1.0 - 0.0001) / 0.0001) / indicator_level
coupling = 10.0
pseudo_step = 0.3 * elem_width / 7.0
rho_offset = 2.3

NX, NY, NZ = (4, 8, 128)
F32 = jnp.float32


def lgl_tables():
    points = np.array([-1.0, -1.0 / math.sqrt(5.0), 1.0 / math.sqrt(5.0), 1.0])
    weights = np.array([1.0, 5.0, 5.0, 1.0]) / 6.0
    barycentric = np.array(
        [1.0 / np.prod([points[a] - points[b] for b in range(4) if b != a]) for a in range(4)]
    )
    derivative = np.zeros((4, 4))
    for a in range(4):
        for b in range(4):
            if b != a:
                derivative[a, b] = barycentric[b] / barycentric[a] / (points[a] - points[b])
        derivative[a, a] = -np.sum(derivative[a])
    legendre = np.stack(
        [np.ones(4), points, 0.5 * (3.0 * points**2 - 1.0), 0.5 * (5.0 * points**3 - 3.0 * points)],
        axis=1,
    )
    legendre = legendre * np.sqrt((2.0 * np.arange(4) + 1.0) / 2.0)
    gram = np.sum(weights[:, None] * legendre * legendre, axis=0)
    modal_map = (legendre * weights[:, None]).T / gram[:, None]
    return (weights, derivative, modal_map)


WEIGHTS, DERIV, MODAL = lgl_tables()


class Line:
    def __init__(self, dim):
        self.dim = dim
        self.length = (NY, NZ)[dim]
        self.at = lax.broadcasted_iota(jnp.int32, (NY, NZ), dim)
        self.node = self.at % 4
        self.lowest = self.at == 0
        self.highest = self.at == self.length - 1
        self.is0 = self.node == 0
        self.is3 = self.node == 3

    def by_node(self, values):
        v = [float(item) for item in values]
        if v[1] == v[2] and v[0] == v[3]:
            return jnp.where(self.is0 | self.is3, v[0], v[1]).astype(F32)
        return jnp.where(
            self.node < 2,
            jnp.where(self.is0, v[0], v[1]),
            jnp.where(self.is3, v[3], v[2]),
        ).astype(F32)

    def roll(self, value, by):
        return pltpu.roll(value, by % self.length, self.dim)

    def cyc(self, value, k):
        return jnp.where(self.node < 4 - k, self.roll(value, -k), self.roll(value, 4 - k))

    def coef(self, matrix, k, scale=1.0):
        return self.by_node([scale * matrix[i, (i + k) % 4] for i in range(4)])

    def element_sum(self, value):
        value = value + self.cyc(value, 2)
        return value + self.cyc(value, 1)


def load(ref):
    return [[ref[c, x] for x in range(NX)] for c in range(ref.shape[0])]


def pack(comps, flags_ref, outs):
    even = [flags_ref[d] == 0 for d in range(3)]
    xo, zo, yo, yp, zp, xp = outs
    lane = lax.broadcasted_iota(jnp.int32, (NY, NZ), 1)
    first = jnp.zeros((NY, NZ), F32)
    last = jnp.zeros((NY, NZ), F32)
    for c, comp in enumerate(comps):
        xp[c] = jnp.where(even[0], comp[NX - 1], comp[0])
        xo[c] = jnp.where(even[0], comp[0], comp[NX - 1])
        for x in range(NX):
            low, high = (comp[x][0:1, :], comp[x][NY - 1 : NY, :])
            yp[c, pl.ds(x, 1), :] = jnp.where(even[1], high, low)
            yo[c, pl.ds(x, 1), :] = jnp.where(even[1], low, high)
            k = c * NX + x
            here = lane == k
            first = jnp.where(here, pltpu.roll(comp[x], k, 1) if k else comp[x], first)
            last = jnp.where(here, pltpu.roll(comp[x], k + 1, 1), last)
    zp[...] = jnp.where(even[2], last, first)
    zo[...] = jnp.where(even[2], first, last)


class Halo:
    def __init__(self, flags_ref, refs):
        self.even = [flags_ref[d] == 0 for d in range(3)]
        self.refs = refs
        zo, zp = (refs[1][...], refs[4][...])
        self.zlo = jnp.where(self.even[2], zo, zp)
        self.zhi = jnp.where(self.even[2], zp, zo)

    def x_low(self, c):
        return jnp.where(self.even[0], self.refs[0][c], self.refs[5][c])

    def x_high(self, c):
        return jnp.where(self.even[0], self.refs[5][c], self.refs[0][c])

    def row(self, c, x, pair, other):
        line = jnp.where(self.even[1], self.refs[pair][c, pl.ds(x, 1), :], self.refs[other][c, pl.ds(x, 1), :])
        return jnp.broadcast_to(line, (NY, NZ))

    def low(self, dim, c, x):
        if dim == 0:
            return self.row(c, x, 2, 3)
        k = c * NX + x
        return pltpu.roll(self.zlo, (NZ - k) % NZ, 1) if k else self.zlo

    def high(self, dim, c, x):
        if dim == 0:
            return self.row(c, x, 3, 2)
        k = c * NX + x
        return pltpu.roll(self.zhi, NZ - 1 - k, 1)


def message_shapes(n):
    plane, rows, columns = (shape(n, NY, NZ), shape(n, NX, NZ), shape(NY, NZ))
    return [plane, columns, rows, rows, columns, plane]


def log_mean(left, right):
    total = left + right
    gap = right - left
    slope = gap / total
    ratio_sq = slope * slope
    is_close = ratio_sq < 0.0001
    series = 2.0 + ratio_sq * (2.0 / 3.0 + ratio_sq * (2.0 / 5.0 + ratio_sq * (2.0 / 7.0)))
    top = jnp.where(is_close, total, gap)
    low = jnp.where(is_close, series, jnp.log(right / left))
    return top / low


def two_point(left, right, d):
    rho_mean = log_mean(left[0], right[0])
    inv_mean = left[4] * right[4] / log_mean(left[0] * right[4], right[0] * left[4])
    vel = [0.5 * (left[1 + i] + right[1 + i]) for i in range(3)]
    product = left[1] * right[1] + left[2] * right[2] + left[3] * right[3]
    mass = rho_mean * vel[d]
    flux = [mass] + [mass * vel[i] for i in range(3)]
    flux[1 + d] = flux[1 + d] + 0.5 * (left[4] + right[4])
    energy = mass * (0.5 * product + inv_mean * (1.0 / (gamma_gas - 1.0))) + 0.5 * (
        left[4] * right[1 + d] + right[4] * left[1 + d]
    )
    return flux + [energy]


def primitive(u):
    inv = 1.0 / u[0]
    vel = [u[1 + i] * inv for i in range(3)]
    kinetic = u[1] * vel[0] + u[2] * vel[1] + u[3] * vel[2]
    pressure = (gamma_gas - 1.0) * (u[4] - 0.5 * kinetic)
    return (vel, pressure, jnp.sqrt(gamma_gas * pressure * inv))


def face_data(u, d, known=None):
    vel, pressure, sound = known or primitive(u)
    normal = vel[d]
    flux = [u[1 + d]] + [u[1 + i] * normal for i in range(3)] + [(u[4] + pressure) * normal]
    flux[1 + d] = flux[1 + d] + pressure
    return (u, flux, jnp.abs(normal) + sound)


def interface(left, right):
    speed = jnp.maximum(left[2], right[2])
    return [
        0.5 * ((left[1][c] + right[1][c]) - speed * (right[0][c] - left[0][c])) for c in range(5)
    ]


def volume_kernel(u_ref, vol_ref, alpha_ref, fast_ref):
    y, z = (Line(0), Line(1))
    u = load(u_ref)
    known = [primitive([u[c][x] for c in range(5)]) for x in range(NX)]
    nodes = [[u[0][x]] + known[x][0] + [known[x][1]] for x in range(NX)]
    speed = [
        jnp.abs(known[x][0][0]) + jnp.abs(known[x][0][1]) + jnp.abs(known[x][0][2]) + 3.0 * known[x][2]
        for x in range(NX)
    ]
    fast_ref[...] = jnp.maximum(jnp.maximum(speed[0], speed[1]), jnp.maximum(speed[2], speed[3]))

    product = [u[0][x] * known[x][1] for x in range(NX)]
    coeffs = [sum(float(MODAL[a, i]) * product[i] for i in range(4)) for a in range(4)]
    for line in (y, z):
        modal = [line.coef(MODAL, k) for k in range(4)]
        coeffs = [
            modal[0] * value + sum(modal[k] * line.cyc(value, k) for k in range(1, 4))
            for value in coeffs
        ]
    energy = [value * value for value in coeffs]
    total = (energy[0] + energy[1]) + (energy[2] + energy[3])
    low = (energy[0] + energy[1]) + energy[2]
    high = energy[3] + jnp.where(y.is3 | z.is3, low, 0.0)
    share = z.element_sum(y.element_sum(high)) / z.element_sum(y.element_sum(total))
    alpha = alpha_most / (1.0 + jnp.exp(-indicator_slope * (share - indicator_level)))
    alpha_ref[...] = alpha

    volume = [[None] * NX for _ in range(5)]
    for i in range(NX):
        for j in range(i + 1, NX):
            flux = two_point(nodes[i], nodes[j], 0)
            for c in range(5):
                for at, other in ((i, j), (j, i)):
                    term = (2.0 * DERIV[at, other]).astype(np.float32) * flux[c]
                    volume[c][at] = term if volume[c][at] is None else volume[c][at] + term
    for d, line in ((1, y), (2, z)):
        up, across, down = [line.coef(DERIV, k, 2.0) for k in (1, 2, 3)]
        for x in range(NX):
            near = two_point(nodes[x], [line.cyc(a, 1) for a in nodes[x]], d)
            far = two_point(nodes[x], [line.cyc(a, 2) for a in nodes[x]], d)
            for c in range(5):
                volume[c][x] = volume[c][x] + (
                    up * near[c] + down * line.cyc(near[c], 3) + across * far[c]
                )
    keep = 1.0 - alpha
    for c in range(5):
        for x in range(NX):
            vol_ref[c, x] = keep * volume[c][x]


def gravity_parts(field, halo, base, y, z):
    total = [[0.0] * NX for _ in range(4)]
    have = [c for c in range(4) if field[c] is not None]
    where = {c: base + i for i, c in enumerate(have)}

    for c, partner in ((0, 1), (1, 0)):
        if field[partner] is not None:
            for i in range(NX):
                terms = [float(2.0 * DERIV[i, j]) * field[partner][j] for j in range(NX) if DERIV[i, j] != 0.0]
                total[c][i] = total[c][i] + sum(terms[1:], terms[0])
    jumps = {}
    for c in have:
        jumps[c] = (halo.x_low(where[c]) - field[c][0], halo.x_high(where[c]) - field[c][NX - 1])
        for side, x in ((0, 0), (1, NX - 1)):
            total[c][x] = total[c][x] + 6.0 * jumps[c][side]
    for c, partner in ((0, 1), (1, 0)):
        if partner in jumps:
            total[c][0] = total[c][0] - 6.0 * jumps[partner][0]
            total[c][NX - 1] = total[c][NX - 1] + 6.0 * jumps[partner][1]
    for d, line in ((1, y), (2, z)):
        comp = 1 + d
        diag = line.coef(DERIV, 0, 2.0)
        coefs = [line.coef(DERIV, k, 2.0) for k in range(1, 4)]
        sign = line.by_node([-6.0, 0.0, 0.0, 6.0])
        for x in range(NX):
            for c, partner in ((0, comp), (comp, 0)):
                if field[partner] is not None:
                    value = field[partner][x]
                    term = diag * value
                    for k in range(1, 4):
                        term = term + coefs[k - 1] * line.cyc(value, k)
                    total[c][x] = total[c][x] + term
            gaps = {}
            for c in have:
                value = field[c][x]
                prev = jnp.where(line.lowest, halo.low(line.dim, where[c], x), line.roll(value, 1))
                after = jnp.where(line.highest, halo.high(line.dim, where[c], x), line.roll(value, -1))
                beside = jnp.where(line.is0, prev, jnp.where(line.is3, after, value))
                gaps[c] = beside - value
                total[c][x] = total[c][x] + 6.0 * gaps[c]
            for c, partner in ((0, comp), (comp, 0)):
                if partner in gaps:
                    total[c][x] = total[c][x] + sign * gaps[partner]
    return total


def advance(field, halo, base, y, z, source):
    total = gravity_parts(field, halo, base, y, z)
    phi_rate = [total[0][x] - coupling * source[x] for x in range(NX)]
    new = [[None] * NX for _ in range(4)]
    for x in range(NX):
        change = pseudo_step * phi_rate[x]
        new[0][x] = change if field[0] is None else field[0][x] + change
        for c in range(1, 4):
            if field[c] is None:
                new[c][x] = pseudo_step * total[c][x]
            else:
                new[c][x] = field[c][x] + pseudo_step * (total[c][x] - field[c][x])
    return (new, phi_rate)


def pack_kernel(flags_ref, u_ref, g_ref, *outs):
    pack(load(u_ref) + load(g_ref), flags_ref, outs)


def face_kernel(flags_ref, u_ref, g_ref, vol_ref, alpha_ref, *refs):
    halo = Halo(flags_ref, refs[:6])
    rate_ref, field_ref = refs[6:8]
    outs = refs[8:]
    y, z = (Line(0), Line(1))
    u = load(u_ref)
    g = load(g_ref)
    alpha = alpha_ref[...]
    keep = 1.0 - alpha
    known = [primitive([u[c][x] for c in range(5)]) for x in range(NX)]
    total = load(vol_ref)

    own = [face_data([u[c][x] for c in range(5)], 0, known[x]) for x in range(NX)]
    below = face_data([halo.x_low(c) for c in range(5)], 0)
    above = face_data([halo.x_high(c) for c in range(5)], 0)
    chain = [below] + own + [above]
    faces = [interface(chain[i], chain[i + 1]) for i in range(NX + 1)]
    for x in range(NX):
        inner = alpha * float(1.0 / WEIGHTS[x])
        edge = inner + keep * 6.0
        low_coef = edge if x == 0 else inner
        high_coef = edge if x == NX - 1 else inner
        for c in range(5):
            total[c][x] = total[c][x] + (high_coef * faces[x + 1][c] - low_coef * faces[x][c])
    for d, line in ((1, y), (2, z)):
        inner = alpha * line.by_node(1.0 / WEIGHTS)
        low_coef = inner + keep * line.by_node([6.0, 0.0, 0.0, 0.0])
        high_coef = inner + keep * line.by_node([0.0, 0.0, 0.0, 6.0])
        for x in range(NX):
            mine = face_data([u[c][x] for c in range(5)], d, known[x])
            prev = face_data(
                [
                    jnp.where(line.lowest, halo.low(line.dim, c, x), line.roll(u[c][x], 1))
                    for c in range(5)
                ],
                d,
            )
            after = face_data(
                [jnp.where(line.highest, halo.high(line.dim, c, x), u[c][x]) for c in range(5)], d
            )
            face = interface(prev, mine)
            end = interface(mine, after)
            for c in range(5):
                following = jnp.where(line.highest, end[c], line.roll(face[c], -1))
                total[c][x] = total[c][x] + (high_coef * following - low_coef * face[c])
    rate = [[-2.0 * total[c][x] for x in range(NX)] for c in range(5)]
    for x in range(NX):
        for i in range(3):
            rate[1 + i][x] = rate[1 + i][x] - u[0][x] * g[1 + i][x]
        rate[4][x] = rate[4][x] - (
            u[1][x] * g[1][x] + u[2][x] * g[2][x] + u[3][x] * g[3][x]
        )
        for c in range(5):
            rate_ref[c, x] = rate[c][x]

    source = [u[0][x] - rho_offset for x in range(NX)]
    new, _ = advance(g, halo, 5, y, z, source)
    slope = [(-pseudo_step * coupling) * rate[0][x] for x in range(NX)]
    comps = new + [slope]
    for c in range(5):
        for x in range(NX):
            field_ref[c, x] = comps[c][x]
    pack(comps, flags_ref, outs)


def middle_kernel(flags_ref, u_ref, rate_ref, field_ref, *refs):
    halo = Halo(flags_ref, refs[:6])
    next_ref = refs[6]
    outs = refs[7:]
    y, z = (Line(0), Line(1))
    field = load(field_ref)
    new, _ = advance(field[:4], halo, 0, y, z, [u_ref[0, x] - rho_offset for x in range(NX)])
    slope, _ = advance([field[4], None, None, None], halo, 4, y, z, [rate_ref[0, x] for x in range(NX)])
    comps = new + slope
    for c in range(8):
        for x in range(NX):
            next_ref[c, x] = comps[c][x]
    pack(comps, flags_ref, outs)


def last_kernel(flags_ref, u_ref, rate_ref, field_ref, fast_ref, *refs):
    halo = Halo(flags_ref, refs[:6])
    next_ref, stat_ref = refs[6:]
    y, z = (Line(0), Line(1))
    field = load(field_ref)
    source = [u_ref[0, x] - rho_offset for x in range(NX)]
    new, base_rate = advance(field[:4], halo, 0, y, z, source)
    slope, slope_rate = advance(field[4:], halo, 4, y, z, [rate_ref[0, x] for x in range(NX)])
    comps = new + slope
    for c in range(8):
        for x in range(NX):
            next_ref[c, x] = comps[c][x]
    weight = y.by_node(WEIGHTS) * z.by_node(WEIGHTS)

    def total(values):
        by_x = [float(WEIGHTS[x]) * values[x] for x in range(NX)]
        return jnp.sum(((by_x[0] + by_x[1]) + (by_x[2] + by_x[3])) * weight)

    stats = [
        jnp.max(fast_ref[...]),
        total([a * a for a in base_rate]),
        total([a * b for a, b in zip(base_rate, slope_rate)]),
        total([b * b for b in slope_rate]),
        total(base_rate),
        total(slope_rate),
        total(source),
    ]
    lane = lax.broadcasted_iota(jnp.int32, (1, NZ), 1)
    out = jnp.zeros((1, NZ), F32)
    for i, value in enumerate(stats):
        out = jnp.where(lane == i, value, out)
    stat_ref[...] = out


def finish_kernel(weight_total, u_ref, rate_ref, field_ref, stat_ref, grav_ref, source_ref, norm_ref):
    stat = stat_ref[...]
    part = [stat[:, i : i + 1] for i in range(7)]
    step = cfl_euler * elem_width / (7.0 * part[0])
    mean = part[6] * (1.0 / weight_total)
    shift = coupling * mean
    squares = (
        part[1]
        + step * (2.0 * part[2] + step * part[3])
        + shift * (2.0 * (part[4] + step * part[5]) + shift * weight_total)
    )
    norm_ref[...] = jnp.sqrt(jnp.maximum(squares, 0.0) * (1.0 / weight_total))
    raised = (ITERS * pseudo_step) * shift
    for x in range(NX):
        phi = field_ref[0, x] + step * field_ref[4, x] + raised
        grad = [field_ref[c, x] + step * field_ref[4 + c, x] for c in range(1, 4)]
        grav_ref[0, x] = phi
        for c in range(3):
            grav_ref[1 + c, x] = grad[c]
        rho = u_ref[0, x] + step * rate_ref[0, x]
        work = 0.0
        for c in range(3):
            source_ref[c, x] = -rho * grad[c]
            work = work + (u_ref[1 + c, x] + step * rate_ref[1 + c, x]) * grad[c]
        source_ref[3, x] = -work


def call(kernel, out_shape, flops, flags=None):
    def run(*args):
        specs = [pl.BlockSpec(memory_space=pltpu.VMEM)] * len(args)
        args = [pltpu.with_memory_space_constraint(a, pltpu.VMEM) for a in args]
        if flags is not None:
            specs = [pl.BlockSpec(memory_space=pltpu.SMEM)] + specs
            args = [flags] + args
        return pl.pallas_call(
            kernel,
            in_specs=specs,
            out_specs=[pl.BlockSpec(memory_space=pltpu.VMEM)] * len(out_shape),
            out_shape=out_shape,
            cost_estimate=pl.CostEstimate(flops=flops, bytes_accessed=400000, transcendentals=0),
        )(*args)

    return run


def pair_of(i, size):
    return i ^ 1


def other_of(i, size):
    return (i + 1 if i % 2 else i - 1) % size


ROUTES = (
    (GX, other_of),
    (GZ, other_of),
    ("gy", other_of),
    ("gy", pair_of),
    (GZ, pair_of),
    (GX, pair_of),
)


def exchange(messages):
    received = []
    for message, (axis, partner) in zip(messages, ROUTES):
        size = lax.axis_size(axis)
        received.append(lax.ppermute(message, axis, [(a, partner(a, size)) for a in range(size)]))
    return received


def slots(stat, axis):
    size = lax.axis_size(axis)
    row = lax.broadcasted_iota(jnp.int32, (size, NZ), 0)
    lane = lax.broadcasted_iota(jnp.int32, (1, NZ), 1)
    every = lax.psum(jnp.where(row == lax.axis_index(axis), stat, 0.0), axis)
    return jnp.where(
        lane == 0, jnp.max(every, axis=0, keepdims=True), jnp.sum(every, axis=0, keepdims=True)
    )


def spread(stat):
    names = ("gx_0", "gx_1", "gy", "gz_0", "gz_1")
    sizes = [lax.axis_size(name) for name in names]
    ring = sizes[0] * sizes[3]
    pairs = []
    for at in np.ndindex(*sizes):
        a, core, b, c, e = at
        place = (a * sizes[3] + c + core * sizes[4] + e - (sizes[3] // 2 - 1)) % ring
        to = (place // sizes[3], core, b, place % sizes[3], e)
        pairs.append(
            (int(np.ravel_multi_index(at, sizes)), int(np.ravel_multi_index(to, sizes)))
        )
    return lax.ppermute(stat, names, pairs)


def over_all(stat):
    for axis in ("gx_1", "gy", "gz_1"):
        stat = slots(stat, axis)
    stat = spread(stat)
    for axis in ("gx_1", "gz_1", "gx_0"):
        stat = slots(stat, axis)
    return stat


def shape(*dims):
    return pltpu.VMEM(dims, F32)


def local(u, g):
    weight_total = float(
        8.0
        * (u.shape[1] // 4 * lax.axis_size(GX))
        * (u.shape[2] // 4 * lax.axis_size("gy"))
        * (u.shape[3] // 4 * lax.axis_size(GZ))
    )
    full = (NX, NY, NZ)
    flags = jnp.stack([lax.axis_index(axis) & 1 for axis in ("gx_1", "gy", "gz_1")])
    messages = call(pack_kernel, message_shapes(9), 10**5, flags)(u, g)
    received = exchange(messages)
    vol, alpha, fast = call(
        volume_kernel, [shape(5, *full), shape(NY, NZ), shape(NY, NZ)], 10**7
    )(u)
    rate, field, *messages = call(
        face_kernel, [shape(5, *full), shape(5, *full)] + message_shapes(5), 10**6, flags
    )(u, g, vol, alpha, *received)
    received = exchange(messages)
    field, *messages = call(middle_kernel, [shape(8, *full)] + message_shapes(8), 10**6, flags)(
        u, rate, field, *received
    )
    received = exchange(messages)
    field, stat = call(last_kernel, [shape(8, *full), shape(1, NZ)], 10**6, flags)(
        u, rate, field, fast, *received
    )
    stat = over_all(stat)
    gravity, gravity_source, norm = call(
        functools.partial(finish_kernel, weight_total),
        [jax.ShapeDtypeStruct((4, *full), F32)] * 2 + [jax.ShapeDtypeStruct((1, 1), F32)],
        10**5,
    )(u, rate, field, stat)
    return (rate, gravity, gravity_source, norm.reshape(()))


def solution(mesh):
    torus = Mesh(
        mesh.devices.reshape(4, 2, mesh.shape["gy"], 8, 4), ("gx_0", "gx_1", "gy", "gz_0", "gz_1")
    )
    placed = (P(None, GX, "gy", GZ), P(None, GX, "gy", GZ))
    return jax.shard_map(
        local,
        mesh=torus,
        in_specs=placed,
        out_specs=(P(None, GX, "gy", GZ), P(None, GX, "gy", GZ), P(None, GX, "gy", GZ), P()),
        check_vma=False,
    )
```

```python
import functools
import math

import jax
import jax.numpy as jnp
import numpy as np
from jax import lax
from jax.experimental import pallas as pl
from jax.experimental.pallas import tpu as pltpu
from jax.sharding import Mesh
from jax.sharding import PartitionSpec as P


ITERS = 3
GX = ("gx_0", "gx_1")
GZ = ("gz_0", "gz_1")

gamma_gas = 1.4
elem_width = 1.0
cfl_euler = 0.5
alpha_most = 0.5
indicator_level = 0.5 * 10.0 ** (-1.8 * 4.0**0.25)
indicator_slope = math.log((1.0 - 0.0001) / 0.0001) / indicator_level
coupling = 10.0
pseudo_step = 0.3 * elem_width / 7.0
rho_offset = 2.3

NX, NY, NZ = (4, 8, 128)
F32 = jnp.float32


def lgl_tables():
    points = np.array([-1.0, -1.0 / math.sqrt(5.0), 1.0 / math.sqrt(5.0), 1.0])
    weights = np.array([1.0, 5.0, 5.0, 1.0]) / 6.0
    barycentric = np.array(
        [1.0 / np.prod([points[a] - points[b] for b in range(4) if b != a]) for a in range(4)]
    )
    derivative = np.zeros((4, 4))
    for a in range(4):
        for b in range(4):
            if b != a:
                derivative[a, b] = barycentric[b] / barycentric[a] / (points[a] - points[b])
        derivative[a, a] = -np.sum(derivative[a])
    legendre = np.stack(
        [np.ones(4), points, 0.5 * (3.0 * points**2 - 1.0), 0.5 * (5.0 * points**3 - 3.0 * points)],
        axis=1,
    )
    legendre = legendre * np.sqrt((2.0 * np.arange(4) + 1.0) / 2.0)
    gram = np.sum(weights[:, None] * legendre * legendre, axis=0)
    modal_map = (legendre * weights[:, None]).T / gram[:, None]
    return (weights, derivative, modal_map)


WEIGHTS, DERIV, MODAL = lgl_tables()


class Line:
    def __init__(self, dim):
        self.dim = dim
        self.length = (NY, NZ)[dim]
        self.at = lax.broadcasted_iota(jnp.int32, (NY, NZ), dim)
        self.node = self.at % 4
        self.lowest = self.at == 0
        self.highest = self.at == self.length - 1
        self.is0 = self.node == 0
        self.is3 = self.node == 3

    def by_node(self, values):
        v = [float(item) for item in values]
        if v[1] == v[2] and v[0] == v[3]:
            return jnp.where(self.is0 | self.is3, v[0], v[1]).astype(F32)
        return jnp.where(
            self.node < 2,
            jnp.where(self.is0, v[0], v[1]),
            jnp.where(self.is3, v[3], v[2]),
        ).astype(F32)

    def roll(self, value, by):
        return pltpu.roll(value, by % self.length, self.dim)

    def cyc(self, value, k):
        return jnp.where(self.node < 4 - k, self.roll(value, -k), self.roll(value, 4 - k))

    def coef(self, matrix, k, scale=1.0):
        return self.by_node([scale * matrix[i, (i + k) % 4] for i in range(4)])

    def element_sum(self, value):
        value = value + self.cyc(value, 2)
        return value + self.cyc(value, 1)


def load(ref):
    return [[ref[c, x] for x in range(NX)] for c in range(ref.shape[0])]


def is_even():
    return [lax.axis_index(axis) % 2 == 0 for axis in ("gx_1", "gy", "gz_1")]


def pack(comps, outs):
    even = is_even()
    xo, zo, yo, yp, zp, xp = outs
    lane = lax.broadcasted_iota(jnp.int32, (NY, NZ), 1)
    first = jnp.zeros((NY, NZ), F32)
    last = jnp.zeros((NY, NZ), F32)
    for c, comp in enumerate(comps):
        xp[c] = jnp.where(even[0], comp[NX - 1], comp[0])
        xo[c] = jnp.where(even[0], comp[0], comp[NX - 1])
        for x in range(NX):
            low, high = (comp[x][0:1, :], comp[x][NY - 1 : NY, :])
            yp[c, pl.ds(x, 1), :] = jnp.where(even[1], high, low)
            yo[c, pl.ds(x, 1), :] = jnp.where(even[1], low, high)
            k = c * NX + x
            here = lane == k
            first = jnp.where(here, pltpu.roll(comp[x], k, 1) if k else comp[x], first)
            last = jnp.where(here, pltpu.roll(comp[x], k + 1, 1), last)
    zp[...] = jnp.where(even[2], last, first)
    zo[...] = jnp.where(even[2], first, last)


class Halo:
    def __init__(self, refs):
        self.even = is_even()
        self.refs = refs
        zo, zp = (refs[1][...], refs[4][...])
        self.zlo = jnp.where(self.even[2], zo, zp)
        self.zhi = jnp.where(self.even[2], zp, zo)

    def x_low(self, c):
        return jnp.where(self.even[0], self.refs[0][c], self.refs[5][c])

    def x_high(self, c):
        return jnp.where(self.even[0], self.refs[5][c], self.refs[0][c])

    def row(self, c, x, pair, other):
        line = jnp.where(self.even[1], self.refs[pair][c, pl.ds(x, 1), :], self.refs[other][c, pl.ds(x, 1), :])
        return jnp.broadcast_to(line, (NY, NZ))

    def low(self, dim, c, x):
        if dim == 0:
            return self.row(c, x, 2, 3)
        k = c * NX + x
        return pltpu.roll(self.zlo, (NZ - k) % NZ, 1) if k else self.zlo

    def high(self, dim, c, x):
        if dim == 0:
            return self.row(c, x, 3, 2)
        k = c * NX + x
        return pltpu.roll(self.zhi, NZ - 1 - k, 1)


def message_shapes(n):
    plane, rows, columns = (shape(n, NY, NZ), shape(n, NX, NZ), shape(NY, NZ))
    return [plane, columns, rows, rows, columns, plane]


def log_mean(left, right):
    total = left + right
    gap = right - left
    slope = gap / total
    ratio_sq = slope * slope
    is_close = ratio_sq < 0.0001
    series = 2.0 + ratio_sq * (2.0 / 3.0 + ratio_sq * (2.0 / 5.0 + ratio_sq * (2.0 / 7.0)))
    top = jnp.where(is_close, total, gap)
    low = jnp.where(is_close, series, jnp.log(right / left))
    return top / low


def two_point(left, right, d):
    rho_mean = log_mean(left[0], right[0])
    inv_mean = left[4] * right[4] / log_mean(left[0] * right[4], right[0] * left[4])
    vel = [0.5 * (left[1 + i] + right[1 + i]) for i in range(3)]
    product = left[1] * right[1] + left[2] * right[2] + left[3] * right[3]
    mass = rho_mean * vel[d]
    flux = [mass] + [mass * vel[i] for i in range(3)]
    flux[1 + d] = flux[1 + d] + 0.5 * (left[4] + right[4])
    energy = mass * (0.5 * product + inv_mean * (1.0 / (gamma_gas - 1.0))) + 0.5 * (
        left[4] * right[1 + d] + right[4] * left[1 + d]
    )
    return flux + [energy]


def primitive(u):
    inv = 1.0 / u[0]
    vel = [u[1 + i] * inv for i in range(3)]
    kinetic = u[1] * vel[0] + u[2] * vel[1] + u[3] * vel[2]
    pressure = (gamma_gas - 1.0) * (u[4] - 0.5 * kinetic)
    return (vel, pressure, jnp.sqrt(gamma_gas * pressure * inv))


def face_data(u, d, known=None):
    vel, pressure, sound = known or primitive(u)
    normal = vel[d]
    flux = [u[1 + d]] + [u[1 + i] * normal for i in range(3)] + [(u[4] + pressure) * normal]
    flux[1 + d] = flux[1 + d] + pressure
    return (u, flux, jnp.abs(normal) + sound)


def interface(left, right):
    speed = jnp.maximum(left[2], right[2])
    return [
        0.5 * ((left[1][c] + right[1][c]) - speed * (right[0][c] - left[0][c])) for c in range(5)
    ]


def volume_kernel(u_ref, vol_ref, alpha_ref, fast_ref):
    y, z = (Line(0), Line(1))
    u = load(u_ref)
    known = [primitive([u[c][x] for c in range(5)]) for x in range(NX)]
    nodes = [[u[0][x]] + known[x][0] + [known[x][1]] for x in range(NX)]
    speed = [
        jnp.abs(known[x][0][0]) + jnp.abs(known[x][0][1]) + jnp.abs(known[x][0][2]) + 3.0 * known[x][2]
        for x in range(NX)
    ]
    fast_ref[...] = jnp.maximum(jnp.maximum(speed[0], speed[1]), jnp.maximum(speed[2], speed[3]))

    product = [u[0][x] * known[x][1] for x in range(NX)]
    coeffs = [sum(float(MODAL[a, i]) * product[i] for i in range(4)) for a in range(4)]
    for line in (y, z):
        modal = [line.coef(MODAL, k) for k in range(4)]
        coeffs = [
            modal[0] * value + sum(modal[k] * line.cyc(value, k) for k in range(1, 4))
            for value in coeffs
        ]
    energy = [value * value for value in coeffs]
    total = (energy[0] + energy[1]) + (energy[2] + energy[3])
    low = (energy[0] + energy[1]) + energy[2]
    high = energy[3] + jnp.where(y.is3 | z.is3, low, 0.0)
    share = z.element_sum(y.element_sum(high)) / z.element_sum(y.element_sum(total))
    alpha = alpha_most / (1.0 + jnp.exp(-indicator_slope * (share - indicator_level)))
    alpha_ref[...] = alpha

    volume = [[None] * NX for _ in range(5)]
    for i in range(NX):
        for j in range(i + 1, NX):
            flux = two_point(nodes[i], nodes[j], 0)
            for c in range(5):
                for at, other in ((i, j), (j, i)):
                    term = (2.0 * DERIV[at, other]).astype(np.float32) * flux[c]
                    volume[c][at] = term if volume[c][at] is None else volume[c][at] + term
    for d, line in ((1, y), (2, z)):
        up, across, down = [line.coef(DERIV, k, 2.0) for k in (1, 2, 3)]
        for x in range(NX):
            near = two_point(nodes[x], [line.cyc(a, 1) for a in nodes[x]], d)
            far = two_point(nodes[x], [line.cyc(a, 2) for a in nodes[x]], d)
            for c in range(5):
                volume[c][x] = volume[c][x] + (
                    up * near[c] + down * line.cyc(near[c], 3) + across * far[c]
                )
    keep = 1.0 - alpha
    for c in range(5):
        for x in range(NX):
            vol_ref[c, x] = keep * volume[c][x]


def gravity_parts(field, halo, base, y, z):
    total = [[0.0] * NX for _ in range(4)]
    have = [c for c in range(4) if field[c] is not None]
    where = {c: base + i for i, c in enumerate(have)}

    for c, partner in ((0, 1), (1, 0)):
        if field[partner] is not None:
            for i in range(NX):
                terms = [float(2.0 * DERIV[i, j]) * field[partner][j] for j in range(NX) if DERIV[i, j] != 0.0]
                total[c][i] = total[c][i] + sum(terms[1:], terms[0])
    jumps = {}
    for c in have:
        jumps[c] = (halo.x_low(where[c]) - field[c][0], halo.x_high(where[c]) - field[c][NX - 1])
        for side, x in ((0, 0), (1, NX - 1)):
            total[c][x] = total[c][x] + 6.0 * jumps[c][side]
    for c, partner in ((0, 1), (1, 0)):
        if partner in jumps:
            total[c][0] = total[c][0] - 6.0 * jumps[partner][0]
            total[c][NX - 1] = total[c][NX - 1] + 6.0 * jumps[partner][1]
    for d, line in ((1, y), (2, z)):
        comp = 1 + d
        diag = line.coef(DERIV, 0, 2.0)
        coefs = [line.coef(DERIV, k, 2.0) for k in range(1, 4)]
        sign = line.by_node([-6.0, 0.0, 0.0, 6.0])
        for x in range(NX):
            for c, partner in ((0, comp), (comp, 0)):
                if field[partner] is not None:
                    value = field[partner][x]
                    term = diag * value
                    for k in range(1, 4):
                        term = term + coefs[k - 1] * line.cyc(value, k)
                    total[c][x] = total[c][x] + term
            gaps = {}
            for c in have:
                value = field[c][x]
                prev = jnp.where(line.lowest, halo.low(line.dim, where[c], x), line.roll(value, 1))
                after = jnp.where(line.highest, halo.high(line.dim, where[c], x), line.roll(value, -1))
                beside = jnp.where(line.is0, prev, jnp.where(line.is3, after, value))
                gaps[c] = beside - value
                total[c][x] = total[c][x] + 6.0 * gaps[c]
            for c, partner in ((0, comp), (comp, 0)):
                if partner in gaps:
                    total[c][x] = total[c][x] + sign * gaps[partner]
    return total


def advance(field, halo, base, y, z, source):
    total = gravity_parts(field, halo, base, y, z)
    phi_rate = [total[0][x] - coupling * source[x] for x in range(NX)]
    new = [[None] * NX for _ in range(4)]
    for x in range(NX):
        change = pseudo_step * phi_rate[x]
        new[0][x] = change if field[0] is None else field[0][x] + change
        for c in range(1, 4):
            if field[c] is None:
                new[c][x] = pseudo_step * total[c][x]
            else:
                new[c][x] = field[c][x] + pseudo_step * (total[c][x] - field[c][x])
    return (new, phi_rate)


def pack_kernel(u_ref, g_ref, u_out, g_out, *outs):
    u_out[...] = u_ref[...]
    g_out[...] = g_ref[...]
    pack(load(u_ref) + load(g_ref), outs)


def face_kernel(u_ref, g_ref, vol_ref, alpha_ref, *refs):
    halo = Halo(refs[:6])
    rate_ref, field_ref = refs[6:8]
    outs = refs[8:]
    y, z = (Line(0), Line(1))
    u = load(u_ref)
    g = load(g_ref)
    alpha = alpha_ref[...]
    keep = 1.0 - alpha
    known = [primitive([u[c][x] for c in range(5)]) for x in range(NX)]
    total = load(vol_ref)

    own = [face_data([u[c][x] for c in range(5)], 0, known[x]) for x in range(NX)]
    below = face_data([halo.x_low(c) for c in range(5)], 0)
    above = face_data([halo.x_high(c) for c in range(5)], 0)
    chain = [below] + own + [above]
    faces = [interface(chain[i], chain[i + 1]) for i in range(NX + 1)]
    for x in range(NX):
        inner = alpha * float(1.0 / WEIGHTS[x])
        edge = inner + keep * 6.0
        low_coef = edge if x == 0 else inner
        high_coef = edge if x == NX - 1 else inner
        for c in range(5):
            total[c][x] = total[c][x] + (high_coef * faces[x + 1][c] - low_coef * faces[x][c])
    for d, line in ((1, y), (2, z)):
        inner = alpha * line.by_node(1.0 / WEIGHTS)
        low_coef = inner + keep * line.by_node([6.0, 0.0, 0.0, 0.0])
        high_coef = inner + keep * line.by_node([0.0, 0.0, 0.0, 6.0])
        for x in range(NX):
            mine = face_data([u[c][x] for c in range(5)], d, known[x])
            prev = face_data(
                [
                    jnp.where(line.lowest, halo.low(line.dim, c, x), line.roll(u[c][x], 1))
                    for c in range(5)
                ],
                d,
            )
            after = face_data(
                [jnp.where(line.highest, halo.high(line.dim, c, x), u[c][x]) for c in range(5)], d
            )
            face = interface(prev, mine)
            end = interface(mine, after)
            for c in range(5):
                following = jnp.where(line.highest, end[c], line.roll(face[c], -1))
                total[c][x] = total[c][x] + (high_coef * following - low_coef * face[c])
    rate = [[-2.0 * total[c][x] for x in range(NX)] for c in range(5)]
    for x in range(NX):
        for i in range(3):
            rate[1 + i][x] = rate[1 + i][x] - u[0][x] * g[1 + i][x]
        rate[4][x] = rate[4][x] - (
            u[1][x] * g[1][x] + u[2][x] * g[2][x] + u[3][x] * g[3][x]
        )
        for c in range(5):
            rate_ref[c, x] = rate[c][x]

    source = [u[0][x] - rho_offset for x in range(NX)]
    new, _ = advance(g, halo, 5, y, z, source)
    slope = [(-pseudo_step * coupling) * rate[0][x] for x in range(NX)]
    comps = new + [slope]
    for c in range(5):
        for x in range(NX):
            field_ref[c, x] = comps[c][x]
    pack(comps, outs)


def middle_kernel(u_ref, rate_ref, field_ref, *refs):
    halo = Halo(refs[:6])
    next_ref = refs[6]
    outs = refs[7:]
    y, z = (Line(0), Line(1))
    field = load(field_ref)
    new, _ = advance(field[:4], halo, 0, y, z, [u_ref[0, x] - rho_offset for x in range(NX)])
    slope, _ = advance([field[4], None, None, None], halo, 4, y, z, [rate_ref[0, x] for x in range(NX)])
    comps = new + slope
    for c in range(8):
        for x in range(NX):
            next_ref[c, x] = comps[c][x]
    pack(comps, outs)


def last_kernel(u_ref, rate_ref, field_ref, fast_ref, *refs):
    halo = Halo(refs[:6])
    next_ref, stat_ref = refs[6:]
    y, z = (Line(0), Line(1))
    field = load(field_ref)
    source = [u_ref[0, x] - rho_offset for x in range(NX)]
    new, base_rate = advance(field[:4], halo, 0, y, z, source)
    slope, slope_rate = advance(field[4:], halo, 4, y, z, [rate_ref[0, x] for x in range(NX)])
    comps = new + slope
    for c in range(8):
        for x in range(NX):
            next_ref[c, x] = comps[c][x]
    weight = y.by_node(WEIGHTS) * z.by_node(WEIGHTS)

    def total(values):
        by_x = [float(WEIGHTS[x]) * values[x] for x in range(NX)]
        return jnp.sum(((by_x[0] + by_x[1]) + (by_x[2] + by_x[3])) * weight)

    stats = [
        jnp.max(fast_ref[...]),
        total([a * a for a in base_rate]),
        total([a * b for a, b in zip(base_rate, slope_rate)]),
        total([b * b for b in slope_rate]),
        total(base_rate),
        total(slope_rate),
        total(source),
    ]
    lane = lax.broadcasted_iota(jnp.int32, (1, NZ), 1)
    out = jnp.zeros((1, NZ), F32)
    for i, value in enumerate(stats):
        out = jnp.where(lane == i, value, out)
    stat_ref[...] = out


def finish_kernel(weight_total, u_ref, rate_ref, field_ref, stat_ref, grav_ref, source_ref, norm_ref):
    stat = stat_ref[...]
    part = [stat[:, i : i + 1] for i in range(7)]
    step = cfl_euler * elem_width / (7.0 * part[0])
    mean = part[6] * (1.0 / weight_total)
    shift = coupling * mean
    squares = (
        part[1]
        + step * (2.0 * part[2] + step * part[3])
        + shift * (2.0 * (part[4] + step * part[5]) + shift * weight_total)
    )
    norm_ref[...] = jnp.sqrt(jnp.maximum(squares, 0.0) * (1.0 / weight_total))
    raised = (ITERS * pseudo_step) * shift
    for x in range(NX):
        phi = field_ref[0, x] + step * field_ref[4, x] + raised
        grad = [field_ref[c, x] + step * field_ref[4 + c, x] for c in range(1, 4)]
        grav_ref[0, x] = phi
        for c in range(3):
            grav_ref[1 + c, x] = grad[c]
        rho = u_ref[0, x] + step * rate_ref[0, x]
        work = 0.0
        for c in range(3):
            source_ref[c, x] = -rho * grad[c]
            work = work + (u_ref[1 + c, x] + step * rate_ref[1 + c, x]) * grad[c]
        source_ref[3, x] = -work


def call(kernel, out_shape, flops, on_chip=True):
    def run(*args):
        if on_chip:
            args = [pltpu.with_memory_space_constraint(a, pltpu.VMEM) for a in args]
        return pl.pallas_call(
            kernel,
            in_specs=[pl.BlockSpec(memory_space=pltpu.VMEM)] * len(args),
            out_specs=[pl.BlockSpec(memory_space=pltpu.VMEM)] * len(out_shape),
            out_shape=out_shape,
            cost_estimate=pl.CostEstimate(flops=flops, bytes_accessed=400000, transcendentals=0),
        )(*args)

    return run


def pair_of(i, size):
    return i ^ 1


def other_of(i, size):
    return (i + 1 if i % 2 else i - 1) % size


ROUTES = (
    (GX, other_of),
    (GZ, other_of),
    ("gy", other_of),
    ("gy", pair_of),
    (GZ, pair_of),
    (GX, pair_of),
)


def exchange(messages):
    received = []
    for message, (axis, partner) in zip(messages, ROUTES):
        size = lax.axis_size(axis)
        received.append(lax.ppermute(message, axis, [(a, partner(a, size)) for a in range(size)]))
    return received


def gather(stat, axis):
    lane = lax.broadcasted_iota(jnp.int32, (1, NZ), 1)
    every = lax.all_gather(stat, axis, tiled=True)
    return jnp.where(
        lane == 0, jnp.max(every, axis=0, keepdims=True), jnp.sum(every, axis=0, keepdims=True)
    )


def spread(stat):
    names = ("gx_0", "gx_1", "gy", "gz_0", "gz_1")
    sizes = [lax.axis_size(name) for name in names]
    ring = sizes[0] * sizes[3]
    pairs = []
    for at in np.ndindex(*sizes):
        a, core, b, c, e = at
        place = (a * sizes[3] + c + core * sizes[4] + e - (sizes[3] // 2 - 1)) % ring
        to = (place // sizes[3], core, b, place % sizes[3], e)
        pairs.append(
            (int(np.ravel_multi_index(at, sizes)), int(np.ravel_multi_index(to, sizes)))
        )
    return lax.ppermute(stat, names, pairs)


def over_all(stat):
    for axis in ("gx_1", "gy", "gz_1"):
        stat = gather(stat, axis)
    stat = spread(stat)
    for axis in ("gx_1", "gz_1", "gx_0"):
        stat = gather(stat, axis)
    return stat


def shape(*dims):
    return pltpu.VMEM(dims, F32)


def local(u, g):
    weight_total = float(
        8.0
        * (u.shape[1] // 4 * lax.axis_size(GX))
        * (u.shape[2] // 4 * lax.axis_size("gy"))
        * (u.shape[3] // 4 * lax.axis_size(GZ))
    )
    full = (NX, NY, NZ)
    u, g, *messages = call(
        pack_kernel, [shape(5, *full), shape(4, *full)] + message_shapes(9), 10**5, False
    )(u, g)
    received = exchange(messages)
    vol, alpha, fast = call(
        volume_kernel, [shape(5, *full), shape(NY, NZ), shape(NY, NZ)], 10**7
    )(u)
    rate, field, *messages = call(
        face_kernel, [shape(5, *full), shape(5, *full)] + message_shapes(5), 10**6
    )(u, g, vol, alpha, *received)
    received = exchange(messages)
    field, *messages = call(middle_kernel, [shape(8, *full)] + message_shapes(8), 10**6)(
        u, rate, field, *received
    )
    received = exchange(messages)
    field, stat = call(last_kernel, [shape(8, *full), shape(1, NZ)], 10**6)(
        u, rate, field, fast, *received
    )
    stat = over_all(stat)
    gravity, gravity_source, norm = call(
        functools.partial(finish_kernel, weight_total),
        [jax.ShapeDtypeStruct((4, *full), F32)] * 2 + [jax.ShapeDtypeStruct((1, 1), F32)],
        10**5,
    )(u, rate, field, stat)
    return (rate, gravity, gravity_source, norm.reshape(()))


def solution(mesh):
    torus = Mesh(
        mesh.devices.reshape(4, 2, mesh.shape["gy"], 8, 4), ("gx_0", "gx_1", "gy", "gz_0", "gz_1")
    )
    placed = (P(None, GX, "gy", GZ), P(None, GX, "gy", GZ))
    return jax.shard_map(
        local,
        mesh=torus,
        in_specs=placed,
        out_specs=(P(None, GX, "gy", GZ), P(None, GX, "gy", GZ), P(None, GX, "gy", GZ), P()),
        check_vma=False,
    )
```

```python
import functools
import math

import jax
import jax.numpy as jnp
import numpy as np
from jax import lax
from jax.experimental import pallas as pl
from jax.experimental.pallas import tpu as pltpu
from jax.sharding import Mesh
from jax.sharding import PartitionSpec as P


ITERS = 3
GX = ("gx_0", "gx_1")
GZ = ("gz_0", "gz_1")

gamma_gas = 1.4
elem_width = 1.0
cfl_euler = 0.5
alpha_most = 0.5
indicator_level = 0.5 * 10.0 ** (-1.8 * 4.0**0.25)
indicator_slope = math.log((1.0 - 0.0001) / 0.0001) / indicator_level
coupling = 10.0
pseudo_step = 0.3 * elem_width / 7.0
rho_offset = 2.3

NX, NY, NZ = (4, 8, 128)
F32 = jnp.float32


def lgl_tables():
    points = np.array([-1.0, -1.0 / math.sqrt(5.0), 1.0 / math.sqrt(5.0), 1.0])
    weights = np.array([1.0, 5.0, 5.0, 1.0]) / 6.0
    barycentric = np.array(
        [1.0 / np.prod([points[a] - points[b] for b in range(4) if b != a]) for a in range(4)]
    )
    derivative = np.zeros((4, 4))
    for a in range(4):
        for b in range(4):
            if b != a:
                derivative[a, b] = barycentric[b] / barycentric[a] / (points[a] - points[b])
        derivative[a, a] = -np.sum(derivative[a])
    legendre = np.stack(
        [np.ones(4), points, 0.5 * (3.0 * points**2 - 1.0), 0.5 * (5.0 * points**3 - 3.0 * points)],
        axis=1,
    )
    legendre = legendre * np.sqrt((2.0 * np.arange(4) + 1.0) / 2.0)
    gram = np.sum(weights[:, None] * legendre * legendre, axis=0)
    modal_map = (legendre * weights[:, None]).T / gram[:, None]
    return (weights, derivative, modal_map)


WEIGHTS, DERIV, MODAL = lgl_tables()


class Line:
    def __init__(self, dim):
        self.dim = dim
        self.length = (NY, NZ)[dim]
        self.at = lax.broadcasted_iota(jnp.int32, (NY, NZ), dim)
        self.node = self.at % 4
        self.lowest = self.at == 0
        self.highest = self.at == self.length - 1
        self.is0 = self.node == 0
        self.is3 = self.node == 3

    def by_node(self, values):
        v = [float(item) for item in values]
        if v[1] == v[2] and v[0] == v[3]:
            return jnp.where(self.is0 | self.is3, v[0], v[1]).astype(F32)
        return jnp.where(
            self.node < 2,
            jnp.where(self.is0, v[0], v[1]),
            jnp.where(self.is3, v[3], v[2]),
        ).astype(F32)

    def roll(self, value, by):
        return pltpu.roll(value, by % self.length, self.dim)

    def cyc(self, value, k):
        return jnp.where(self.node < 4 - k, self.roll(value, -k), self.roll(value, 4 - k))

    def coef(self, matrix, k, scale=1.0):
        return self.by_node([scale * matrix[i, (i + k) % 4] for i in range(4)])

    def element_sum(self, value):
        value = value + self.cyc(value, 2)
        return value + self.cyc(value, 1)


def load(ref):
    return [[ref[c, x] for x in range(NX)] for c in range(ref.shape[0])]


def is_even():
    return [lax.axis_index(axis) % 2 == 0 for axis in ("gx_1", "gy", "gz_1")]


def pack_x(comps, other, pair):
    even = is_even()[0]
    for c, comp in enumerate(comps):
        other[c] = jnp.where(even, comp[0], comp[NX - 1])
        pair[c] = jnp.where(even, comp[NX - 1], comp[0])


def pack_y(comps, other, pair):
    even = is_even()[1]
    for c, comp in enumerate(comps):
        for x, tile in enumerate(comp):
            low, high = (tile[0:1, :], tile[NY - 1 : NY, :])
            other[c, pl.ds(x, 1), :] = jnp.where(even, low, high)
            pair[c, pl.ds(x, 1), :] = jnp.where(even, high, low)


def pack_z(tiles, other, pair):
    even = is_even()[2]
    lane = lax.broadcasted_iota(jnp.int32, (NY, NZ), 1)
    first = jnp.zeros((NY, NZ), F32)
    last = jnp.zeros((NY, NZ), F32)
    for k, tile in enumerate(tiles):
        here = lane == k
        first = jnp.where(here, pltpu.roll(tile, k, 1) if k else tile, first)
        last = jnp.where(here, pltpu.roll(tile, k + 1, 1), last)
    other[...] = jnp.where(even, first, last)
    pair[...] = jnp.where(even, last, first)


def flat(comps):
    return [tile for comp in comps for tile in comp]


class Halo:
    def __init__(self, refs):
        self.even = is_even()
        self.refs = refs
        zo, zp = (refs[1][...], refs[4][...])
        self.zlo = jnp.where(self.even[2], zo, zp)
        self.zhi = jnp.where(self.even[2], zp, zo)

    def x_low(self, c):
        return jnp.where(self.even[0], self.refs[0][c], self.refs[5][c])

    def x_high(self, c):
        return jnp.where(self.even[0], self.refs[5][c], self.refs[0][c])

    def row(self, c, x, pair, other):
        line = jnp.where(self.even[1], self.refs[pair][c, pl.ds(x, 1), :], self.refs[other][c, pl.ds(x, 1), :])
        return jnp.broadcast_to(line, (NY, NZ))

    def low(self, dim, c, x):
        if dim == 0:
            return self.row(c, x, 2, 3)
        k = c * NX + x
        return pltpu.roll(self.zlo, (NZ - k) % NZ, 1) if k else self.zlo

    def high(self, dim, c, x):
        if dim == 0:
            return self.row(c, x, 3, 2)
        k = c * NX + x
        return pltpu.roll(self.zhi, NZ - 1 - k, 1)


def log_mean(left, right):
    total = left + right
    gap = right - left
    slope = gap / total
    ratio_sq = slope * slope
    is_close = ratio_sq < 0.0001
    series = 2.0 + ratio_sq * (2.0 / 3.0 + ratio_sq * (2.0 / 5.0 + ratio_sq * (2.0 / 7.0)))
    top = jnp.where(is_close, total, gap)
    low = jnp.where(is_close, series, jnp.log(right / left))
    return top / low


def two_point(left, right, d):
    rho_mean = log_mean(left[0], right[0])
    inv_mean = left[4] * right[4] / log_mean(left[0] * right[4], right[0] * left[4])
    vel = [0.5 * (left[1 + i] + right[1 + i]) for i in range(3)]
    product = left[1] * right[1] + left[2] * right[2] + left[3] * right[3]
    mass = rho_mean * vel[d]
    flux = [mass] + [mass * vel[i] for i in range(3)]
    flux[1 + d] = flux[1 + d] + 0.5 * (left[4] + right[4])
    energy = mass * (0.5 * product + inv_mean * (1.0 / (gamma_gas - 1.0))) + 0.5 * (
        left[4] * right[1 + d] + right[4] * left[1 + d]
    )
    return flux + [energy]


def primitive(u):
    inv = 1.0 / u[0]
    vel = [u[1 + i] * inv for i in range(3)]
    kinetic = u[1] * vel[0] + u[2] * vel[1] + u[3] * vel[2]
    pressure = (gamma_gas - 1.0) * (u[4] - 0.5 * kinetic)
    return (vel, pressure, jnp.sqrt(gamma_gas * pressure * inv))


def face_data(u, d, known=None):
    vel, pressure, sound = known or primitive(u)
    normal = vel[d]
    flux = [u[1 + d]] + [u[1 + i] * normal for i in range(3)] + [(u[4] + pressure) * normal]
    flux[1 + d] = flux[1 + d] + pressure
    return (u, flux, jnp.abs(normal) + sound)


def interface(left, right):
    speed = jnp.maximum(left[2], right[2])
    return [
        0.5 * ((left[1][c] + right[1][c]) - speed * (right[0][c] - left[0][c])) for c in range(5)
    ]


def volume_kernel(u_ref, vol_ref, alpha_ref, fast_ref):
    y, z = (Line(0), Line(1))
    u = load(u_ref)
    known = [primitive([u[c][x] for c in range(5)]) for x in range(NX)]
    nodes = [[u[0][x]] + known[x][0] + [known[x][1]] for x in range(NX)]
    speed = [
        jnp.abs(known[x][0][0]) + jnp.abs(known[x][0][1]) + jnp.abs(known[x][0][2]) + 3.0 * known[x][2]
        for x in range(NX)
    ]
    fast_ref[...] = jnp.maximum(jnp.maximum(speed[0], speed[1]), jnp.maximum(speed[2], speed[3]))

    product = [u[0][x] * known[x][1] for x in range(NX)]
    coeffs = [sum(float(MODAL[a, i]) * product[i] for i in range(4)) for a in range(4)]
    for line in (y, z):
        modal = [line.coef(MODAL, k) for k in range(4)]
        coeffs = [
            modal[0] * value + sum(modal[k] * line.cyc(value, k) for k in range(1, 4))
            for value in coeffs
        ]
    energy = [value * value for value in coeffs]
    total = (energy[0] + energy[1]) + (energy[2] + energy[3])
    low = (energy[0] + energy[1]) + energy[2]
    high = energy[3] + jnp.where(y.is3 | z.is3, low, 0.0)
    share = z.element_sum(y.element_sum(high)) / z.element_sum(y.element_sum(total))
    alpha = alpha_most / (1.0 + jnp.exp(-indicator_slope * (share - indicator_level)))
    alpha_ref[...] = alpha

    volume = [[None] * NX for _ in range(5)]
    for i in range(NX):
        for j in range(i + 1, NX):
            flux = two_point(nodes[i], nodes[j], 0)
            for c in range(5):
                for at, other in ((i, j), (j, i)):
                    term = (2.0 * DERIV[at, other]).astype(np.float32) * flux[c]
                    volume[c][at] = term if volume[c][at] is None else volume[c][at] + term
    for d, line in ((1, y), (2, z)):
        up, across, down = [line.coef(DERIV, k, 2.0) for k in (1, 2, 3)]
        for x in range(NX):
            near = two_point(nodes[x], [line.cyc(a, 1) for a in nodes[x]], d)
            far = two_point(nodes[x], [line.cyc(a, 2) for a in nodes[x]], d)
            for c in range(5):
                volume[c][x] = volume[c][x] + (
                    up * near[c] + down * line.cyc(near[c], 3) + across * far[c]
                )
    keep = 1.0 - alpha
    for c in range(5):
        for x in range(NX):
            vol_ref[c, x] = keep * volume[c][x]


def gravity_parts(field, halo, base, y, z):
    total = [[0.0] * NX for _ in range(4)]
    have = [c for c in range(4) if field[c] is not None]
    where = {c: base + i for i, c in enumerate(have)}

    for c, partner in ((0, 1), (1, 0)):
        if field[partner] is not None:
            for i in range(NX):
                terms = [float(2.0 * DERIV[i, j]) * field[partner][j] for j in range(NX) if DERIV[i, j] != 0.0]
                total[c][i] = total[c][i] + sum(terms[1:], terms[0])
    jumps = {}
    for c in have if halo is not None else ():
        jumps[c] = (halo.x_low(where[c]) - field[c][0], halo.x_high(where[c]) - field[c][NX - 1])
        for side, x in ((0, 0), (1, NX - 1)):
            total[c][x] = total[c][x] + 6.0 * jumps[c][side]
    for c, partner in ((0, 1), (1, 0)):
        if partner in jumps:
            total[c][0] = total[c][0] - 6.0 * jumps[partner][0]
            total[c][NX - 1] = total[c][NX - 1] + 6.0 * jumps[partner][1]
    for d, line in ((1, y), (2, z)):
        comp = 1 + d
        diag = line.coef(DERIV, 0, 2.0)
        coefs = [line.coef(DERIV, k, 2.0) for k in range(1, 4)]
        sign = line.by_node([-6.0, 0.0, 0.0, 6.0])
        for x in range(NX):
            for c, partner in ((0, comp), (comp, 0)):
                if field[partner] is not None:
                    value = field[partner][x]
                    term = diag * value
                    for k in range(1, 4):
                        term = term + coefs[k - 1] * line.cyc(value, k)
                    total[c][x] = total[c][x] + term
            gaps = {}
            for c in have:
                value = field[c][x]
                low, high = (value, value)
                if halo is not None:
                    low = halo.low(line.dim, where[c], x)
                    high = halo.high(line.dim, where[c], x)
                prev = jnp.where(line.lowest, low, line.roll(value, 1))
                after = jnp.where(line.highest, high, line.roll(value, -1))
                beside = jnp.where(line.is0, prev, jnp.where(line.is3, after, value))
                gaps[c] = beside - value
                total[c][x] = total[c][x] + 6.0 * gaps[c]
            for c, partner in ((0, comp), (comp, 0)):
                if partner in gaps:
                    total[c][x] = total[c][x] + sign * gaps[partner]
    return total


def advance(field, halo, base, y, z, source):
    total = gravity_parts(field, halo, base, y, z)
    phi_rate = [total[0][x] - coupling * source[x] for x in range(NX)]
    new = [[None] * NX for _ in range(4)]
    for x in range(NX):
        change = pseudo_step * phi_rate[x]
        new[0][x] = change if field[0] is None else field[0][x] + change
        for c in range(1, 4):
            if field[c] is None:
                new[c][x] = pseudo_step * total[c][x]
            else:
                new[c][x] = field[c][x] + pseudo_step * (total[c][x] - field[c][x])
    return (new, phi_rate)


def pack_kernel(u_ref, g_ref, u_out, g_out, *outs):
    u_out[...] = u_ref[...]
    g_out[...] = g_ref[...]
    comps = load(u_ref) + load(g_ref)
    xo, zo, yo, yp, zp, xp = outs
    pack_x(comps, xo, xp)
    pack_y(comps, yo, yp)
    pack_z(flat(comps), zo, zp)


def face_kernel(u_ref, g_ref, vol_ref, alpha_ref, *refs):
    halo = Halo(refs[:6])
    rate_ref, f1_ref, f2_ref, xo, yo, yp, xp = refs[6:]
    y, z = (Line(0), Line(1))
    u = load(u_ref)
    g = load(g_ref)
    alpha = alpha_ref[...]
    keep = 1.0 - alpha
    known = [primitive([u[c][x] for c in range(5)]) for x in range(NX)]
    total = load(vol_ref)

    own = [face_data([u[c][x] for c in range(5)], 0, known[x]) for x in range(NX)]
    below = face_data([halo.x_low(c) for c in range(5)], 0)
    above = face_data([halo.x_high(c) for c in range(5)], 0)
    chain = [below] + own + [above]
    faces = [interface(chain[i], chain[i + 1]) for i in range(NX + 1)]
    for x in range(NX):
        inner = alpha * float(1.0 / WEIGHTS[x])
        edge = inner + keep * 6.0
        low_coef = edge if x == 0 else inner
        high_coef = edge if x == NX - 1 else inner
        for c in range(5):
            total[c][x] = total[c][x] + (high_coef * faces[x + 1][c] - low_coef * faces[x][c])
    for d, line in ((1, y), (2, z)):
        inner = alpha * line.by_node(1.0 / WEIGHTS)
        low_coef = inner + keep * line.by_node([6.0, 0.0, 0.0, 0.0])
        high_coef = inner + keep * line.by_node([0.0, 0.0, 0.0, 6.0])
        for x in range(NX):
            mine = face_data([u[c][x] for c in range(5)], d, known[x])
            prev = face_data(
                [
                    jnp.where(line.lowest, halo.low(line.dim, c, x), line.roll(u[c][x], 1))
                    for c in range(5)
                ],
                d,
            )
            after = face_data(
                [jnp.where(line.highest, halo.high(line.dim, c, x), u[c][x]) for c in range(5)], d
            )
            face = interface(prev, mine)
            end = interface(mine, after)
            for c in range(5):
                following = jnp.where(line.highest, end[c], line.roll(face[c], -1))
                total[c][x] = total[c][x] + (high_coef * following - low_coef * face[c])
    rate = [[-2.0 * total[c][x] for x in range(NX)] for c in range(5)]
    for x in range(NX):
        for i in range(3):
            rate[1 + i][x] = rate[1 + i][x] - u[0][x] * g[1 + i][x]
        rate[4][x] = rate[4][x] - (
            u[1][x] * g[1][x] + u[2][x] * g[2][x] + u[3][x] * g[3][x]
        )
        for c in range(5):
            rate_ref[c, x] = rate[c][x]

    source = [u[0][x] - rho_offset for x in range(NX)]
    new, _ = advance(g, halo, 5, y, z, source)
    slope = [(-pseudo_step * coupling) * rate[0][x] for x in range(NX)]
    partial, _ = advance(new, None, 0, y, z, source)
    partial_slope, _ = advance([slope, None, None, None], None, 0, y, z, rate[0])
    f1 = new + [slope]
    f2 = partial + partial_slope
    for x in range(NX):
        for c in range(5):
            f1_ref[c, x] = f1[c][x]
        for c in range(8):
            f2_ref[c, x] = f2[c][x]
    pack_x(f1 + f2, xo, xp)
    pack_y(f1 + f2, yo, yp)


def face_terms(gap, d, sign):
    terms = [None if value is None else 6.0 * value for value in gap]
    for c, partner in ((0, 1 + d), (1 + d, 0)):
        if gap[partner] is not None:
            extra = sign * gap[partner]
            terms[c] = extra if terms[c] is None else terms[c] + extra
    return terms


def meet(field, gap, d, sign):
    terms = face_terms(gap[:4], d, sign) + face_terms([gap[4], None, None, None], d, sign)
    return [
        value if term is None else value + pseudo_step * term for value, term in zip(field, terms)
    ]


def ends(line):
    outer = line.lowest | line.highest
    sign = jnp.where(line.lowest, -6.0, jnp.where(line.highest, 6.0, 0.0)).astype(F32)
    return (outer, sign)


def at(field, x, first, count):
    return [field[first + c][x] for c in range(count)]


def join_kernel(f1_ref, f2_ref, xo, yo, yp, xp, f2_out, side_ref, row_ref, zo, zp, eo, ep):
    even = is_even()
    y = Line(0)
    f1, f2 = (load(f1_ref), load(f2_ref))
    sides = []
    for low, x, sign in ((True, 0, -6.0), (False, NX - 1, 6.0)):
        near, away = (xo, xp) if low else (xp, xo)
        side = [jnp.where(even[0], near[c], away[c]) for c in range(13)]
        gap = [side[c] - f1[c][x] for c in range(5)]
        for c, value in enumerate(meet(at(f2, x, 0, 8), gap, 0, sign)):
            f2[c][x] = value
        side[5:] = meet(side[5:], [-value for value in gap], 0, -sign)
        sides.append(side)
    outer, sign = ends(y)
    rows = [[None] * NX for _ in range(13)]
    for x in range(NX):
        for c in range(13):
            other, pair = (yo[c, pl.ds(x, 1), :], yp[c, pl.ds(x, 1), :])
            low = jnp.broadcast_to(jnp.where(even[1], other, pair), (NY, NZ))
            high = jnp.broadcast_to(jnp.where(even[1], pair, other), (NY, NZ))
            rows[c][x] = jnp.where(y.lowest, low, jnp.where(y.highest, high, 0.0))
        gap = [jnp.where(outer, rows[c][x] - f1[c][x], 0.0) for c in range(5)]
        for c, value in enumerate(meet(at(f2, x, 0, 8), gap, 1, sign)):
            f2[c][x] = value
        for c, value in enumerate(meet(at(rows, x, 5, 8), [-v for v in gap], 1, -sign)):
            rows[5 + c][x] = value
    for x in range(NX):
        for c in range(8):
            f2_out[c, x] = f2[c][x]
        for c in range(13):
            row_ref[c, x] = rows[c][x]
    for w, side in enumerate(sides):
        for c in range(13):
            side_ref[w, c] = side[c]
        for c in range(5):
            low, high = (side[c][0:1, :], side[c][NY - 1 : NY, :])
            eo[pl.ds(5 * w + c, 1), :] = jnp.where(even[1], low, high)
            ep[pl.ds(5 * w + c, 1), :] = jnp.where(even[1], high, low)
    pack_z(flat(f1 + f2) + sides[0][:5] + sides[1][:5] + flat(rows[:5]), zo, zp)


class Around:
    def __init__(self, sides, rows, columns):
        self.sides, self.rows, self.columns = (sides, rows, columns)

    def x_low(self, c):
        return self.sides[0][c]

    def x_high(self, c):
        return self.sides[1][c]

    def low(self, dim, c, x):
        return (self.rows, self.columns)[dim][c][x]

    high = low


def last_kernel(
    u_ref, rate_ref, fast_ref, f1_ref, f2_ref, side_ref, row_ref, zo, zp, eo, ep, next_ref, stat_ref
):
    even = is_even()
    y, z = (Line(0), Line(1))
    f1, f2, rows = (load(f1_ref), load(f2_ref), load(row_ref))
    sides = [[side_ref[w, c] for c in range(13)] for w in range(2)]
    z_other, z_pair = (zo[...], zp[...])
    z_low = jnp.where(even[2], z_other, z_pair)
    z_high = jnp.where(even[2], z_pair, z_other)
    z_outer, z_sign = ends(z)
    y_outer, y_sign = ends(y)

    def column(k):
        low = pltpu.roll(z_low, (NZ - k) % NZ, 1) if k else z_low
        return jnp.where(z.lowest, low, pltpu.roll(z_high, NZ - 1 - k, 1))

    def gaps(outer, beside, own):
        return [jnp.where(outer, b - o, 0.0) for b, o in zip(beside, own)]

    columns = [[column(c * NX + x) for x in range(NX)] for c in range(13)]
    for x in range(NX):
        gap = gaps(z_outer, at(columns, x, 0, 5), at(f1, x, 0, 5))
        for c, value in enumerate(meet(at(f2, x, 0, 8), gap, 2, z_sign)):
            f2[c][x] = value
        for c, value in enumerate(meet(at(columns, x, 5, 8), [-v for v in gap], 2, -z_sign)):
            columns[5 + c][x] = value
    for w, x, sign in ((0, 0, -6.0), (1, NX - 1, 6.0)):
        corner = []
        for c in range(5):
            other, pair = (eo[pl.ds(5 * w + c, 1), :], ep[pl.ds(5 * w + c, 1), :])
            low = jnp.broadcast_to(jnp.where(even[1], other, pair), (NY, NZ))
            high = jnp.broadcast_to(jnp.where(even[1], pair, other), (NY, NZ))
            corner.append(jnp.where(y.lowest, low, high))
        side = sides[w]
        beside = [column(13 * NX + 5 * w + c) for c in range(5)]
        side[5:] = meet(side[5:], gaps(z_outer, beside, side[:5]), 2, z_sign)
        side[5:] = meet(side[5:], gaps(y_outer, corner, side[:5]), 1, y_sign)
        gap = gaps(y_outer, corner, at(rows, x, 0, 5))
        for c, value in enumerate(meet(at(rows, x, 5, 8), gap, 0, sign)):
            rows[5 + c][x] = value
    for x in range(NX):
        beside = [column(13 * NX + 10 + c * NX + x) for c in range(5)]
        gap = gaps(z_outer & y_outer, beside, at(rows, x, 0, 5))
        for c, value in enumerate(meet(at(rows, x, 5, 8), gap, 2, z_sign)):
            rows[5 + c][x] = value

    around = Around([side[5:] for side in sides], rows[5:], columns[5:])
    source = [u_ref[0, x] - rho_offset for x in range(NX)]
    new, base_rate = advance(f2[:4], around, 0, y, z, source)
    slope, slope_rate = advance(f2[4:], around, 4, y, z, [rate_ref[0, x] for x in range(NX)])
    comps = new + slope
    for c in range(8):
        for x in range(NX):
            next_ref[c, x] = comps[c][x]
    weight = y.by_node(WEIGHTS) * z.by_node(WEIGHTS)

    def total(values):
        by_x = [float(WEIGHTS[x]) * values[x] for x in range(NX)]
        return jnp.sum(((by_x[0] + by_x[1]) + (by_x[2] + by_x[3])) * weight)

    stats = [
        jnp.max(fast_ref[...]),
        total([a * a for a in base_rate]),
        total([a * b for a, b in zip(base_rate, slope_rate)]),
        total([b * b for b in slope_rate]),
        total(base_rate),
        total(slope_rate),
        total(source),
    ]
    lane = lax.broadcasted_iota(jnp.int32, (1, NZ), 1)
    out = jnp.zeros((1, NZ), F32)
    for i, value in enumerate(stats):
        out = jnp.where(lane == i, value, out)
    stat_ref[...] = out


def finish_kernel(weight_total, u_ref, rate_ref, field_ref, stat_ref, grav_ref, source_ref, norm_ref):
    stat = stat_ref[...]
    part = [stat[:, i : i + 1] for i in range(7)]
    step = cfl_euler * elem_width / (7.0 * part[0])
    mean = part[6] * (1.0 / weight_total)
    shift = coupling * mean
    squares = (
        part[1]
        + step * (2.0 * part[2] + step * part[3])
        + shift * (2.0 * (part[4] + step * part[5]) + shift * weight_total)
    )
    norm_ref[...] = jnp.sqrt(jnp.maximum(squares, 0.0) * (1.0 / weight_total))
    raised = (ITERS * pseudo_step) * shift
    for x in range(NX):
        phi = field_ref[0, x] + step * field_ref[4, x] + raised
        grad = [field_ref[c, x] + step * field_ref[4 + c, x] for c in range(1, 4)]
        grav_ref[0, x] = phi
        for c in range(3):
            grav_ref[1 + c, x] = grad[c]
        rho = u_ref[0, x] + step * rate_ref[0, x]
        work = 0.0
        for c in range(3):
            source_ref[c, x] = -rho * grad[c]
            work = work + (u_ref[1 + c, x] + step * rate_ref[1 + c, x]) * grad[c]
        source_ref[3, x] = -work


def call(kernel, out_shape, flops, on_chip=True):
    def run(*args):
        if on_chip:
            args = [pltpu.with_memory_space_constraint(a, pltpu.VMEM) for a in args]
        return pl.pallas_call(
            kernel,
            in_specs=[pl.BlockSpec(memory_space=pltpu.VMEM)] * len(args),
            out_specs=[pl.BlockSpec(memory_space=pltpu.VMEM)] * len(out_shape),
            out_shape=out_shape,
            cost_estimate=pl.CostEstimate(flops=flops, bytes_accessed=400000, transcendentals=0),
        )(*args)

    return run


def pair_of(i, size):
    return i ^ 1


def other_of(i, size):
    return (i + 1 if i % 2 else i - 1) % size


ROUTES = {
    "state": (
        (GX, other_of),
        (GZ, other_of),
        ("gy", other_of),
        ("gy", pair_of),
        (GZ, pair_of),
        (GX, pair_of),
    ),
    "second": ((GX, other_of), ("gy", other_of), ("gy", pair_of), (GX, pair_of)),
    "third": ((GZ, other_of), (GZ, pair_of), ("gy", other_of), ("gy", pair_of)),
}


def exchange(messages, stage):
    received = []
    for message, (axis, partner) in zip(messages, ROUTES[stage]):
        size = lax.axis_size(axis)
        received.append(lax.ppermute(message, axis, [(a, partner(a, size)) for a in range(size)]))
    return received


def gather(stat, axis):
    lane = lax.broadcasted_iota(jnp.int32, (1, NZ), 1)
    every = lax.all_gather(stat, axis, tiled=True)
    return jnp.where(
        lane == 0, jnp.max(every, axis=0, keepdims=True), jnp.sum(every, axis=0, keepdims=True)
    )


def spread(stat):
    names = ("gx_0", "gx_1", "gy", "gz_0", "gz_1")
    sizes = [lax.axis_size(name) for name in names]
    ring = sizes[0] * sizes[3]
    pairs = []
    for at in np.ndindex(*sizes):
        a, core, b, c, e = at
        place = (a * sizes[3] + c + core * sizes[4] + e - (sizes[3] // 2 - 1)) % ring
        to = (place // sizes[3], core, b, place % sizes[3], e)
        pairs.append(
            (int(np.ravel_multi_index(at, sizes)), int(np.ravel_multi_index(to, sizes)))
        )
    return lax.ppermute(stat, names, pairs)


def over_all(stat):
    for axis in ("gx_1", "gy", "gz_1"):
        stat = gather(stat, axis)
    stat = spread(stat)
    for axis in ("gx_1", "gz_1", "gx_0"):
        stat = gather(stat, axis)
    return stat


def shape(*dims):
    return pltpu.VMEM(dims, F32)


def local(u, g):
    weight_total = float(
        8.0
        * (u.shape[1] // 4 * lax.axis_size(GX))
        * (u.shape[2] // 4 * lax.axis_size("gy"))
        * (u.shape[3] // 4 * lax.axis_size(GZ))
    )
    full = (NX, NY, NZ)
    tile = shape(NY, NZ)
    planes, rows = (shape(9, NY, NZ), shape(9, NX, NZ))
    u, g, *messages = call(
        pack_kernel,
        [shape(5, *full), shape(4, *full), planes, tile, rows, rows, tile, planes],
        10**5,
        False,
    )(u, g)
    received = exchange(messages, "state")
    vol, alpha, fast = call(volume_kernel, [shape(5, *full), tile, tile], 10**7)(u)
    planes, rows = (shape(13, NY, NZ), shape(13, NX, NZ))
    rate, f1, f2, *messages = call(
        face_kernel,
        [shape(5, *full), shape(5, *full), shape(8, *full), planes, rows, rows, planes],
        10**6,
    )(u, g, vol, alpha, *received)
    received = exchange(messages, "second")
    corners = shape(10, NZ)
    f2, sides, rows, *messages = call(
        join_kernel,
        [shape(8, *full), shape(2, 13, NY, NZ), shape(13, *full), tile, tile, corners, corners],
        10**6,
    )(f1, f2, *received)
    received = exchange(messages, "third")
    field, stat = call(last_kernel, [shape(8, *full), shape(1, NZ)], 10**6)(
        u, rate, fast, f1, f2, sides, rows, *received
    )
    stat = over_all(stat)
    gravity, gravity_source, norm = call(
        functools.partial(finish_kernel, weight_total),
        [jax.ShapeDtypeStruct((4, *full), F32)] * 2 + [jax.ShapeDtypeStruct((1, 1), F32)],
        10**5,
    )(u, rate, field, stat)
    return (rate, gravity, gravity_source, norm.reshape(()))


def solution(mesh):
    torus = Mesh(
        mesh.devices.reshape(4, 2, mesh.shape["gy"], 8, 4), ("gx_0", "gx_1", "gy", "gz_0", "gz_1")
    )
    placed = (P(None, GX, "gy", GZ), P(None, GX, "gy", GZ))
    return jax.shard_map(
        local,
        mesh=torus,
        in_specs=placed,
        out_specs=(P(None, GX, "gy", GZ), P(None, GX, "gy", GZ), P(None, GX, "gy", GZ), P()),
        check_vma=False,
    )
```

```python
import functools
import math

import jax
import jax.numpy as jnp
import numpy as np
from jax import lax
from jax.experimental import pallas as pl
from jax.experimental.pallas import tpu as pltpu
from jax.sharding import Mesh
from jax.sharding import PartitionSpec as P


ITERS = 3
GX = ("gx_0", "gx_1")
GZ = ("gz_0", "gz_1")

gamma_gas = 1.4
elem_width = 1.0
cfl_euler = 0.5
alpha_most = 0.5
indicator_level = 0.5 * 10.0 ** (-1.8 * 4.0**0.25)
indicator_slope = math.log((1.0 - 0.0001) / 0.0001) / indicator_level
coupling = 10.0
pseudo_step = 0.3 * elem_width / 7.0
rho_offset = 2.3

NX, NY, NZ = (4, 8, 128)
F32 = jnp.float32


def lgl_tables():
    points = np.array([-1.0, -1.0 / math.sqrt(5.0), 1.0 / math.sqrt(5.0), 1.0])
    weights = np.array([1.0, 5.0, 5.0, 1.0]) / 6.0
    barycentric = np.array(
        [1.0 / np.prod([points[a] - points[b] for b in range(4) if b != a]) for a in range(4)]
    )
    derivative = np.zeros((4, 4))
    for a in range(4):
        for b in range(4):
            if b != a:
                derivative[a, b] = barycentric[b] / barycentric[a] / (points[a] - points[b])
        derivative[a, a] = -np.sum(derivative[a])
    legendre = np.stack(
        [np.ones(4), points, 0.5 * (3.0 * points**2 - 1.0), 0.5 * (5.0 * points**3 - 3.0 * points)],
        axis=1,
    )
    legendre = legendre * np.sqrt((2.0 * np.arange(4) + 1.0) / 2.0)
    gram = np.sum(weights[:, None] * legendre * legendre, axis=0)
    modal_map = (legendre * weights[:, None]).T / gram[:, None]
    return (weights, derivative, modal_map)


WEIGHTS, DERIV, MODAL = lgl_tables()


class Line:
    def __init__(self, dim):
        self.dim = dim
        self.length = (NY, NZ)[dim]
        self.at = lax.broadcasted_iota(jnp.int32, (NY, NZ), dim)
        self.node = self.at % 4
        self.lowest = self.at == 0
        self.highest = self.at == self.length - 1
        self.is0 = self.node == 0
        self.is3 = self.node == 3

    def by_node(self, values):
        v = [float(item) for item in values]
        if v[1] == v[2] and v[0] == v[3]:
            return jnp.where(self.is0 | self.is3, v[0], v[1]).astype(F32)
        return jnp.where(
            self.node < 2,
            jnp.where(self.is0, v[0], v[1]),
            jnp.where(self.is3, v[3], v[2]),
        ).astype(F32)

    def roll(self, value, by):
        return pltpu.roll(value, by % self.length, self.dim)

    def cyc(self, value, k):
        return jnp.where(self.node < 4 - k, self.roll(value, -k), self.roll(value, 4 - k))

    def coef(self, matrix, k, scale=1.0):
        return self.by_node([scale * matrix[i, (i + k) % 4] for i in range(4)])

    def element_sum(self, value):
        value = value + self.cyc(value, 2)
        return value + self.cyc(value, 1)


def load(ref):
    return [[ref[c, x] for x in range(NX)] for c in range(ref.shape[0])]


def is_even():
    return [lax.axis_index(axis) % 2 == 0 for axis in ("gx_1", "gy", "gz_1")]


def pack_x(comps, other, pair):
    even = is_even()[0]
    for c, comp in enumerate(comps):
        other[c] = jnp.where(even, comp[0], comp[NX - 1])
        pair[c] = jnp.where(even, comp[NX - 1], comp[0])


def pack_y(comps, other, pair):
    even = is_even()[1]
    for c, comp in enumerate(comps):
        for x, tile in enumerate(comp):
            low, high = (tile[0:1, :], tile[NY - 1 : NY, :])
            other[c, pl.ds(x, 1), :] = jnp.where(even, low, high)
            pair[c, pl.ds(x, 1), :] = jnp.where(even, high, low)


def pack_z(tiles, other, pair):
    even = is_even()[2]
    lane = lax.broadcasted_iota(jnp.int32, (NY, NZ), 1)
    first = jnp.zeros((NY, NZ), F32)
    last = jnp.zeros((NY, NZ), F32)
    for k, tile in enumerate(tiles):
        here = lane == k
        first = jnp.where(here, pltpu.roll(tile, k, 1) if k else tile, first)
        last = jnp.where(here, pltpu.roll(tile, k + 1, 1), last)
    other[...] = jnp.where(even, first, last)
    pair[...] = jnp.where(even, last, first)


def flat(comps):
    return [tile for comp in comps for tile in comp]


class Halo:
    def __init__(self, refs):
        self.even = is_even()
        self.refs = refs
        zo, zp = (refs[1][...], refs[4][...])
        self.zlo = jnp.where(self.even[2], zo, zp)
        self.zhi = jnp.where(self.even[2], zp, zo)

    def x_low(self, c):
        return jnp.where(self.even[0], self.refs[0][c], self.refs[5][c])

    def x_high(self, c):
        return jnp.where(self.even[0], self.refs[5][c], self.refs[0][c])

    def row(self, c, x, pair, other):
        line = jnp.where(self.even[1], self.refs[pair][c, pl.ds(x, 1), :], self.refs[other][c, pl.ds(x, 1), :])
        return jnp.broadcast_to(line, (NY, NZ))

    def low(self, dim, c, x):
        if dim == 0:
            return self.row(c, x, 2, 3)
        k = c * NX + x
        return pltpu.roll(self.zlo, (NZ - k) % NZ, 1) if k else self.zlo

    def high(self, dim, c, x):
        if dim == 0:
            return self.row(c, x, 3, 2)
        k = c * NX + x
        return pltpu.roll(self.zhi, NZ - 1 - k, 1)


def log_mean(left, right):
    total = left + right
    gap = right - left
    slope = gap / total
    ratio_sq = slope * slope
    is_close = ratio_sq < 0.0001
    series = 2.0 + ratio_sq * (2.0 / 3.0 + ratio_sq * (2.0 / 5.0 + ratio_sq * (2.0 / 7.0)))
    top = jnp.where(is_close, total, gap)
    low = jnp.where(is_close, series, jnp.log(right / left))
    return top / low


def two_point(left, right, d):
    rho_mean = log_mean(left[0], right[0])
    inv_mean = left[4] * right[4] / log_mean(left[0] * right[4], right[0] * left[4])
    vel = [0.5 * (left[1 + i] + right[1 + i]) for i in range(3)]
    product = left[1] * right[1] + left[2] * right[2] + left[3] * right[3]
    mass = rho_mean * vel[d]
    flux = [mass] + [mass * vel[i] for i in range(3)]
    flux[1 + d] = flux[1 + d] + 0.5 * (left[4] + right[4])
    energy = mass * (0.5 * product + inv_mean * (1.0 / (gamma_gas - 1.0))) + 0.5 * (
        left[4] * right[1 + d] + right[4] * left[1 + d]
    )
    return flux + [energy]


def primitive(u):
    inv = 1.0 / u[0]
    vel = [u[1 + i] * inv for i in range(3)]
    kinetic = u[1] * vel[0] + u[2] * vel[1] + u[3] * vel[2]
    pressure = (gamma_gas - 1.0) * (u[4] - 0.5 * kinetic)
    return (vel, pressure, jnp.sqrt(gamma_gas * pressure * inv))


def face_data(u, d, known=None):
    vel, pressure, sound = known or primitive(u)
    normal = vel[d]
    flux = [u[1 + d]] + [u[1 + i] * normal for i in range(3)] + [(u[4] + pressure) * normal]
    flux[1 + d] = flux[1 + d] + pressure
    return (u, flux, jnp.abs(normal) + sound)


def interface(left, right):
    speed = jnp.maximum(left[2], right[2])
    return [
        0.5 * ((left[1][c] + right[1][c]) - speed * (right[0][c] - left[0][c])) for c in range(5)
    ]


def volume_kernel(u_ref, vol_ref, alpha_ref, fast_ref):
    y, z = (Line(0), Line(1))
    u = load(u_ref)
    known = [primitive([u[c][x] for c in range(5)]) for x in range(NX)]
    nodes = [[u[0][x]] + known[x][0] + [known[x][1]] for x in range(NX)]
    speed = [
        jnp.abs(known[x][0][0]) + jnp.abs(known[x][0][1]) + jnp.abs(known[x][0][2]) + 3.0 * known[x][2]
        for x in range(NX)
    ]
    fast_ref[...] = jnp.maximum(jnp.maximum(speed[0], speed[1]), jnp.maximum(speed[2], speed[3]))

    product = [u[0][x] * known[x][1] for x in range(NX)]
    coeffs = [sum(float(MODAL[a, i]) * product[i] for i in range(4)) for a in range(4)]
    for line in (y, z):
        modal = [line.coef(MODAL, k) for k in range(4)]
        coeffs = [
            modal[0] * value + sum(modal[k] * line.cyc(value, k) for k in range(1, 4))
            for value in coeffs
        ]
    energy = [value * value for value in coeffs]
    total = (energy[0] + energy[1]) + (energy[2] + energy[3])
    low = (energy[0] + energy[1]) + energy[2]
    high = energy[3] + jnp.where(y.is3 | z.is3, low, 0.0)
    share = z.element_sum(y.element_sum(high)) / z.element_sum(y.element_sum(total))
    alpha = alpha_most / (1.0 + jnp.exp(-indicator_slope * (share - indicator_level)))
    alpha_ref[...] = alpha

    volume = [[None] * NX for _ in range(5)]
    for i in range(NX):
        for j in range(i + 1, NX):
            flux = two_point(nodes[i], nodes[j], 0)
            for c in range(5):
                for at, other in ((i, j), (j, i)):
                    term = (2.0 * DERIV[at, other]).astype(np.float32) * flux[c]
                    volume[c][at] = term if volume[c][at] is None else volume[c][at] + term
    for d, line in ((1, y), (2, z)):
        up, across, down = [line.coef(DERIV, k, 2.0) for k in (1, 2, 3)]
        for x in range(NX):
            near = two_point(nodes[x], [line.cyc(a, 1) for a in nodes[x]], d)
            far = two_point(nodes[x], [line.cyc(a, 2) for a in nodes[x]], d)
            for c in range(5):
                volume[c][x] = volume[c][x] + (
                    up * near[c] + down * line.cyc(near[c], 3) + across * far[c]
                )
    keep = 1.0 - alpha
    for c in range(5):
        for x in range(NX):
            vol_ref[c, x] = keep * volume[c][x]


def gravity_parts(field, halo, base, y, z):
    total = [[0.0] * NX for _ in range(4)]
    have = [c for c in range(4) if field[c] is not None]
    where = {c: base + i for i, c in enumerate(have)}

    for c, partner in ((0, 1), (1, 0)):
        if field[partner] is not None:
            for i in range(NX):
                terms = [float(2.0 * DERIV[i, j]) * field[partner][j] for j in range(NX) if DERIV[i, j] != 0.0]
                total[c][i] = total[c][i] + sum(terms[1:], terms[0])
    jumps = {}
    for c in have if halo is not None else ():
        jumps[c] = (halo.x_low(where[c]) - field[c][0], halo.x_high(where[c]) - field[c][NX - 1])
        for side, x in ((0, 0), (1, NX - 1)):
            total[c][x] = total[c][x] + 6.0 * jumps[c][side]
    for c, partner in ((0, 1), (1, 0)):
        if partner in jumps:
            total[c][0] = total[c][0] - 6.0 * jumps[partner][0]
            total[c][NX - 1] = total[c][NX - 1] + 6.0 * jumps[partner][1]
    for d, line in ((1, y), (2, z)):
        comp = 1 + d
        diag = line.coef(DERIV, 0, 2.0)
        coefs = [line.coef(DERIV, k, 2.0) for k in range(1, 4)]
        sign = line.by_node([-6.0, 0.0, 0.0, 6.0])
        for x in range(NX):
            for c, partner in ((0, comp), (comp, 0)):
                if field[partner] is not None:
                    value = field[partner][x]
                    term = diag * value
                    for k in range(1, 4):
                        term = term + coefs[k - 1] * line.cyc(value, k)
                    total[c][x] = total[c][x] + term
            gaps = {}
            for c in have:
                value = field[c][x]
                low, high = (value, value)
                if halo is not None:
                    low = halo.low(line.dim, where[c], x)
                    high = halo.high(line.dim, where[c], x)
                prev = jnp.where(line.lowest, low, line.roll(value, 1))
                after = jnp.where(line.highest, high, line.roll(value, -1))
                beside = jnp.where(line.is0, prev, jnp.where(line.is3, after, value))
                gaps[c] = beside - value
                total[c][x] = total[c][x] + 6.0 * gaps[c]
            for c, partner in ((0, comp), (comp, 0)):
                if partner in gaps:
                    total[c][x] = total[c][x] + sign * gaps[partner]
    return total


def advance(field, halo, base, y, z, source):
    total = gravity_parts(field, halo, base, y, z)
    phi_rate = [total[0][x] - coupling * source[x] for x in range(NX)]
    new = [[None] * NX for _ in range(4)]
    for x in range(NX):
        change = pseudo_step * phi_rate[x]
        new[0][x] = change if field[0] is None else field[0][x] + change
        for c in range(1, 4):
            if field[c] is None:
                new[c][x] = pseudo_step * total[c][x]
            else:
                new[c][x] = field[c][x] + pseudo_step * (total[c][x] - field[c][x])
    return (new, phi_rate)


def pack_kernel(u_ref, g_ref, u_out, g_out, *outs):
    u_out[...] = u_ref[...]
    g_out[...] = g_ref[...]
    comps = load(u_ref) + load(g_ref)
    xo, zo, yo, yp, zp, xp = outs
    pack_x(comps, xo, xp)
    pack_y(comps, yo, yp)
    pack_z(flat(comps), zo, zp)


def face_kernel(u_ref, g_ref, vol_ref, alpha_ref, *refs):
    halo = Halo(refs[:6])
    rate_ref, f1_ref, f2_ref, xo, yo, yp, xp = refs[6:]
    y, z = (Line(0), Line(1))
    u = load(u_ref)
    g = load(g_ref)
    alpha = alpha_ref[...]
    keep = 1.0 - alpha
    known = [primitive([u[c][x] for c in range(5)]) for x in range(NX)]
    total = load(vol_ref)

    own = [face_data([u[c][x] for c in range(5)], 0, known[x]) for x in range(NX)]
    below = face_data([halo.x_low(c) for c in range(5)], 0)
    above = face_data([halo.x_high(c) for c in range(5)], 0)
    chain = [below] + own + [above]
    faces = [interface(chain[i], chain[i + 1]) for i in range(NX + 1)]
    for x in range(NX):
        inner = alpha * float(1.0 / WEIGHTS[x])
        edge = inner + keep * 6.0
        low_coef = edge if x == 0 else inner
        high_coef = edge if x == NX - 1 else inner
        for c in range(5):
            total[c][x] = total[c][x] + (high_coef * faces[x + 1][c] - low_coef * faces[x][c])
    for d, line in ((1, y), (2, z)):
        inner = alpha * line.by_node(1.0 / WEIGHTS)
        low_coef = inner + keep * line.by_node([6.0, 0.0, 0.0, 0.0])
        high_coef = inner + keep * line.by_node([0.0, 0.0, 0.0, 6.0])
        for x in range(NX):
            mine = face_data([u[c][x] for c in range(5)], d, known[x])
            prev = face_data(
                [
                    jnp.where(line.lowest, halo.low(line.dim, c, x), line.roll(u[c][x], 1))
                    for c in range(5)
                ],
                d,
            )
            after = face_data(
                [jnp.where(line.highest, halo.high(line.dim, c, x), u[c][x]) for c in range(5)], d
            )
            face = interface(prev, mine)
            end = interface(mine, after)
            for c in range(5):
                following = jnp.where(line.highest, end[c], line.roll(face[c], -1))
                total[c][x] = total[c][x] + (high_coef * following - low_coef * face[c])
    rate = [[-2.0 * total[c][x] for x in range(NX)] for c in range(5)]
    for x in range(NX):
        for i in range(3):
            rate[1 + i][x] = rate[1 + i][x] - u[0][x] * g[1 + i][x]
        rate[4][x] = rate[4][x] - (
            u[1][x] * g[1][x] + u[2][x] * g[2][x] + u[3][x] * g[3][x]
        )
        for c in range(5):
            rate_ref[c, x] = rate[c][x]

    source = [u[0][x] - rho_offset for x in range(NX)]
    new, _ = advance(g, halo, 5, y, z, source)
    slope = [(-pseudo_step * coupling) * rate[0][x] for x in range(NX)]
    partial, _ = advance(new, None, 0, y, z, source)
    partial_slope, _ = advance([slope, None, None, None], None, 0, y, z, rate[0])
    f1 = new + [slope]
    f2 = partial + partial_slope
    for x in range(NX):
        for c in range(5):
            f1_ref[c, x] = f1[c][x]
        for c in range(8):
            f2_ref[c, x] = f2[c][x]
    pack_x(f1 + f2, xo, xp)
    pack_y(f1 + f2, yo, yp)


def face_terms(gap, d, sign):
    terms = [None if value is None else 6.0 * value for value in gap]
    for c, partner in ((0, 1 + d), (1 + d, 0)):
        if gap[partner] is not None:
            extra = sign * gap[partner]
            terms[c] = extra if terms[c] is None else terms[c] + extra
    return terms


def meet(field, gap, d, sign):
    terms = face_terms(gap[:4], d, sign) + face_terms([gap[4], None, None, None], d, sign)
    return [
        value if term is None else value + pseudo_step * term for value, term in zip(field, terms)
    ]


def ends(line):
    outer = line.lowest | line.highest
    sign = jnp.where(line.lowest, -6.0, jnp.where(line.highest, 6.0, 0.0)).astype(F32)
    return (outer, sign)


def at(field, x, first, count):
    return [field[first + c][x] for c in range(count)]


def join_kernel(f1_ref, f2_ref, xo, yo, yp, xp, f2_out, side_ref, row_ref, zo, eo, ep, zp):
    even = is_even()
    y = Line(0)
    f1, f2 = (load(f1_ref), load(f2_ref))
    sides = []
    for low, x, sign in ((True, 0, -6.0), (False, NX - 1, 6.0)):
        near, away = (xo, xp) if low else (xp, xo)
        side = [jnp.where(even[0], near[c], away[c]) for c in range(13)]
        gap = [side[c] - f1[c][x] for c in range(5)]
        for c, value in enumerate(meet(at(f2, x, 0, 8), gap, 0, sign)):
            f2[c][x] = value
        side[5:] = meet(side[5:], [-value for value in gap], 0, -sign)
        sides.append(side)
    outer, sign = ends(y)
    rows = [[None] * NX for _ in range(13)]
    for x in range(NX):
        for c in range(13):
            other, pair = (yo[c, pl.ds(x, 1), :], yp[c, pl.ds(x, 1), :])
            low = jnp.broadcast_to(jnp.where(even[1], other, pair), (NY, NZ))
            high = jnp.broadcast_to(jnp.where(even[1], pair, other), (NY, NZ))
            rows[c][x] = jnp.where(y.lowest, low, jnp.where(y.highest, high, 0.0))
        gap = [jnp.where(outer, rows[c][x] - f1[c][x], 0.0) for c in range(5)]
        for c, value in enumerate(meet(at(f2, x, 0, 8), gap, 1, sign)):
            f2[c][x] = value
        for c, value in enumerate(meet(at(rows, x, 5, 8), [-v for v in gap], 1, -sign)):
            rows[5 + c][x] = value
    for x in range(NX):
        for c in range(8):
            f2_out[c, x] = f2[c][x]
        for c in range(13):
            row_ref[c, x] = rows[c][x]
    for w, side in enumerate(sides):
        for c in range(13):
            side_ref[w, c] = side[c]
        for c in range(5):
            low, high = (side[c][0:1, :], side[c][NY - 1 : NY, :])
            eo[pl.ds(5 * w + c, 1), :] = jnp.where(even[1], low, high)
            ep[pl.ds(5 * w + c, 1), :] = jnp.where(even[1], high, low)
    pack_z(flat(f1 + f2) + sides[0][:5] + sides[1][:5] + flat(rows[:5]), zo, zp)


class Around:
    def __init__(self, sides, rows, columns):
        self.sides, self.rows, self.columns = (sides, rows, columns)

    def x_low(self, c):
        return self.sides[0][c]

    def x_high(self, c):
        return self.sides[1][c]

    def low(self, dim, c, x):
        return (self.rows, self.columns)[dim][c][x]

    high = low


def last_kernel(
    u_ref, rate_ref, fast_ref, f1_ref, f2_ref, side_ref, row_ref, zo, eo, ep, zp, next_ref, stat_ref
):
    even = is_even()
    y, z = (Line(0), Line(1))
    f1, f2, rows = (load(f1_ref), load(f2_ref), load(row_ref))
    sides = [[side_ref[w, c] for c in range(13)] for w in range(2)]
    z_other, z_pair = (zo[...], zp[...])
    z_low = jnp.where(even[2], z_other, z_pair)
    z_high = jnp.where(even[2], z_pair, z_other)
    z_outer, z_sign = ends(z)
    y_outer, y_sign = ends(y)

    def column(k):
        low = pltpu.roll(z_low, (NZ - k) % NZ, 1) if k else z_low
        return jnp.where(z.lowest, low, pltpu.roll(z_high, NZ - 1 - k, 1))

    def gaps(outer, beside, own):
        return [jnp.where(outer, b - o, 0.0) for b, o in zip(beside, own)]

    columns = [[column(c * NX + x) for x in range(NX)] for c in range(13)]
    for x in range(NX):
        gap = gaps(z_outer, at(columns, x, 0, 5), at(f1, x, 0, 5))
        for c, value in enumerate(meet(at(f2, x, 0, 8), gap, 2, z_sign)):
            f2[c][x] = value
        for c, value in enumerate(meet(at(columns, x, 5, 8), [-v for v in gap], 2, -z_sign)):
            columns[5 + c][x] = value
    for w, x, sign in ((0, 0, -6.0), (1, NX - 1, 6.0)):
        corner = []
        for c in range(5):
            other, pair = (eo[pl.ds(5 * w + c, 1), :], ep[pl.ds(5 * w + c, 1), :])
            low = jnp.broadcast_to(jnp.where(even[1], other, pair), (NY, NZ))
            high = jnp.broadcast_to(jnp.where(even[1], pair, other), (NY, NZ))
            corner.append(jnp.where(y.lowest, low, high))
        side = sides[w]
        beside = [column(13 * NX + 5 * w + c) for c in range(5)]
        side[5:] = meet(side[5:], gaps(z_outer, beside, side[:5]), 2, z_sign)
        side[5:] = meet(side[5:], gaps(y_outer, corner, side[:5]), 1, y_sign)
        gap = gaps(y_outer, corner, at(rows, x, 0, 5))
        for c, value in enumerate(meet(at(rows, x, 5, 8), gap, 0, sign)):
            rows[5 + c][x] = value
    for x in range(NX):
        beside = [column(13 * NX + 10 + c * NX + x) for c in range(5)]
        gap = gaps(z_outer & y_outer, beside, at(rows, x, 0, 5))
        for c, value in enumerate(meet(at(rows, x, 5, 8), gap, 2, z_sign)):
            rows[5 + c][x] = value

    around = Around([side[5:] for side in sides], rows[5:], columns[5:])
    source = [u_ref[0, x] - rho_offset for x in range(NX)]
    new, base_rate = advance(f2[:4], around, 0, y, z, source)
    slope, slope_rate = advance(f2[4:], around, 4, y, z, [rate_ref[0, x] for x in range(NX)])
    comps = new + slope
    for c in range(8):
        for x in range(NX):
            next_ref[c, x] = comps[c][x]
    weight = y.by_node(WEIGHTS) * z.by_node(WEIGHTS)

    def total(values):
        by_x = [float(WEIGHTS[x]) * values[x] for x in range(NX)]
        return jnp.sum(((by_x[0] + by_x[1]) + (by_x[2] + by_x[3])) * weight)

    stats = [
        jnp.max(fast_ref[...]),
        total([a * a for a in base_rate]),
        total([a * b for a, b in zip(base_rate, slope_rate)]),
        total([b * b for b in slope_rate]),
        total(base_rate),
        total(slope_rate),
        total(source),
    ]
    lane = lax.broadcasted_iota(jnp.int32, (1, NZ), 1)
    out = jnp.zeros((1, NZ), F32)
    for i, value in enumerate(stats):
        out = jnp.where(lane == i, value, out)
    stat_ref[...] = out


def finish_kernel(weight_total, u_ref, rate_ref, field_ref, stat_ref, grav_ref, source_ref, norm_ref):
    stat = stat_ref[...]
    part = [stat[:, i : i + 1] for i in range(7)]
    step = cfl_euler * elem_width / (7.0 * part[0])
    mean = part[6] * (1.0 / weight_total)
    shift = coupling * mean
    squares = (
        part[1]
        + step * (2.0 * part[2] + step * part[3])
        + shift * (2.0 * (part[4] + step * part[5]) + shift * weight_total)
    )
    norm_ref[...] = jnp.sqrt(jnp.maximum(squares, 0.0) * (1.0 / weight_total))
    raised = (ITERS * pseudo_step) * shift
    for x in range(NX):
        phi = field_ref[0, x] + step * field_ref[4, x] + raised
        grad = [field_ref[c, x] + step * field_ref[4 + c, x] for c in range(1, 4)]
        grav_ref[0, x] = phi
        for c in range(3):
            grav_ref[1 + c, x] = grad[c]
        rho = u_ref[0, x] + step * rate_ref[0, x]
        work = 0.0
        for c in range(3):
            source_ref[c, x] = -rho * grad[c]
            work = work + (u_ref[1 + c, x] + step * rate_ref[1 + c, x]) * grad[c]
        source_ref[3, x] = -work


def call(kernel, out_shape, flops, on_chip=True):
    def run(*args):
        if on_chip:
            args = [pltpu.with_memory_space_constraint(a, pltpu.VMEM) for a in args]
        return pl.pallas_call(
            kernel,
            in_specs=[pl.BlockSpec(memory_space=pltpu.VMEM)] * len(args),
            out_specs=[pl.BlockSpec(memory_space=pltpu.VMEM)] * len(out_shape),
            out_shape=out_shape,
            cost_estimate=pl.CostEstimate(flops=flops, bytes_accessed=400000, transcendentals=0),
        )(*args)

    return run


def pair_of(i, size):
    return i ^ 1


def other_of(i, size):
    return (i + 1 if i % 2 else i - 1) % size


ROUTES = {
    "state": (
        (GX, other_of),
        (GZ, other_of),
        ("gy", other_of),
        ("gy", pair_of),
        (GZ, pair_of),
        (GX, pair_of),
    ),
    "second": ((GX, other_of), ("gy", other_of), ("gy", pair_of), (GX, pair_of)),
    "third": ((GZ, other_of), ("gy", other_of), ("gy", pair_of), (GZ, pair_of)),
}


def exchange(messages, stage):
    received = []
    for message, (axis, partner) in zip(messages, ROUTES[stage]):
        size = lax.axis_size(axis)
        received.append(lax.ppermute(message, axis, [(a, partner(a, size)) for a in range(size)]))
    return received


def gather(stat, axis):
    lane = lax.broadcasted_iota(jnp.int32, (1, NZ), 1)
    every = lax.all_gather(stat, axis, tiled=True)
    return jnp.where(
        lane == 0, jnp.max(every, axis=0, keepdims=True), jnp.sum(every, axis=0, keepdims=True)
    )


def spread(stat):
    names = ("gx_0", "gx_1", "gy", "gz_0", "gz_1")
    sizes = [lax.axis_size(name) for name in names]
    ring = sizes[0] * sizes[3]
    pairs = []
    for at in np.ndindex(*sizes):
        a, core, b, c, e = at
        half = sizes[4] // 2
        step = e - (half - 1)
        if core:
            step += half if step > 0 else -half
        place = (a * sizes[3] + c + step) % ring
        to = (place // sizes[3], core, b, place % sizes[3], e)
        pairs.append(
            (int(np.ravel_multi_index(at, sizes)), int(np.ravel_multi_index(to, sizes)))
        )
    return lax.ppermute(stat, names, pairs)


def over_all(stat):
    for axis in ("gx_1", "gy", "gz_1"):
        stat = gather(stat, axis)
    stat = spread(stat)
    for axis in ("gx_1", "gz_1", "gx_0"):
        stat = gather(stat, axis)
    return stat


def shape(*dims):
    return pltpu.VMEM(dims, F32)


def local(u, g):
    weight_total = float(
        8.0
        * (u.shape[1] // 4 * lax.axis_size(GX))
        * (u.shape[2] // 4 * lax.axis_size("gy"))
        * (u.shape[3] // 4 * lax.axis_size(GZ))
    )
    full = (NX, NY, NZ)
    tile = shape(NY, NZ)
    planes, rows = (shape(9, NY, NZ), shape(9, NX, NZ))
    u, g, *messages = call(
        pack_kernel,
        [shape(5, *full), shape(4, *full), planes, tile, rows, rows, tile, planes],
        10**5,
        False,
    )(u, g)
    received = exchange(messages, "state")
    vol, alpha, fast = call(volume_kernel, [shape(5, *full), tile, tile], 10**7)(u)
    planes, rows = (shape(13, NY, NZ), shape(13, NX, NZ))
    rate, f1, f2, *messages = call(
        face_kernel,
        [shape(5, *full), shape(5, *full), shape(8, *full), planes, rows, rows, planes],
        10**6,
    )(u, g, vol, alpha, *received)
    received = exchange(messages, "second")
    corners = shape(10, NZ)
    f2, sides, rows, *messages = call(
        join_kernel,
        [shape(8, *full), shape(2, 13, NY, NZ), shape(13, *full), tile, corners, corners, tile],
        10**6,
    )(f1, f2, *received)
    received = exchange(messages, "third")
    field, stat = call(last_kernel, [shape(8, *full), shape(1, NZ)], 10**6)(
        u, rate, fast, f1, f2, sides, rows, *received
    )
    stat = over_all(stat)
    gravity, gravity_source, norm = call(
        functools.partial(finish_kernel, weight_total),
        [jax.ShapeDtypeStruct((4, *full), F32)] * 2 + [jax.ShapeDtypeStruct((1, 1), F32)],
        10**5,
    )(u, rate, field, stat)
    return (rate, gravity, gravity_source, norm.reshape(()))


def solution(mesh):
    torus = Mesh(
        mesh.devices.reshape(4, 2, mesh.shape["gy"], 8, 4), ("gx_0", "gx_1", "gy", "gz_0", "gz_1")
    )
    placed = (P(None, GX, "gy", GZ), P(None, GX, "gy", GZ))
    return jax.shard_map(
        local,
        mesh=torus,
        in_specs=placed,
        out_specs=(P(None, GX, "gy", GZ), P(None, GX, "gy", GZ), P(None, GX, "gy", GZ), P()),
        check_vma=False,
    )
```

```python
import functools
import math

import jax
import jax.numpy as jnp
import numpy as np
from jax import lax
from jax.experimental import pallas as pl
from jax.experimental.pallas import tpu as pltpu
from jax.sharding import Mesh
from jax.sharding import PartitionSpec as P


ITERS = 3
GX = ("gx_0", "gx_1")
GZ = ("gz_0", "gz_1")

gamma_gas = 1.4
elem_width = 1.0
cfl_euler = 0.5
alpha_most = 0.5
indicator_level = 0.5 * 10.0 ** (-1.8 * 4.0**0.25)
indicator_slope = math.log((1.0 - 0.0001) / 0.0001) / indicator_level
coupling = 10.0
pseudo_step = 0.3 * elem_width / 7.0
rho_offset = 2.3

NX, NY, NZ = (4, 8, 128)
F32 = jnp.float32


def lgl_tables():
    points = np.array([-1.0, -1.0 / math.sqrt(5.0), 1.0 / math.sqrt(5.0), 1.0])
    weights = np.array([1.0, 5.0, 5.0, 1.0]) / 6.0
    barycentric = np.array(
        [1.0 / np.prod([points[a] - points[b] for b in range(4) if b != a]) for a in range(4)]
    )
    derivative = np.zeros((4, 4))
    for a in range(4):
        for b in range(4):
            if b != a:
                derivative[a, b] = barycentric[b] / barycentric[a] / (points[a] - points[b])
        derivative[a, a] = -np.sum(derivative[a])
    legendre = np.stack(
        [np.ones(4), points, 0.5 * (3.0 * points**2 - 1.0), 0.5 * (5.0 * points**3 - 3.0 * points)],
        axis=1,
    )
    legendre = legendre * np.sqrt((2.0 * np.arange(4) + 1.0) / 2.0)
    gram = np.sum(weights[:, None] * legendre * legendre, axis=0)
    modal_map = (legendre * weights[:, None]).T / gram[:, None]
    return (weights, derivative, modal_map)


WEIGHTS, DERIV, MODAL = lgl_tables()


class Line:
    def __init__(self, dim):
        self.dim = dim
        self.length = (NY, NZ)[dim]
        self.at = lax.broadcasted_iota(jnp.int32, (NY, NZ), dim)
        self.node = self.at % 4
        self.lowest = self.at == 0
        self.highest = self.at == self.length - 1
        self.is0 = self.node == 0
        self.is3 = self.node == 3

    def by_node(self, values):
        v = [float(item) for item in values]
        if v[1] == v[2] and v[0] == v[3]:
            return jnp.where(self.is0 | self.is3, v[0], v[1]).astype(F32)
        return jnp.where(
            self.node < 2,
            jnp.where(self.is0, v[0], v[1]),
            jnp.where(self.is3, v[3], v[2]),
        ).astype(F32)

    def roll(self, value, by):
        return pltpu.roll(value, by % self.length, self.dim)

    def cyc(self, value, k):
        return jnp.where(self.node < 4 - k, self.roll(value, -k), self.roll(value, 4 - k))

    def coef(self, matrix, k, scale=1.0):
        return self.by_node([scale * matrix[i, (i + k) % 4] for i in range(4)])

    def element_sum(self, value):
        value = value + self.cyc(value, 2)
        return value + self.cyc(value, 1)


def load(ref):
    return [[ref[c, x] for x in range(NX)] for c in range(ref.shape[0])]


def is_even():
    return [lax.axis_index(axis) % 2 == 0 for axis in ("gx_1", "gy", "gz_1")]


def pack_x(comps, other, pair):
    even = is_even()[0]
    for c, comp in enumerate(comps):
        other[c] = jnp.where(even, comp[0], comp[NX - 1])
        pair[c] = jnp.where(even, comp[NX - 1], comp[0])


def pack_y(comps, other, pair):
    even = is_even()[1]
    for c, comp in enumerate(comps):
        for x, tile in enumerate(comp):
            low, high = (tile[0:1, :], tile[NY - 1 : NY, :])
            other[c, pl.ds(x, 1), :] = jnp.where(even, low, high)
            pair[c, pl.ds(x, 1), :] = jnp.where(even, high, low)


def pack_z(tiles, other, pair):
    even = is_even()[2]
    lane = lax.broadcasted_iota(jnp.int32, (NY, NZ), 1)
    first = jnp.zeros((NY, NZ), F32)
    last = jnp.zeros((NY, NZ), F32)
    for k, tile in enumerate(tiles):
        here = lane == k
        first = jnp.where(here, pltpu.roll(tile, k, 1) if k else tile, first)
        last = jnp.where(here, pltpu.roll(tile, k + 1, 1), last)
    other[...] = jnp.where(even, first, last)
    pair[...] = jnp.where(even, last, first)


def flat(comps):
    return [tile for comp in comps for tile in comp]


class Halo:
    def __init__(self, refs):
        self.even = is_even()
        self.refs = refs
        zo, zp = (refs[1][...], refs[4][...])
        self.zlo = jnp.where(self.even[2], zo, zp)
        self.zhi = jnp.where(self.even[2], zp, zo)

    def x_low(self, c):
        return jnp.where(self.even[0], self.refs[0][c], self.refs[5][c])

    def x_high(self, c):
        return jnp.where(self.even[0], self.refs[5][c], self.refs[0][c])

    def row(self, c, x, pair, other):
        line = jnp.where(self.even[1], self.refs[pair][c, pl.ds(x, 1), :], self.refs[other][c, pl.ds(x, 1), :])
        return jnp.broadcast_to(line, (NY, NZ))

    def low(self, dim, c, x):
        if dim == 0:
            return self.row(c, x, 2, 3)
        k = c * NX + x
        return pltpu.roll(self.zlo, (NZ - k) % NZ, 1) if k else self.zlo

    def high(self, dim, c, x):
        if dim == 0:
            return self.row(c, x, 3, 2)
        k = c * NX + x
        return pltpu.roll(self.zhi, NZ - 1 - k, 1)


def log_mean(left, right):
    total = left + right
    gap = right - left
    slope = gap / total
    ratio_sq = slope * slope
    is_close = ratio_sq < 0.0001
    series = 2.0 + ratio_sq * (2.0 / 3.0 + ratio_sq * (2.0 / 5.0 + ratio_sq * (2.0 / 7.0)))
    top = jnp.where(is_close, total, gap)
    low = jnp.where(is_close, series, jnp.log(right / left))
    return top / low


def two_point(left, right, d):
    rho_mean = log_mean(left[0], right[0])
    inv_mean = left[4] * right[4] / log_mean(left[0] * right[4], right[0] * left[4])
    vel = [0.5 * (left[1 + i] + right[1 + i]) for i in range(3)]
    product = left[1] * right[1] + left[2] * right[2] + left[3] * right[3]
    mass = rho_mean * vel[d]
    flux = [mass] + [mass * vel[i] for i in range(3)]
    flux[1 + d] = flux[1 + d] + 0.5 * (left[4] + right[4])
    energy = mass * (0.5 * product + inv_mean * (1.0 / (gamma_gas - 1.0))) + 0.5 * (
        left[4] * right[1 + d] + right[4] * left[1 + d]
    )
    return flux + [energy]


def primitive(u):
    inv = 1.0 / u[0]
    vel = [u[1 + i] * inv for i in range(3)]
    kinetic = u[1] * vel[0] + u[2] * vel[1] + u[3] * vel[2]
    pressure = (gamma_gas - 1.0) * (u[4] - 0.5 * kinetic)
    return (vel, pressure, jnp.sqrt(gamma_gas * pressure * inv))


def face_data(u, d, known=None):
    vel, pressure, sound = known or primitive(u)
    normal = vel[d]
    flux = [u[1 + d]] + [u[1 + i] * normal for i in range(3)] + [(u[4] + pressure) * normal]
    flux[1 + d] = flux[1 + d] + pressure
    return (u, flux, jnp.abs(normal) + sound)


def interface(left, right):
    speed = jnp.maximum(left[2], right[2])
    return [
        0.5 * ((left[1][c] + right[1][c]) - speed * (right[0][c] - left[0][c])) for c in range(5)
    ]


def volume_kernel(u_ref, vol_ref, alpha_ref, fast_ref):
    y, z = (Line(0), Line(1))
    u = load(u_ref)
    known = [primitive([u[c][x] for c in range(5)]) for x in range(NX)]
    nodes = [[u[0][x]] + known[x][0] + [known[x][1]] for x in range(NX)]
    speed = [
        jnp.abs(known[x][0][0]) + jnp.abs(known[x][0][1]) + jnp.abs(known[x][0][2]) + 3.0 * known[x][2]
        for x in range(NX)
    ]
    fast_ref[...] = jnp.maximum(jnp.maximum(speed[0], speed[1]), jnp.maximum(speed[2], speed[3]))

    product = [u[0][x] * known[x][1] for x in range(NX)]
    coeffs = [sum(float(MODAL[a, i]) * product[i] for i in range(4)) for a in range(4)]
    for line in (y, z):
        modal = [line.coef(MODAL, k) for k in range(4)]
        coeffs = [
            modal[0] * value + sum(modal[k] * line.cyc(value, k) for k in range(1, 4))
            for value in coeffs
        ]
    energy = [value * value for value in coeffs]
    total = (energy[0] + energy[1]) + (energy[2] + energy[3])
    low = (energy[0] + energy[1]) + energy[2]
    high = energy[3] + jnp.where(y.is3 | z.is3, low, 0.0)
    share = z.element_sum(y.element_sum(high)) / z.element_sum(y.element_sum(total))
    alpha = alpha_most / (1.0 + jnp.exp(-indicator_slope * (share - indicator_level)))
    alpha_ref[...] = alpha

    volume = [[None] * NX for _ in range(5)]
    for i in range(NX):
        for j in range(i + 1, NX):
            flux = two_point(nodes[i], nodes[j], 0)
            for c in range(5):
                for at, other in ((i, j), (j, i)):
                    term = (2.0 * DERIV[at, other]).astype(np.float32) * flux[c]
                    volume[c][at] = term if volume[c][at] is None else volume[c][at] + term
    for d, line in ((1, y), (2, z)):
        up, across, down = [line.coef(DERIV, k, 2.0) for k in (1, 2, 3)]
        for x in range(NX):
            near = two_point(nodes[x], [line.cyc(a, 1) for a in nodes[x]], d)
            far = two_point(nodes[x], [line.cyc(a, 2) for a in nodes[x]], d)
            for c in range(5):
                volume[c][x] = volume[c][x] + (
                    up * near[c] + down * line.cyc(near[c], 3) + across * far[c]
                )
    keep = 1.0 - alpha
    for c in range(5):
        for x in range(NX):
            vol_ref[c, x] = keep * volume[c][x]


def gravity_parts(field, halo, base, y, z):
    total = [[0.0] * NX for _ in range(4)]
    have = [c for c in range(4) if field[c] is not None]
    where = {c: base + i for i, c in enumerate(have)}

    for c, partner in ((0, 1), (1, 0)):
        if field[partner] is not None:
            for i in range(NX):
                terms = [float(2.0 * DERIV[i, j]) * field[partner][j] for j in range(NX) if DERIV[i, j] != 0.0]
                total[c][i] = total[c][i] + sum(terms[1:], terms[0])
    jumps = {}
    for c in have if halo is not None else ():
        jumps[c] = (halo.x_low(where[c]) - field[c][0], halo.x_high(where[c]) - field[c][NX - 1])
        for side, x in ((0, 0), (1, NX - 1)):
            total[c][x] = total[c][x] + 6.0 * jumps[c][side]
    for c, partner in ((0, 1), (1, 0)):
        if partner in jumps:
            total[c][0] = total[c][0] - 6.0 * jumps[partner][0]
            total[c][NX - 1] = total[c][NX - 1] + 6.0 * jumps[partner][1]
    for d, line in ((1, y), (2, z)):
        comp = 1 + d
        diag = line.coef(DERIV, 0, 2.0)
        coefs = [line.coef(DERIV, k, 2.0) for k in range(1, 4)]
        sign = line.by_node([-6.0, 0.0, 0.0, 6.0])
        for x in range(NX):
            for c, partner in ((0, comp), (comp, 0)):
                if field[partner] is not None:
                    value = field[partner][x]
                    term = diag * value
                    for k in range(1, 4):
                        term = term + coefs[k - 1] * line.cyc(value, k)
                    total[c][x] = total[c][x] + term
            gaps = {}
            for c in have:
                value = field[c][x]
                low, high = (value, value)
                if halo is not None:
                    low = halo.low(line.dim, where[c], x)
                    high = halo.high(line.dim, where[c], x)
                prev = jnp.where(line.lowest, low, line.roll(value, 1))
                after = jnp.where(line.highest, high, line.roll(value, -1))
                beside = jnp.where(line.is0, prev, jnp.where(line.is3, after, value))
                gaps[c] = beside - value
                total[c][x] = total[c][x] + 6.0 * gaps[c]
            for c, partner in ((0, comp), (comp, 0)):
                if partner in gaps:
                    total[c][x] = total[c][x] + sign * gaps[partner]
    return total


def advance(field, halo, base, y, z, source):
    total = gravity_parts(field, halo, base, y, z)
    phi_rate = [total[0][x] - coupling * source[x] for x in range(NX)]
    new = [[None] * NX for _ in range(4)]
    for x in range(NX):
        change = pseudo_step * phi_rate[x]
        new[0][x] = change if field[0] is None else field[0][x] + change
        for c in range(1, 4):
            if field[c] is None:
                new[c][x] = pseudo_step * total[c][x]
            else:
                new[c][x] = field[c][x] + pseudo_step * (total[c][x] - field[c][x])
    return (new, phi_rate)


def pack_kernel(u_ref, g_ref, u_out, g_out, *outs):
    u_out[...] = u_ref[...]
    g_out[...] = g_ref[...]
    comps = load(u_ref) + load(g_ref)
    xo, zo, yo, yp, zp, xp = outs
    pack_x(comps, xo, xp)
    pack_y(comps, yo, yp)
    pack_z(flat(comps), zo, zp)


def face_kernel(u_ref, g_ref, vol_ref, alpha_ref, *refs):
    halo = Halo(refs[:6])
    rate_ref, f1_ref, f2_ref, xo, yo, yp, xp = refs[6:]
    y, z = (Line(0), Line(1))
    u = load(u_ref)
    g = load(g_ref)
    alpha = alpha_ref[...]
    keep = 1.0 - alpha
    known = [primitive([u[c][x] for c in range(5)]) for x in range(NX)]
    total = load(vol_ref)

    own = [face_data([u[c][x] for c in range(5)], 0, known[x]) for x in range(NX)]
    below = face_data([halo.x_low(c) for c in range(5)], 0)
    above = face_data([halo.x_high(c) for c in range(5)], 0)
    chain = [below] + own + [above]
    faces = [interface(chain[i], chain[i + 1]) for i in range(NX + 1)]
    for x in range(NX):
        inner = alpha * float(1.0 / WEIGHTS[x])
        edge = inner + keep * 6.0
        low_coef = edge if x == 0 else inner
        high_coef = edge if x == NX - 1 else inner
        for c in range(5):
            total[c][x] = total[c][x] + (high_coef * faces[x + 1][c] - low_coef * faces[x][c])
    for d, line in ((1, y), (2, z)):
        inner = alpha * line.by_node(1.0 / WEIGHTS)
        low_coef = inner + keep * line.by_node([6.0, 0.0, 0.0, 0.0])
        high_coef = inner + keep * line.by_node([0.0, 0.0, 0.0, 6.0])
        for x in range(NX):
            mine = face_data([u[c][x] for c in range(5)], d, known[x])
            prev = face_data(
                [
                    jnp.where(line.lowest, halo.low(line.dim, c, x), line.roll(u[c][x], 1))
                    for c in range(5)
                ],
                d,
            )
            after = face_data(
                [jnp.where(line.highest, halo.high(line.dim, c, x), u[c][x]) for c in range(5)], d
            )
            face = interface(prev, mine)
            end = interface(mine, after)
            for c in range(5):
                following = jnp.where(line.highest, end[c], line.roll(face[c], -1))
                total[c][x] = total[c][x] + (high_coef * following - low_coef * face[c])
    rate = [[-2.0 * total[c][x] for x in range(NX)] for c in range(5)]
    for x in range(NX):
        for i in range(3):
            rate[1 + i][x] = rate[1 + i][x] - u[0][x] * g[1 + i][x]
        rate[4][x] = rate[4][x] - (
            u[1][x] * g[1][x] + u[2][x] * g[2][x] + u[3][x] * g[3][x]
        )
        for c in range(5):
            rate_ref[c, x] = rate[c][x]

    source = [u[0][x] - rho_offset for x in range(NX)]
    new, _ = advance(g, halo, 5, y, z, source)
    slope = [(-pseudo_step * coupling) * rate[0][x] for x in range(NX)]
    partial, _ = advance(new, None, 0, y, z, source)
    partial_slope, _ = advance([slope, None, None, None], None, 0, y, z, rate[0])
    f1 = new + [slope]
    f2 = partial + partial_slope
    for x in range(NX):
        for c in range(5):
            f1_ref[c, x] = f1[c][x]
        for c in range(8):
            f2_ref[c, x] = f2[c][x]
    pack_x(f1 + f2, xo, xp)
    pack_y(f1 + f2, yo, yp)


def face_terms(gap, d, sign):
    terms = [None if value is None else 6.0 * value for value in gap]
    for c, partner in ((0, 1 + d), (1 + d, 0)):
        if gap[partner] is not None:
            extra = sign * gap[partner]
            terms[c] = extra if terms[c] is None else terms[c] + extra
    return terms


def meet(field, gap, d, sign):
    terms = face_terms(gap[:4], d, sign) + face_terms([gap[4], None, None, None], d, sign)
    return [
        value if term is None else value + pseudo_step * term for value, term in zip(field, terms)
    ]


def ends(line):
    outer = line.lowest | line.highest
    sign = jnp.where(line.lowest, -6.0, jnp.where(line.highest, 6.0, 0.0)).astype(F32)
    return (outer, sign)


def at(field, x, first, count):
    return [field[first + c][x] for c in range(count)]


def join_kernel(f1_ref, f2_ref, xo, yo, yp, xp, f2_out, side_ref, row_ref, zo, zp, corner_ref):
    even = is_even()
    y = Line(0)
    f1, f2 = (load(f1_ref), load(f2_ref))
    sides = []
    for low, x, sign in ((True, 0, -6.0), (False, NX - 1, 6.0)):
        near, away = (xo, xp) if low else (xp, xo)
        side = [jnp.where(even[0], near[c], away[c]) for c in range(13)]
        gap = [side[c] - f1[c][x] for c in range(5)]
        for c, value in enumerate(meet(at(f2, x, 0, 8), gap, 0, sign)):
            f2[c][x] = value
        side[5:] = meet(side[5:], [-value for value in gap], 0, -sign)
        sides.append(side)
    outer, sign = ends(y)
    rows = [[None] * NX for _ in range(13)]
    for x in range(NX):
        for c in range(13):
            other, pair = (yo[c, pl.ds(x, 1), :], yp[c, pl.ds(x, 1), :])
            low = jnp.broadcast_to(jnp.where(even[1], other, pair), (NY, NZ))
            high = jnp.broadcast_to(jnp.where(even[1], pair, other), (NY, NZ))
            rows[c][x] = jnp.where(y.lowest, low, jnp.where(y.highest, high, 0.0))
        gap = [jnp.where(outer, rows[c][x] - f1[c][x], 0.0) for c in range(5)]
        for c, value in enumerate(meet(at(f2, x, 0, 8), gap, 1, sign)):
            f2[c][x] = value
        for c, value in enumerate(meet(at(rows, x, 5, 8), [-v for v in gap], 1, -sign)):
            rows[5 + c][x] = value
    for x in range(NX):
        for c in range(8):
            f2_out[c, x] = f2[c][x]
        for c in range(13):
            row_ref[c, x] = rows[c][x]
    for w, side in enumerate(sides):
        for c in range(13):
            side_ref[w, c] = side[c]
        for c in range(5):
            corner_ref[0, pl.ds(5 * w + c, 1), :] = side[c][0:1, :]
            corner_ref[1, pl.ds(5 * w + c, 1), :] = side[c][NY - 1 : NY, :]
    pack_z(flat(f1 + f2) + sides[0][:5] + sides[1][:5] + flat(rows[:5]), zo, zp)


class Around:
    def __init__(self, sides, rows, columns):
        self.sides, self.rows, self.columns = (sides, rows, columns)

    def x_low(self, c):
        return self.sides[0][c]

    def x_high(self, c):
        return self.sides[1][c]

    def low(self, dim, c, x):
        return (self.rows, self.columns)[dim][c][x]

    high = low


def last_kernel(
    u_ref, rate_ref, fast_ref, f1_ref, f2_ref, side_ref, row_ref, zo, zp, corner_ref, next_ref, stat_ref
):
    even = is_even()
    y, z = (Line(0), Line(1))
    f1, f2, rows = (load(f1_ref), load(f2_ref), load(row_ref))
    sides = [[side_ref[w, c] for c in range(13)] for w in range(2)]
    places = lax.axis_size("gy")
    below = lax.rem(lax.axis_index("gy") + (places - 1), places)
    above = lax.rem(lax.axis_index("gy") + 1, places)
    z_other, z_pair = (zo[...], zp[...])
    z_low = jnp.where(even[2], z_other, z_pair)
    z_high = jnp.where(even[2], z_pair, z_other)
    z_outer, z_sign = ends(z)
    y_outer, y_sign = ends(y)

    def column(k):
        low = pltpu.roll(z_low, (NZ - k) % NZ, 1) if k else z_low
        return jnp.where(z.lowest, low, pltpu.roll(z_high, NZ - 1 - k, 1))

    def gaps(outer, beside, own):
        return [jnp.where(outer, b - o, 0.0) for b, o in zip(beside, own)]

    columns = [[column(c * NX + x) for x in range(NX)] for c in range(13)]
    for x in range(NX):
        gap = gaps(z_outer, at(columns, x, 0, 5), at(f1, x, 0, 5))
        for c, value in enumerate(meet(at(f2, x, 0, 8), gap, 2, z_sign)):
            f2[c][x] = value
        for c, value in enumerate(meet(at(columns, x, 5, 8), [-v for v in gap], 2, -z_sign)):
            columns[5 + c][x] = value
    for w, x, sign in ((0, 0, -6.0), (1, NX - 1, 6.0)):
        corner = []
        for c in range(5):
            low = corner_ref[2 * below + 1, pl.ds(5 * w + c, 1), :]
            high = corner_ref[2 * above, pl.ds(5 * w + c, 1), :]
            corner.append(
                jnp.where(
                    y.lowest, jnp.broadcast_to(low, (NY, NZ)), jnp.broadcast_to(high, (NY, NZ))
                )
            )
        side = sides[w]
        beside = [column(13 * NX + 5 * w + c) for c in range(5)]
        side[5:] = meet(side[5:], gaps(z_outer, beside, side[:5]), 2, z_sign)
        side[5:] = meet(side[5:], gaps(y_outer, corner, side[:5]), 1, y_sign)
        gap = gaps(y_outer, corner, at(rows, x, 0, 5))
        for c, value in enumerate(meet(at(rows, x, 5, 8), gap, 0, sign)):
            rows[5 + c][x] = value
    for x in range(NX):
        beside = [column(13 * NX + 10 + c * NX + x) for c in range(5)]
        gap = gaps(z_outer & y_outer, beside, at(rows, x, 0, 5))
        for c, value in enumerate(meet(at(rows, x, 5, 8), gap, 2, z_sign)):
            rows[5 + c][x] = value

    around = Around([side[5:] for side in sides], rows[5:], columns[5:])
    source = [u_ref[0, x] - rho_offset for x in range(NX)]
    new, base_rate = advance(f2[:4], around, 0, y, z, source)
    slope, slope_rate = advance(f2[4:], around, 4, y, z, [rate_ref[0, x] for x in range(NX)])
    comps = new + slope
    for c in range(8):
        for x in range(NX):
            next_ref[c, x] = comps[c][x]
    weight = y.by_node(WEIGHTS) * z.by_node(WEIGHTS)

    def total(values):
        by_x = [float(WEIGHTS[x]) * values[x] for x in range(NX)]
        return jnp.sum(((by_x[0] + by_x[1]) + (by_x[2] + by_x[3])) * weight)

    stats = [
        jnp.max(fast_ref[...]),
        total([a * a for a in base_rate]),
        total([a * b for a, b in zip(base_rate, slope_rate)]),
        total([b * b for b in slope_rate]),
        total(base_rate),
        total(slope_rate),
        total(source),
    ]
    lane = lax.broadcasted_iota(jnp.int32, (1, NZ), 1)
    out = jnp.zeros((1, NZ), F32)
    for i, value in enumerate(stats):
        out = jnp.where(lane == i, value, out)
    stat_ref[...] = out


def finish_kernel(weight_total, u_ref, rate_ref, field_ref, stat_ref, grav_ref, source_ref, norm_ref):
    stat = stat_ref[...]
    part = [stat[:, i : i + 1] for i in range(7)]
    step = cfl_euler * elem_width / (7.0 * part[0])
    mean = part[6] * (1.0 / weight_total)
    shift = coupling * mean
    squares = (
        part[1]
        + step * (2.0 * part[2] + step * part[3])
        + shift * (2.0 * (part[4] + step * part[5]) + shift * weight_total)
    )
    norm_ref[...] = jnp.sqrt(jnp.maximum(squares, 0.0) * (1.0 / weight_total))
    raised = (ITERS * pseudo_step) * shift
    for x in range(NX):
        phi = field_ref[0, x] + step * field_ref[4, x] + raised
        grad = [field_ref[c, x] + step * field_ref[4 + c, x] for c in range(1, 4)]
        grav_ref[0, x] = phi
        for c in range(3):
            grav_ref[1 + c, x] = grad[c]
        rho = u_ref[0, x] + step * rate_ref[0, x]
        work = 0.0
        for c in range(3):
            source_ref[c, x] = -rho * grad[c]
            work = work + (u_ref[1 + c, x] + step * rate_ref[1 + c, x]) * grad[c]
        source_ref[3, x] = -work


def call(kernel, out_shape, flops, on_chip=True):
    def run(*args):
        if on_chip:
            args = [pltpu.with_memory_space_constraint(a, pltpu.VMEM) for a in args]
        return pl.pallas_call(
            kernel,
            in_specs=[pl.BlockSpec(memory_space=pltpu.VMEM)] * len(args),
            out_specs=[pl.BlockSpec(memory_space=pltpu.VMEM)] * len(out_shape),
            out_shape=out_shape,
            cost_estimate=pl.CostEstimate(flops=flops, bytes_accessed=400000, transcendentals=0),
        )(*args)

    return run


def pair_of(i, size):
    return i ^ 1


def other_of(i, size):
    return (i + 1 if i % 2 else i - 1) % size


ROUTES = {
    "state": (
        (GX, other_of),
        (GZ, other_of),
        ("gy", other_of),
        ("gy", pair_of),
        (GZ, pair_of),
        (GX, pair_of),
    ),
    "second": ((GX, other_of), ("gy", other_of), ("gy", pair_of), (GX, pair_of)),
    "third": ((GZ, other_of), (GZ, pair_of)),
}


def exchange(messages, stage):
    received = []
    for message, (axis, partner) in zip(messages, ROUTES[stage]):
        size = lax.axis_size(axis)
        received.append(lax.ppermute(message, axis, [(a, partner(a, size)) for a in range(size)]))
    return received


def gather(stat, axis):
    lane = lax.broadcasted_iota(jnp.int32, (1, NZ), 1)
    every = lax.all_gather(stat, axis, tiled=True)
    return jnp.where(
        lane == 0, jnp.max(every, axis=0, keepdims=True), jnp.sum(every, axis=0, keepdims=True)
    )


def spread(stat):
    names = ("gx_0", "gx_1", "gy", "gz_0", "gz_1")
    sizes = [lax.axis_size(name) for name in names]
    ring = sizes[0] * sizes[3]
    pairs = []
    for at in np.ndindex(*sizes):
        a, core, b, c, e = at
        place = (a * sizes[3] + c + core * sizes[4] + e - (sizes[3] // 2 - 1)) % ring
        to = (place // sizes[3], core, b, place % sizes[3], e)
        pairs.append(
            (int(np.ravel_multi_index(at, sizes)), int(np.ravel_multi_index(to, sizes)))
        )
    return lax.ppermute(stat, names, pairs)


def over_all(stat):
    for axis in ("gx_1", "gy", "gz_1"):
        stat = gather(stat, axis)
    stat = spread(stat)
    for axis in ("gx_1", "gz_1", "gx_0"):
        stat = gather(stat, axis)
    return stat


def shape(*dims):
    return pltpu.VMEM(dims, F32)


def local(u, g):
    weight_total = float(
        8.0
        * (u.shape[1] // 4 * lax.axis_size(GX))
        * (u.shape[2] // 4 * lax.axis_size("gy"))
        * (u.shape[3] // 4 * lax.axis_size(GZ))
    )
    full = (NX, NY, NZ)
    tile = shape(NY, NZ)
    planes, rows = (shape(9, NY, NZ), shape(9, NX, NZ))
    u, g, *messages = call(
        pack_kernel,
        [shape(5, *full), shape(4, *full), planes, tile, rows, rows, tile, planes],
        10**5,
        False,
    )(u, g)
    received = exchange(messages, "state")
    vol, alpha, fast = call(volume_kernel, [shape(5, *full), tile, tile], 10**7)(u)
    planes, rows = (shape(13, NY, NZ), shape(13, NX, NZ))
    rate, f1, f2, *messages = call(
        face_kernel,
        [shape(5, *full), shape(5, *full), shape(8, *full), planes, rows, rows, planes],
        10**6,
    )(u, g, vol, alpha, *received)
    received = exchange(messages, "second")
    f2, sides, rows, *messages, corners = call(
        join_kernel,
        [shape(8, *full), shape(2, 13, NY, NZ), shape(13, *full), tile, tile, shape(2, 10, NZ)],
        10**6,
    )(f1, f2, *received)
    received = exchange(messages, "third")
    corners = lax.all_gather(corners, "gy", tiled=True)
    field, stat = call(last_kernel, [shape(8, *full), shape(1, NZ)], 10**6)(
        u, rate, fast, f1, f2, sides, rows, *received, corners
    )
    stat = over_all(stat)
    gravity, gravity_source, norm = call(
        functools.partial(finish_kernel, weight_total),
        [jax.ShapeDtypeStruct((4, *full), F32)] * 2 + [jax.ShapeDtypeStruct((1, 1), F32)],
        10**5,
    )(u, rate, field, stat)
    return (rate, gravity, gravity_source, norm.reshape(()))


def solution(mesh):
    torus = Mesh(
        mesh.devices.reshape(4, 2, mesh.shape["gy"], 8, 4), ("gx_0", "gx_1", "gy", "gz_0", "gz_1")
    )
    placed = (P(None, GX, "gy", GZ), P(None, GX, "gy", GZ))
    return jax.shard_map(
        local,
        mesh=torus,
        in_specs=placed,
        out_specs=(P(None, GX, "gy", GZ), P(None, GX, "gy", GZ), P(None, GX, "gy", GZ), P()),
        check_vma=False,
    )
```

```python
import functools
import math

import jax
import jax.numpy as jnp
import numpy as np
from jax import lax
from jax.experimental import pallas as pl
from jax.experimental.pallas import tpu as pltpu
from jax.sharding import Mesh
from jax.sharding import PartitionSpec as P


ITERS = 3
GX = ("gx_0", "gx_1")
GZ = ("gz_0", "gz_1")

gamma_gas = 1.4
elem_width = 1.0
cfl_euler = 0.5
alpha_most = 0.5
indicator_level = 0.5 * 10.0 ** (-1.8 * 4.0**0.25)
indicator_slope = math.log((1.0 - 0.0001) / 0.0001) / indicator_level
coupling = 10.0
pseudo_step = 0.3 * elem_width / 7.0
rho_offset = 2.3

NX, NY, NZ = (4, 8, 128)
F32 = jnp.float32


def lgl_tables():
    points = np.array([-1.0, -1.0 / math.sqrt(5.0), 1.0 / math.sqrt(5.0), 1.0])
    weights = np.array([1.0, 5.0, 5.0, 1.0]) / 6.0
    barycentric = np.array(
        [1.0 / np.prod([points[a] - points[b] for b in range(4) if b != a]) for a in range(4)]
    )
    derivative = np.zeros((4, 4))
    for a in range(4):
        for b in range(4):
            if b != a:
                derivative[a, b] = barycentric[b] / barycentric[a] / (points[a] - points[b])
        derivative[a, a] = -np.sum(derivative[a])
    legendre = np.stack(
        [np.ones(4), points, 0.5 * (3.0 * points**2 - 1.0), 0.5 * (5.0 * points**3 - 3.0 * points)],
        axis=1,
    )
    legendre = legendre * np.sqrt((2.0 * np.arange(4) + 1.0) / 2.0)
    gram = np.sum(weights[:, None] * legendre * legendre, axis=0)
    modal_map = (legendre * weights[:, None]).T / gram[:, None]
    return (weights, derivative, modal_map)


WEIGHTS, DERIV, MODAL = lgl_tables()


class Line:
    def __init__(self, dim):
        self.dim = dim
        self.length = (NY, NZ)[dim]
        self.at = lax.broadcasted_iota(jnp.int32, (NY, NZ), dim)
        self.node = self.at % 4
        self.lowest = self.at == 0
        self.highest = self.at == self.length - 1
        self.is0 = self.node == 0
        self.is3 = self.node == 3

    def by_node(self, values):
        v = [float(item) for item in values]
        if v[1] == v[2] and v[0] == v[3]:
            return jnp.where(self.is0 | self.is3, v[0], v[1]).astype(F32)
        return jnp.where(
            self.node < 2,
            jnp.where(self.is0, v[0], v[1]),
            jnp.where(self.is3, v[3], v[2]),
        ).astype(F32)

    def roll(self, value, by):
        return pltpu.roll(value, by % self.length, self.dim)

    def cyc(self, value, k):
        return jnp.where(self.node < 4 - k, self.roll(value, -k), self.roll(value, 4 - k))

    def coef(self, matrix, k, scale=1.0):
        return self.by_node([scale * matrix[i, (i + k) % 4] for i in range(4)])

    def element_sum(self, value):
        value = value + self.cyc(value, 2)
        return value + self.cyc(value, 1)


def load(ref):
    return [[ref[c, x] for x in range(NX)] for c in range(ref.shape[0])]


def is_even():
    return [lax.axis_index(axis) % 2 == 0 for axis in ("gx_1", "gy", "gz_1")]


def pack_x(comps, other, pair):
    even = is_even()[0]
    for c, comp in enumerate(comps):
        other[c] = jnp.where(even, comp[0], comp[NX - 1])
        pair[c] = jnp.where(even, comp[NX - 1], comp[0])


def pack_y(comps, other, pair):
    even = is_even()[1]
    for c, comp in enumerate(comps):
        for x, tile in enumerate(comp):
            low, high = (tile[0:1, :], tile[NY - 1 : NY, :])
            other[c, pl.ds(x, 1), :] = jnp.where(even, low, high)
            pair[c, pl.ds(x, 1), :] = jnp.where(even, high, low)


def pack_z(tiles, other, pair):
    even = is_even()[2]
    lane = lax.broadcasted_iota(jnp.int32, (NY, NZ), 1)
    first = jnp.zeros((NY, NZ), F32)
    last = jnp.zeros((NY, NZ), F32)
    for k, tile in enumerate(tiles):
        here = lane == k
        first = jnp.where(here, pltpu.roll(tile, k, 1) if k else tile, first)
        last = jnp.where(here, pltpu.roll(tile, k + 1, 1), last)
    other[...] = jnp.where(even, first, last)
    pair[...] = jnp.where(even, last, first)


def flat(comps):
    return [tile for comp in comps for tile in comp]


class Halo:
    def __init__(self, refs):
        self.even = is_even()
        self.refs = refs
        zo, zp = (refs[1][...], refs[4][...])
        self.zlo = jnp.where(self.even[2], zo, zp)
        self.zhi = jnp.where(self.even[2], zp, zo)

    def x_low(self, c):
        return jnp.where(self.even[0], self.refs[0][c], self.refs[5][c])

    def x_high(self, c):
        return jnp.where(self.even[0], self.refs[5][c], self.refs[0][c])

    def row(self, c, x, pair, other):
        line = jnp.where(self.even[1], self.refs[pair][c, pl.ds(x, 1), :], self.refs[other][c, pl.ds(x, 1), :])
        return jnp.broadcast_to(line, (NY, NZ))

    def low(self, dim, c, x):
        if dim == 0:
            return self.row(c, x, 2, 3)
        k = c * NX + x
        return pltpu.roll(self.zlo, (NZ - k) % NZ, 1) if k else self.zlo

    def high(self, dim, c, x):
        if dim == 0:
            return self.row(c, x, 3, 2)
        k = c * NX + x
        return pltpu.roll(self.zhi, NZ - 1 - k, 1)


def log_mean(left, right):
    total = left + right
    gap = right - left
    slope = gap / total
    ratio_sq = slope * slope
    is_close = ratio_sq < 0.0001
    series = 2.0 + ratio_sq * (2.0 / 3.0 + ratio_sq * (2.0 / 5.0 + ratio_sq * (2.0 / 7.0)))
    top = jnp.where(is_close, total, gap)
    low = jnp.where(is_close, series, jnp.log(right / left))
    return top / low


def two_point(left, right, d):
    rho_mean = log_mean(left[0], right[0])
    inv_mean = left[4] * right[4] / log_mean(left[0] * right[4], right[0] * left[4])
    vel = [0.5 * (left[1 + i] + right[1 + i]) for i in range(3)]
    product = left[1] * right[1] + left[2] * right[2] + left[3] * right[3]
    mass = rho_mean * vel[d]
    flux = [mass] + [mass * vel[i] for i in range(3)]
    flux[1 + d] = flux[1 + d] + 0.5 * (left[4] + right[4])
    energy = mass * (0.5 * product + inv_mean * (1.0 / (gamma_gas - 1.0))) + 0.5 * (
        left[4] * right[1 + d] + right[4] * left[1 + d]
    )
    return flux + [energy]


def primitive(u):
    inv = 1.0 / u[0]
    vel = [u[1 + i] * inv for i in range(3)]
    kinetic = u[1] * vel[0] + u[2] * vel[1] + u[3] * vel[2]
    pressure = (gamma_gas - 1.0) * (u[4] - 0.5 * kinetic)
    return (vel, pressure, jnp.sqrt(gamma_gas * pressure * inv))


def face_data(u, d, known=None):
    vel, pressure, sound = known or primitive(u)
    normal = vel[d]
    flux = [u[1 + d]] + [u[1 + i] * normal for i in range(3)] + [(u[4] + pressure) * normal]
    flux[1 + d] = flux[1 + d] + pressure
    return (u, flux, jnp.abs(normal) + sound)


def interface(left, right):
    speed = jnp.maximum(left[2], right[2])
    return [
        0.5 * ((left[1][c] + right[1][c]) - speed * (right[0][c] - left[0][c])) for c in range(5)
    ]


def volume_kernel(u_ref, vol_ref, alpha_ref, fast_ref):
    y, z = (Line(0), Line(1))
    u = load(u_ref)
    known = [primitive([u[c][x] for c in range(5)]) for x in range(NX)]
    nodes = [[u[0][x]] + known[x][0] + [known[x][1]] for x in range(NX)]
    speed = [
        jnp.abs(known[x][0][0]) + jnp.abs(known[x][0][1]) + jnp.abs(known[x][0][2]) + 3.0 * known[x][2]
        for x in range(NX)
    ]
    fast_ref[...] = jnp.maximum(jnp.maximum(speed[0], speed[1]), jnp.maximum(speed[2], speed[3]))

    product = [u[0][x] * known[x][1] for x in range(NX)]
    coeffs = [sum(float(MODAL[a, i]) * product[i] for i in range(4)) for a in range(4)]
    for line in (y, z):
        modal = [line.coef(MODAL, k) for k in range(4)]
        coeffs = [
            modal[0] * value + sum(modal[k] * line.cyc(value, k) for k in range(1, 4))
            for value in coeffs
        ]
    energy = [value * value for value in coeffs]
    total = (energy[0] + energy[1]) + (energy[2] + energy[3])
    low = (energy[0] + energy[1]) + energy[2]
    high = energy[3] + jnp.where(y.is3 | z.is3, low, 0.0)
    share = z.element_sum(y.element_sum(high)) / z.element_sum(y.element_sum(total))
    alpha = alpha_most / (1.0 + jnp.exp(-indicator_slope * (share - indicator_level)))
    alpha_ref[...] = alpha

    volume = [[None] * NX for _ in range(5)]
    for i in range(NX):
        for j in range(i + 1, NX):
            flux = two_point(nodes[i], nodes[j], 0)
            for c in range(5):
                for at, other in ((i, j), (j, i)):
                    term = (2.0 * DERIV[at, other]).astype(np.float32) * flux[c]
                    volume[c][at] = term if volume[c][at] is None else volume[c][at] + term
    for d, line in ((1, y), (2, z)):
        up, across, down = [line.coef(DERIV, k, 2.0) for k in (1, 2, 3)]
        for x in range(NX):
            near = two_point(nodes[x], [line.cyc(a, 1) for a in nodes[x]], d)
            far = two_point(nodes[x], [line.cyc(a, 2) for a in nodes[x]], d)
            for c in range(5):
                volume[c][x] = volume[c][x] + (
                    up * near[c] + down * line.cyc(near[c], 3) + across * far[c]
                )
    keep = 1.0 - alpha
    for c in range(5):
        for x in range(NX):
            vol_ref[c, x] = keep * volume[c][x]


def gravity_parts(field, halo, base, y, z):
    total = [[0.0] * NX for _ in range(4)]
    have = [c for c in range(4) if field[c] is not None]
    where = {c: base + i for i, c in enumerate(have)}

    for c, partner in ((0, 1), (1, 0)):
        if field[partner] is not None:
            for i in range(NX):
                terms = [float(2.0 * DERIV[i, j]) * field[partner][j] for j in range(NX) if DERIV[i, j] != 0.0]
                total[c][i] = total[c][i] + sum(terms[1:], terms[0])
    jumps = {}
    for c in have if halo is not None else ():
        jumps[c] = (halo.x_low(where[c]) - field[c][0], halo.x_high(where[c]) - field[c][NX - 1])
        for side, x in ((0, 0), (1, NX - 1)):
            total[c][x] = total[c][x] + 6.0 * jumps[c][side]
    for c, partner in ((0, 1), (1, 0)):
        if partner in jumps:
            total[c][0] = total[c][0] - 6.0 * jumps[partner][0]
            total[c][NX - 1] = total[c][NX - 1] + 6.0 * jumps[partner][1]
    for d, line in ((1, y), (2, z)):
        comp = 1 + d
        diag = line.coef(DERIV, 0, 2.0)
        coefs = [line.coef(DERIV, k, 2.0) for k in range(1, 4)]
        sign = line.by_node([-6.0, 0.0, 0.0, 6.0])
        for x in range(NX):
            for c, partner in ((0, comp), (comp, 0)):
                if field[partner] is not None:
                    value = field[partner][x]
                    term = diag * value
                    for k in range(1, 4):
                        term = term + coefs[k - 1] * line.cyc(value, k)
                    total[c][x] = total[c][x] + term
            gaps = {}
            for c in have:
                value = field[c][x]
                low, high = (value, value)
                if halo is not None:
                    low = halo.low(line.dim, where[c], x)
                    high = halo.high(line.dim, where[c], x)
                prev = jnp.where(line.lowest, low, line.roll(value, 1))
                after = jnp.where(line.highest, high, line.roll(value, -1))
                beside = jnp.where(line.is0, prev, jnp.where(line.is3, after, value))
                gaps[c] = beside - value
                total[c][x] = total[c][x] + 6.0 * gaps[c]
            for c, partner in ((0, comp), (comp, 0)):
                if partner in gaps:
                    total[c][x] = total[c][x] + sign * gaps[partner]
    return total


def advance(field, halo, base, y, z, source):
    total = gravity_parts(field, halo, base, y, z)
    phi_rate = [total[0][x] - coupling * source[x] for x in range(NX)]
    new = [[None] * NX for _ in range(4)]
    for x in range(NX):
        change = pseudo_step * phi_rate[x]
        new[0][x] = change if field[0] is None else field[0][x] + change
        for c in range(1, 4):
            if field[c] is None:
                new[c][x] = pseudo_step * total[c][x]
            else:
                new[c][x] = field[c][x] + pseudo_step * (total[c][x] - field[c][x])
    return (new, phi_rate)


def pack_kernel(u_ref, g_ref, u_out, g_out, *outs):
    u_out[...] = u_ref[...]
    g_out[...] = g_ref[...]
    comps = load(u_ref) + load(g_ref)
    xo, zo, yo, yp, zp, xp = outs
    pack_x(comps, xo, xp)
    pack_y(comps, yo, yp)
    pack_z(flat(comps), zo, zp)


def face_kernel(u_ref, g_ref, vol_ref, alpha_ref, *refs):
    halo = Halo(refs[:6])
    rate_ref, f1_ref, f2_ref, xo, yo, yp, xp = refs[6:]
    y, z = (Line(0), Line(1))
    u = load(u_ref)
    g = load(g_ref)
    alpha = alpha_ref[...]
    keep = 1.0 - alpha
    known = [primitive([u[c][x] for c in range(5)]) for x in range(NX)]
    total = load(vol_ref)

    own = [face_data([u[c][x] for c in range(5)], 0, known[x]) for x in range(NX)]
    below = face_data([halo.x_low(c) for c in range(5)], 0)
    above = face_data([halo.x_high(c) for c in range(5)], 0)
    chain = [below] + own + [above]
    faces = [interface(chain[i], chain[i + 1]) for i in range(NX + 1)]
    for x in range(NX):
        inner = alpha * float(1.0 / WEIGHTS[x])
        edge = inner + keep * 6.0
        low_coef = edge if x == 0 else inner
        high_coef = edge if x == NX - 1 else inner
        for c in range(5):
            total[c][x] = total[c][x] + (high_coef * faces[x + 1][c] - low_coef * faces[x][c])
    for d, line in ((1, y), (2, z)):
        inner = alpha * line.by_node(1.0 / WEIGHTS)
        low_coef = inner + keep * line.by_node([6.0, 0.0, 0.0, 0.0])
        high_coef = inner + keep * line.by_node([0.0, 0.0, 0.0, 6.0])
        for x in range(NX):
            mine = face_data([u[c][x] for c in range(5)], d, known[x])
            prev = face_data(
                [
                    jnp.where(line.lowest, halo.low(line.dim, c, x), line.roll(u[c][x], 1))
                    for c in range(5)
                ],
                d,
            )
            after = face_data(
                [jnp.where(line.highest, halo.high(line.dim, c, x), u[c][x]) for c in range(5)], d
            )
            face = interface(prev, mine)
            end = interface(mine, after)
            for c in range(5):
                following = jnp.where(line.highest, end[c], line.roll(face[c], -1))
                total[c][x] = total[c][x] + (high_coef * following - low_coef * face[c])
    rate = [[-2.0 * total[c][x] for x in range(NX)] for c in range(5)]
    for x in range(NX):
        for i in range(3):
            rate[1 + i][x] = rate[1 + i][x] - u[0][x] * g[1 + i][x]
        rate[4][x] = rate[4][x] - (
            u[1][x] * g[1][x] + u[2][x] * g[2][x] + u[3][x] * g[3][x]
        )
        for c in range(5):
            rate_ref[c, x] = rate[c][x]

    source = [u[0][x] - rho_offset for x in range(NX)]
    new, _ = advance(g, halo, 5, y, z, source)
    slope = [(-pseudo_step * coupling) * rate[0][x] for x in range(NX)]
    partial, _ = advance(new, None, 0, y, z, source)
    partial_slope, _ = advance([slope, None, None, None], None, 0, y, z, rate[0])
    f1 = new + [slope]
    f2 = partial + partial_slope
    for x in range(NX):
        for c in range(5):
            f1_ref[c, x] = f1[c][x]
        for c in range(8):
            f2_ref[c, x] = f2[c][x]
    pack_x(f1 + f2, xo, xp)
    pack_y(f1 + f2, yo, yp)


def face_terms(gap, d, sign):
    terms = [None if value is None else 6.0 * value for value in gap]
    for c, partner in ((0, 1 + d), (1 + d, 0)):
        if gap[partner] is not None:
            extra = sign * gap[partner]
            terms[c] = extra if terms[c] is None else terms[c] + extra
    return terms


def meet(field, gap, d, sign):
    terms = face_terms(gap[:4], d, sign) + face_terms([gap[4], None, None, None], d, sign)
    return [
        value if term is None else value + pseudo_step * term for value, term in zip(field, terms)
    ]


def ends(line):
    outer = line.lowest | line.highest
    sign = jnp.where(line.lowest, -6.0, jnp.where(line.highest, 6.0, 0.0)).astype(F32)
    return (outer, sign)


def at(field, x, first, count):
    return [field[first + c][x] for c in range(count)]


def join_kernel(f1_ref, f2_ref, xo, yo, yp, xp, f2_out, side_ref, row_ref, zo, eo, ep, zp):
    even = is_even()
    y = Line(0)
    f1, f2 = (load(f1_ref), load(f2_ref))
    sides = []
    for low, x, sign in ((True, 0, -6.0), (False, NX - 1, 6.0)):
        near, away = (xo, xp) if low else (xp, xo)
        side = [jnp.where(even[0], near[c], away[c]) for c in range(13)]
        gap = [side[c] - f1[c][x] for c in range(5)]
        for c, value in enumerate(meet(at(f2, x, 0, 8), gap, 0, sign)):
            f2[c][x] = value
        side[5:] = meet(side[5:], [-value for value in gap], 0, -sign)
        sides.append(side)
    outer, sign = ends(y)
    rows = [[None] * NX for _ in range(13)]
    for x in range(NX):
        for c in range(13):
            other, pair = (yo[c, pl.ds(x, 1), :], yp[c, pl.ds(x, 1), :])
            low = jnp.broadcast_to(jnp.where(even[1], other, pair), (NY, NZ))
            high = jnp.broadcast_to(jnp.where(even[1], pair, other), (NY, NZ))
            rows[c][x] = jnp.where(y.lowest, low, jnp.where(y.highest, high, 0.0))
        gap = [jnp.where(outer, rows[c][x] - f1[c][x], 0.0) for c in range(5)]
        for c, value in enumerate(meet(at(f2, x, 0, 8), gap, 1, sign)):
            f2[c][x] = value
        for c, value in enumerate(meet(at(rows, x, 5, 8), [-v for v in gap], 1, -sign)):
            rows[5 + c][x] = value
    for x in range(NX):
        for c in range(8):
            f2_out[c, x] = f2[c][x]
        for c in range(13):
            row_ref[c, x] = rows[c][x]
    for w, side in enumerate(sides):
        for c in range(13):
            side_ref[w, c] = side[c]
        for c in range(5):
            low, high = (side[c][0:1, :], side[c][NY - 1 : NY, :])
            eo[pl.ds(5 * w + c, 1), :] = jnp.where(even[1], low, high)
            ep[pl.ds(5 * w + c, 1), :] = jnp.where(even[1], high, low)
    pack_z(flat(f1 + f2) + sides[0][:5] + sides[1][:5] + flat(rows[:5]), zo, zp)


class Around:
    def __init__(self, sides, rows, columns):
        self.sides, self.rows, self.columns = (sides, rows, columns)

    def x_low(self, c):
        return self.sides[0][c]

    def x_high(self, c):
        return self.sides[1][c]

    def low(self, dim, c, x):
        return (self.rows, self.columns)[dim][c][x]

    high = low


def last_kernel(
    u_ref, rate_ref, fast_ref, f1_ref, f2_ref, side_ref, row_ref, zo, eo, ep, zp, next_ref, stat_ref
):
    even = is_even()
    y, z = (Line(0), Line(1))
    f1, f2, rows = (load(f1_ref), load(f2_ref), load(row_ref))
    sides = [[side_ref[w, c] for c in range(13)] for w in range(2)]
    z_other, z_pair = (zo[...], zp[...])
    z_low = jnp.where(even[2], z_other, z_pair)
    z_high = jnp.where(even[2], z_pair, z_other)
    z_outer, z_sign = ends(z)
    y_outer, y_sign = ends(y)

    def column(k):
        low = pltpu.roll(z_low, (NZ - k) % NZ, 1) if k else z_low
        return jnp.where(z.lowest, low, pltpu.roll(z_high, NZ - 1 - k, 1))

    def gaps(outer, beside, own):
        return [jnp.where(outer, b - o, 0.0) for b, o in zip(beside, own)]

    columns = [[column(c * NX + x) for x in range(NX)] for c in range(13)]
    for x in range(NX):
        gap = gaps(z_outer, at(columns, x, 0, 5), at(f1, x, 0, 5))
        for c, value in enumerate(meet(at(f2, x, 0, 8), gap, 2, z_sign)):
            f2[c][x] = value
        for c, value in enumerate(meet(at(columns, x, 5, 8), [-v for v in gap], 2, -z_sign)):
            columns[5 + c][x] = value
    for w, x, sign in ((0, 0, -6.0), (1, NX - 1, 6.0)):
        corner = []
        for c in range(5):
            other, pair = (eo[pl.ds(5 * w + c, 1), :], ep[pl.ds(5 * w + c, 1), :])
            low = jnp.broadcast_to(jnp.where(even[1], other, pair), (NY, NZ))
            high = jnp.broadcast_to(jnp.where(even[1], pair, other), (NY, NZ))
            corner.append(jnp.where(y.lowest, low, high))
        side = sides[w]
        beside = [column(13 * NX + 5 * w + c) for c in range(5)]
        side[5:] = meet(side[5:], gaps(z_outer, beside, side[:5]), 2, z_sign)
        side[5:] = meet(side[5:], gaps(y_outer, corner, side[:5]), 1, y_sign)
        gap = gaps(y_outer, corner, at(rows, x, 0, 5))
        for c, value in enumerate(meet(at(rows, x, 5, 8), gap, 0, sign)):
            rows[5 + c][x] = value
    for x in range(NX):
        beside = [column(13 * NX + 10 + c * NX + x) for c in range(5)]
        gap = gaps(z_outer & y_outer, beside, at(rows, x, 0, 5))
        for c, value in enumerate(meet(at(rows, x, 5, 8), gap, 2, z_sign)):
            rows[5 + c][x] = value

    around = Around([side[5:] for side in sides], rows[5:], columns[5:])
    source = [u_ref[0, x] - rho_offset for x in range(NX)]
    new, base_rate = advance(f2[:4], around, 0, y, z, source)
    slope, slope_rate = advance(f2[4:], around, 4, y, z, [rate_ref[0, x] for x in range(NX)])
    comps = new + slope
    for c in range(8):
        for x in range(NX):
            next_ref[c, x] = comps[c][x]
    weight = y.by_node(WEIGHTS) * z.by_node(WEIGHTS)

    def total(values):
        by_x = [float(WEIGHTS[x]) * values[x] for x in range(NX)]
        return jnp.sum(((by_x[0] + by_x[1]) + (by_x[2] + by_x[3])) * weight)

    stats = [
        jnp.max(fast_ref[...]),
        total([a * a for a in base_rate]),
        total([a * b for a, b in zip(base_rate, slope_rate)]),
        total([b * b for b in slope_rate]),
        total(base_rate),
        total(slope_rate),
        total(source),
    ]
    lane = lax.broadcasted_iota(jnp.int32, (1, NZ), 1)
    out = jnp.zeros((1, NZ), F32)
    for i, value in enumerate(stats):
        out = jnp.where(lane == i, value, out)
    stat_ref[...] = out


def finish_kernel(weight_total, u_ref, rate_ref, field_ref, stat_ref, grav_ref, source_ref, norm_ref):
    stat = stat_ref[...]
    part = [stat[:, i : i + 1] for i in range(7)]
    step = cfl_euler * elem_width / (7.0 * part[0])
    mean = part[6] * (1.0 / weight_total)
    shift = coupling * mean
    squares = (
        part[1]
        + step * (2.0 * part[2] + step * part[3])
        + shift * (2.0 * (part[4] + step * part[5]) + shift * weight_total)
    )
    norm_ref[...] = jnp.sqrt(jnp.maximum(squares, 0.0) * (1.0 / weight_total))
    raised = (ITERS * pseudo_step) * shift
    for x in range(NX):
        phi = field_ref[0, x] + step * field_ref[4, x] + raised
        grad = [field_ref[c, x] + step * field_ref[4 + c, x] for c in range(1, 4)]
        grav_ref[0, x] = phi
        for c in range(3):
            grav_ref[1 + c, x] = grad[c]
        rho = u_ref[0, x] + step * rate_ref[0, x]
        work = 0.0
        for c in range(3):
            source_ref[c, x] = -rho * grad[c]
            work = work + (u_ref[1 + c, x] + step * rate_ref[1 + c, x]) * grad[c]
        source_ref[3, x] = -work


def call(kernel, out_shape, flops, on_chip=True):
    def run(*args):
        if on_chip:
            args = [pltpu.with_memory_space_constraint(a, pltpu.VMEM) for a in args]
        return pl.pallas_call(
            kernel,
            in_specs=[pl.BlockSpec(memory_space=pltpu.VMEM)] * len(args),
            out_specs=[pl.BlockSpec(memory_space=pltpu.VMEM)] * len(out_shape),
            out_shape=out_shape,
            cost_estimate=pl.CostEstimate(flops=flops, bytes_accessed=400000, transcendentals=0),
        )(*args)

    return run


def pair_of(i, size):
    return i ^ 1


def other_of(i, size):
    return (i + 1 if i % 2 else i - 1) % size


ROUTES = {
    "state": (
        (GX, other_of),
        (GZ, other_of),
        ("gy", other_of),
        ("gy", pair_of),
        (GZ, pair_of),
        (GX, pair_of),
    ),
    "second": ((GX, other_of), ("gy", other_of), ("gy", pair_of), (GX, pair_of)),
    "third": ((GZ, other_of), ("gy", other_of), ("gy", pair_of), (GZ, pair_of)),
}


def exchange(messages, stage):
    received = []
    for message, (axis, partner) in zip(messages, ROUTES[stage]):
        size = lax.axis_size(axis)
        received.append(lax.ppermute(message, axis, [(a, partner(a, size)) for a in range(size)]))
    return received


def gather(stat, axis):
    lane = lax.broadcasted_iota(jnp.int32, (1, NZ), 1)
    every = lax.all_gather(stat, axis, tiled=True)
    return jnp.where(
        lane == 0, jnp.max(every, axis=0, keepdims=True), jnp.sum(every, axis=0, keepdims=True)
    )


def spread(stat):
    names = ("gx_0", "gx_1", "gy", "gz_0", "gz_1")
    sizes = [lax.axis_size(name) for name in names]
    ring = sizes[0] * sizes[3]
    pairs = []
    for at in np.ndindex(*sizes):
        a, core, b, c, e = at
        place = (a * sizes[3] + c + core * sizes[4] + e - (sizes[3] // 2 - 1)) % ring
        to = (place // sizes[3], core, b, place % sizes[3], e)
        pairs.append(
            (int(np.ravel_multi_index(at, sizes)), int(np.ravel_multi_index(to, sizes)))
        )
    return lax.ppermute(stat, names, pairs)


def over_all(stat):
    for axis in ("gx_0", "gx_1", "gy", "gz_1"):
        stat = gather(stat, axis)
    stat = spread(stat)
    for axis in ("gx_1", "gz_1"):
        stat = gather(stat, axis)
    return stat


def shape(*dims):
    return pltpu.VMEM(dims, F32)


def local(u, g):
    weight_total = float(
        8.0
        * (u.shape[1] // 4 * lax.axis_size(GX))
        * (u.shape[2] // 4 * lax.axis_size("gy"))
        * (u.shape[3] // 4 * lax.axis_size(GZ))
    )
    full = (NX, NY, NZ)
    tile = shape(NY, NZ)
    planes, rows = (shape(9, NY, NZ), shape(9, NX, NZ))
    u, g, *messages = call(
        pack_kernel,
        [shape(5, *full), shape(4, *full), planes, tile, rows, rows, tile, planes],
        10**5,
        False,
    )(u, g)
    received = exchange(messages, "state")
    vol, alpha, fast = call(volume_kernel, [shape(5, *full), tile, tile], 10**7)(u)
    planes, rows = (shape(13, NY, NZ), shape(13, NX, NZ))
    rate, f1, f2, *messages = call(
        face_kernel,
        [shape(5, *full), shape(5, *full), shape(8, *full), planes, rows, rows, planes],
        10**6,
    )(u, g, vol, alpha, *received)
    received = exchange(messages, "second")
    corners = shape(10, NZ)
    f2, sides, rows, *messages = call(
        join_kernel,
        [shape(8, *full), shape(2, 13, NY, NZ), shape(13, *full), tile, corners, corners, tile],
        10**6,
    )(f1, f2, *received)
    received = exchange(messages, "third")
    field, stat = call(last_kernel, [shape(8, *full), shape(1, NZ)], 10**6)(
        u, rate, fast, f1, f2, sides, rows, *received
    )
    stat = over_all(stat)
    gravity, gravity_source, norm = call(
        functools.partial(finish_kernel, weight_total),
        [jax.ShapeDtypeStruct((4, *full), F32)] * 2 + [jax.ShapeDtypeStruct((1, 1), F32)],
        10**5,
    )(u, rate, field, stat)
    return (rate, gravity, gravity_source, norm.reshape(()))


def solution(mesh):
    torus = Mesh(
        mesh.devices.reshape(4, 2, mesh.shape["gy"], 8, 4), ("gx_0", "gx_1", "gy", "gz_0", "gz_1")
    )
    placed = (P(None, GX, "gy", GZ), P(None, GX, "gy", GZ))
    return jax.shard_map(
        local,
        mesh=torus,
        in_specs=placed,
        out_specs=(P(None, GX, "gy", GZ), P(None, GX, "gy", GZ), P(None, GX, "gy", GZ), P()),
        check_vma=False,
    )
```

```python
import functools
import math

import jax
import jax.numpy as jnp
import numpy as np
from jax import lax
from jax.experimental import pallas as pl
from jax.experimental.pallas import tpu as pltpu
from jax.sharding import Mesh
from jax.sharding import PartitionSpec as P


ITERS = 3
GX = ("gx_0", "gx_1")
GZ = ("gz_0", "gz_1")

gamma_gas = 1.4
elem_width = 1.0
cfl_euler = 0.5
alpha_most = 0.5
indicator_level = 0.5 * 10.0 ** (-1.8 * 4.0**0.25)
indicator_slope = math.log((1.0 - 0.0001) / 0.0001) / indicator_level
coupling = 10.0
pseudo_step = 0.3 * elem_width / 7.0
rho_offset = 2.3

NX, NY, NZ = (4, 8, 128)
F32 = jnp.float32


def lgl_tables():
    points = np.array([-1.0, -1.0 / math.sqrt(5.0), 1.0 / math.sqrt(5.0), 1.0])
    weights = np.array([1.0, 5.0, 5.0, 1.0]) / 6.0
    barycentric = np.array(
        [1.0 / np.prod([points[a] - points[b] for b in range(4) if b != a]) for a in range(4)]
    )
    derivative = np.zeros((4, 4))
    for a in range(4):
        for b in range(4):
            if b != a:
                derivative[a, b] = barycentric[b] / barycentric[a] / (points[a] - points[b])
        derivative[a, a] = -np.sum(derivative[a])
    legendre = np.stack(
        [np.ones(4), points, 0.5 * (3.0 * points**2 - 1.0), 0.5 * (5.0 * points**3 - 3.0 * points)],
        axis=1,
    )
    legendre = legendre * np.sqrt((2.0 * np.arange(4) + 1.0) / 2.0)
    gram = np.sum(weights[:, None] * legendre * legendre, axis=0)
    modal_map = (legendre * weights[:, None]).T / gram[:, None]
    return (weights, derivative, modal_map)


WEIGHTS, DERIV, MODAL = lgl_tables()


class Line:
    def __init__(self, dim):
        self.dim = dim
        self.length = (NY, NZ)[dim]
        self.at = lax.broadcasted_iota(jnp.int32, (NY, NZ), dim)
        self.node = self.at % 4
        self.lowest = self.at == 0
        self.highest = self.at == self.length - 1
        self.is0 = self.node == 0
        self.is3 = self.node == 3

    def by_node(self, values):
        v = [float(item) for item in values]
        if v[1] == v[2] and v[0] == v[3]:
            return jnp.where(self.is0 | self.is3, v[0], v[1]).astype(F32)
        return jnp.where(
            self.node < 2,
            jnp.where(self.is0, v[0], v[1]),
            jnp.where(self.is3, v[3], v[2]),
        ).astype(F32)

    def roll(self, value, by):
        return pltpu.roll(value, by % self.length, self.dim)

    def cyc(self, value, k):
        return jnp.where(self.node < 4 - k, self.roll(value, -k), self.roll(value, 4 - k))

    def coef(self, matrix, k, scale=1.0):
        return self.by_node([scale * matrix[i, (i + k) % 4] for i in range(4)])

    def element_sum(self, value):
        value = value + self.cyc(value, 2)
        return value + self.cyc(value, 1)


def load(ref):
    return [[ref[c, x] for x in range(NX)] for c in range(ref.shape[0])]


def is_even():
    return [lax.axis_index(axis) % 2 == 0 for axis in ("gx_1", "gy", "gz_1")]


def pack_x(comps, other, pair):
    even = is_even()[0]
    for c, comp in enumerate(comps):
        other[c] = jnp.where(even, comp[0], comp[NX - 1])
        pair[c] = jnp.where(even, comp[NX - 1], comp[0])


def pack_y(comps, other, pair):
    even = is_even()[1]
    for c, comp in enumerate(comps):
        for x, tile in enumerate(comp):
            low, high = (tile[0:1, :], tile[NY - 1 : NY, :])
            other[c, pl.ds(x, 1), :] = jnp.where(even, low, high)
            pair[c, pl.ds(x, 1), :] = jnp.where(even, high, low)


def pack_z(tiles, other, pair):
    even = is_even()[2]
    lane = lax.broadcasted_iota(jnp.int32, (NY, NZ), 1)
    first = jnp.zeros((NY, NZ), F32)
    last = jnp.zeros((NY, NZ), F32)
    for k, tile in enumerate(tiles):
        here = lane == k
        first = jnp.where(here, pltpu.roll(tile, k, 1) if k else tile, first)
        last = jnp.where(here, pltpu.roll(tile, k + 1, 1), last)
    other[...] = jnp.where(even, first, last)
    pair[...] = jnp.where(even, last, first)


def flat(comps):
    return [tile for comp in comps for tile in comp]


class Halo:
    def __init__(self, refs):
        self.even = is_even()
        self.refs = refs
        zo, zp = (refs[1][...], refs[4][...])
        self.zlo = jnp.where(self.even[2], zo, zp)
        self.zhi = jnp.where(self.even[2], zp, zo)

    def x_low(self, c):
        return jnp.where(self.even[0], self.refs[0][c], self.refs[5][c])

    def x_high(self, c):
        return jnp.where(self.even[0], self.refs[5][c], self.refs[0][c])

    def row(self, c, x, pair, other):
        line = jnp.where(self.even[1], self.refs[pair][c, pl.ds(x, 1), :], self.refs[other][c, pl.ds(x, 1), :])
        return jnp.broadcast_to(line, (NY, NZ))

    def low(self, dim, c, x):
        if dim == 0:
            return self.row(c, x, 2, 3)
        k = c * NX + x
        return pltpu.roll(self.zlo, (NZ - k) % NZ, 1) if k else self.zlo

    def high(self, dim, c, x):
        if dim == 0:
            return self.row(c, x, 3, 2)
        k = c * NX + x
        return pltpu.roll(self.zhi, NZ - 1 - k, 1)


def log_mean(left, right):
    total = left + right
    gap = right - left
    slope = gap / total
    ratio_sq = slope * slope
    is_close = ratio_sq < 0.0001
    series = 2.0 + ratio_sq * (2.0 / 3.0 + ratio_sq * (2.0 / 5.0 + ratio_sq * (2.0 / 7.0)))
    top = jnp.where(is_close, total, gap)
    low = jnp.where(is_close, series, jnp.log(right / left))
    return top / low


def two_point(left, right, d):
    rho_mean = log_mean(left[0], right[0])
    inv_mean = left[4] * right[4] / log_mean(left[0] * right[4], right[0] * left[4])
    vel = [0.5 * (left[1 + i] + right[1 + i]) for i in range(3)]
    product = left[1] * right[1] + left[2] * right[2] + left[3] * right[3]
    mass = rho_mean * vel[d]
    flux = [mass] + [mass * vel[i] for i in range(3)]
    flux[1 + d] = flux[1 + d] + 0.5 * (left[4] + right[4])
    energy = mass * (0.5 * product + inv_mean * (1.0 / (gamma_gas - 1.0))) + 0.5 * (
        left[4] * right[1 + d] + right[4] * left[1 + d]
    )
    return flux + [energy]


def primitive(u):
    inv = 1.0 / u[0]
    vel = [u[1 + i] * inv for i in range(3)]
    kinetic = u[1] * vel[0] + u[2] * vel[1] + u[3] * vel[2]
    pressure = (gamma_gas - 1.0) * (u[4] - 0.5 * kinetic)
    return (vel, pressure, jnp.sqrt(gamma_gas * pressure * inv))


def face_data(u, d, known=None):
    vel, pressure, sound = known or primitive(u)
    normal = vel[d]
    flux = [u[1 + d]] + [u[1 + i] * normal for i in range(3)] + [(u[4] + pressure) * normal]
    flux[1 + d] = flux[1 + d] + pressure
    return (u, flux, jnp.abs(normal) + sound)


def interface(left, right):
    speed = jnp.maximum(left[2], right[2])
    return [
        0.5 * ((left[1][c] + right[1][c]) - speed * (right[0][c] - left[0][c])) for c in range(5)
    ]


def volume_kernel(u_ref, vol_ref, alpha_ref, fast_ref):
    y, z = (Line(0), Line(1))
    u = load(u_ref)
    known = [primitive([u[c][x] for c in range(5)]) for x in range(NX)]
    nodes = [[u[0][x]] + known[x][0] + [known[x][1]] for x in range(NX)]
    speed = [
        jnp.abs(known[x][0][0]) + jnp.abs(known[x][0][1]) + jnp.abs(known[x][0][2]) + 3.0 * known[x][2]
        for x in range(NX)
    ]
    fast_ref[...] = jnp.maximum(jnp.maximum(speed[0], speed[1]), jnp.maximum(speed[2], speed[3]))

    product = [u[0][x] * known[x][1] for x in range(NX)]
    coeffs = [sum(float(MODAL[a, i]) * product[i] for i in range(4)) for a in range(4)]
    for line in (y, z):
        modal = [line.coef(MODAL, k) for k in range(4)]
        coeffs = [
            modal[0] * value + sum(modal[k] * line.cyc(value, k) for k in range(1, 4))
            for value in coeffs
        ]
    energy = [value * value for value in coeffs]
    total = (energy[0] + energy[1]) + (energy[2] + energy[3])
    low = (energy[0] + energy[1]) + energy[2]
    high = energy[3] + jnp.where(y.is3 | z.is3, low, 0.0)
    share = z.element_sum(y.element_sum(high)) / z.element_sum(y.element_sum(total))
    alpha = alpha_most / (1.0 + jnp.exp(-indicator_slope * (share - indicator_level)))
    alpha_ref[...] = alpha

    volume = [[None] * NX for _ in range(5)]
    for i in range(NX):
        for j in range(i + 1, NX):
            flux = two_point(nodes[i], nodes[j], 0)
            for c in range(5):
                for at, other in ((i, j), (j, i)):
                    term = (2.0 * DERIV[at, other]).astype(np.float32) * flux[c]
                    volume[c][at] = term if volume[c][at] is None else volume[c][at] + term
    for d, line in ((1, y), (2, z)):
        up, across, down = [line.coef(DERIV, k, 2.0) for k in (1, 2, 3)]
        for x in range(NX):
            near = two_point(nodes[x], [line.cyc(a, 1) for a in nodes[x]], d)
            far = two_point(nodes[x], [line.cyc(a, 2) for a in nodes[x]], d)
            for c in range(5):
                volume[c][x] = volume[c][x] + (
                    up * near[c] + down * line.cyc(near[c], 3) + across * far[c]
                )
    keep = 1.0 - alpha
    for c in range(5):
        for x in range(NX):
            vol_ref[c, x] = keep * volume[c][x]


def gravity_parts(field, halo, base, y, z):
    total = [[0.0] * NX for _ in range(4)]
    have = [c for c in range(4) if field[c] is not None]
    where = {c: base + i for i, c in enumerate(have)}

    for c, partner in ((0, 1), (1, 0)):
        if field[partner] is not None:
            for i in range(NX):
                terms = [float(2.0 * DERIV[i, j]) * field[partner][j] for j in range(NX) if DERIV[i, j] != 0.0]
                total[c][i] = total[c][i] + sum(terms[1:], terms[0])
    jumps = {}
    for c in have if halo is not None else ():
        jumps[c] = (halo.x_low(where[c]) - field[c][0], halo.x_high(where[c]) - field[c][NX - 1])
        for side, x in ((0, 0), (1, NX - 1)):
            total[c][x] = total[c][x] + 6.0 * jumps[c][side]
    for c, partner in ((0, 1), (1, 0)):
        if partner in jumps:
            total[c][0] = total[c][0] - 6.0 * jumps[partner][0]
            total[c][NX - 1] = total[c][NX - 1] + 6.0 * jumps[partner][1]
    for d, line in ((1, y), (2, z)):
        comp = 1 + d
        diag = line.coef(DERIV, 0, 2.0)
        coefs = [line.coef(DERIV, k, 2.0) for k in range(1, 4)]
        sign = line.by_node([-6.0, 0.0, 0.0, 6.0])
        for x in range(NX):
            for c, partner in ((0, comp), (comp, 0)):
                if field[partner] is not None:
                    value = field[partner][x]
                    term = diag * value
                    for k in range(1, 4):
                        term = term + coefs[k - 1] * line.cyc(value, k)
                    total[c][x] = total[c][x] + term
            gaps = {}
            for c in have:
                value = field[c][x]
                low, high = (value, value)
                if halo is not None:
                    low = halo.low(line.dim, where[c], x)
                    high = halo.high(line.dim, where[c], x)
                prev = jnp.where(line.lowest, low, line.roll(value, 1))
                after = jnp.where(line.highest, high, line.roll(value, -1))
                beside = jnp.where(line.is0, prev, jnp.where(line.is3, after, value))
                gaps[c] = beside - value
                total[c][x] = total[c][x] + 6.0 * gaps[c]
            for c, partner in ((0, comp), (comp, 0)):
                if partner in gaps:
                    total[c][x] = total[c][x] + sign * gaps[partner]
    return total


def advance(field, halo, base, y, z, source):
    total = gravity_parts(field, halo, base, y, z)
    phi_rate = [total[0][x] - coupling * source[x] for x in range(NX)]
    new = [[None] * NX for _ in range(4)]
    for x in range(NX):
        change = pseudo_step * phi_rate[x]
        new[0][x] = change if field[0] is None else field[0][x] + change
        for c in range(1, 4):
            if field[c] is None:
                new[c][x] = pseudo_step * total[c][x]
            else:
                new[c][x] = field[c][x] + pseudo_step * (total[c][x] - field[c][x])
    return (new, phi_rate)


def pack_kernel(u_ref, g_ref, u_out, g_out, *outs):
    u_out[...] = u_ref[...]
    g_out[...] = g_ref[...]
    comps = load(u_ref) + load(g_ref)
    xo, zo, yo, yp, zp, xp = outs
    pack_x(comps, xo, xp)
    pack_y(comps, yo, yp)
    pack_z(flat(comps), zo, zp)


def face_kernel(u_ref, g_ref, vol_ref, alpha_ref, *refs):
    halo = Halo(refs[:6])
    rate_ref, f1_ref, f2_ref, xo, yo, yp, xp = refs[6:]
    y, z = (Line(0), Line(1))
    u = load(u_ref)
    g = load(g_ref)
    alpha = alpha_ref[...]
    keep = 1.0 - alpha
    known = [primitive([u[c][x] for c in range(5)]) for x in range(NX)]
    total = load(vol_ref)

    own = [face_data([u[c][x] for c in range(5)], 0, known[x]) for x in range(NX)]
    below = face_data([halo.x_low(c) for c in range(5)], 0)
    above = face_data([halo.x_high(c) for c in range(5)], 0)
    chain = [below] + own + [above]
    faces = [interface(chain[i], chain[i + 1]) for i in range(NX + 1)]
    for x in range(NX):
        inner = alpha * float(1.0 / WEIGHTS[x])
        edge = inner + keep * 6.0
        low_coef = edge if x == 0 else inner
        high_coef = edge if x == NX - 1 else inner
        for c in range(5):
            total[c][x] = total[c][x] + (high_coef * faces[x + 1][c] - low_coef * faces[x][c])
    for d, line in ((1, y), (2, z)):
        inner = alpha * line.by_node(1.0 / WEIGHTS)
        low_coef = inner + keep * line.by_node([6.0, 0.0, 0.0, 0.0])
        high_coef = inner + keep * line.by_node([0.0, 0.0, 0.0, 6.0])
        for x in range(NX):
            mine = face_data([u[c][x] for c in range(5)], d, known[x])
            prev = face_data(
                [
                    jnp.where(line.lowest, halo.low(line.dim, c, x), line.roll(u[c][x], 1))
                    for c in range(5)
                ],
                d,
            )
            after = face_data(
                [jnp.where(line.highest, halo.high(line.dim, c, x), u[c][x]) for c in range(5)], d
            )
            face = interface(prev, mine)
            end = interface(mine, after)
            for c in range(5):
                following = jnp.where(line.highest, end[c], line.roll(face[c], -1))
                total[c][x] = total[c][x] + (high_coef * following - low_coef * face[c])
    rate = [[-2.0 * total[c][x] for x in range(NX)] for c in range(5)]
    for x in range(NX):
        for i in range(3):
            rate[1 + i][x] = rate[1 + i][x] - u[0][x] * g[1 + i][x]
        rate[4][x] = rate[4][x] - (
            u[1][x] * g[1][x] + u[2][x] * g[2][x] + u[3][x] * g[3][x]
        )
        for c in range(5):
            rate_ref[c, x] = rate[c][x]

    source = [u[0][x] - rho_offset for x in range(NX)]
    new, _ = advance(g, halo, 5, y, z, source)
    slope = [(-pseudo_step * coupling) * rate[0][x] for x in range(NX)]
    partial, _ = advance(new, None, 0, y, z, source)
    partial_slope, _ = advance([slope, None, None, None], None, 0, y, z, rate[0])
    f1 = new + [slope]
    f2 = partial + partial_slope
    for x in range(NX):
        for c in range(5):
            f1_ref[c, x] = f1[c][x]
        for c in range(8):
            f2_ref[c, x] = f2[c][x]
    pack_x(f1 + f2, xo, xp)
    pack_y(f1 + f2, yo, yp)


def face_terms(gap, d, sign):
    terms = [None if value is None else 6.0 * value for value in gap]
    for c, partner in ((0, 1 + d), (1 + d, 0)):
        if gap[partner] is not None:
            extra = sign * gap[partner]
            terms[c] = extra if terms[c] is None else terms[c] + extra
    return terms


def meet(field, gap, d, sign):
    terms = face_terms(gap[:4], d, sign) + face_terms([gap[4], None, None, None], d, sign)
    return [
        value if term is None else value + pseudo_step * term for value, term in zip(field, terms)
    ]


def ends(line):
    outer = line.lowest | line.highest
    sign = jnp.where(line.lowest, -6.0, jnp.where(line.highest, 6.0, 0.0)).astype(F32)
    return (outer, sign)


def at(field, x, first, count):
    return [field[first + c][x] for c in range(count)]


def join_kernel(f1_ref, f2_ref, xo, yo, yp, xp, f2_out, side_ref, row_ref, eo, zo, ep, zp):
    even = is_even()
    y = Line(0)
    f1, f2 = (load(f1_ref), load(f2_ref))
    sides = []
    for low, x, sign in ((True, 0, -6.0), (False, NX - 1, 6.0)):
        near, away = (xo, xp) if low else (xp, xo)
        side = [jnp.where(even[0], near[c], away[c]) for c in range(13)]
        gap = [side[c] - f1[c][x] for c in range(5)]
        for c, value in enumerate(meet(at(f2, x, 0, 8), gap, 0, sign)):
            f2[c][x] = value
        side[5:] = meet(side[5:], [-value for value in gap], 0, -sign)
        sides.append(side)
    outer, sign = ends(y)
    rows = [[None] * NX for _ in range(13)]
    for x in range(NX):
        for c in range(13):
            other, pair = (yo[c, pl.ds(x, 1), :], yp[c, pl.ds(x, 1), :])
            low = jnp.broadcast_to(jnp.where(even[1], other, pair), (NY, NZ))
            high = jnp.broadcast_to(jnp.where(even[1], pair, other), (NY, NZ))
            rows[c][x] = jnp.where(y.lowest, low, jnp.where(y.highest, high, 0.0))
        gap = [jnp.where(outer, rows[c][x] - f1[c][x], 0.0) for c in range(5)]
        for c, value in enumerate(meet(at(f2, x, 0, 8), gap, 1, sign)):
            f2[c][x] = value
        for c, value in enumerate(meet(at(rows, x, 5, 8), [-v for v in gap], 1, -sign)):
            rows[5 + c][x] = value
    for x in range(NX):
        for c in range(8):
            f2_out[c, x] = f2[c][x]
        for c in range(13):
            row_ref[c, x] = rows[c][x]
    for w, side in enumerate(sides):
        for c in range(13):
            side_ref[w, c] = side[c]
        for c in range(5):
            low, high = (side[c][0:1, :], side[c][NY - 1 : NY, :])
            eo[pl.ds(5 * w + c, 1), :] = jnp.where(even[1], low, high)
            ep[pl.ds(5 * w + c, 1), :] = jnp.where(even[1], high, low)
    pack_z(flat(f1 + f2) + sides[0][:5] + sides[1][:5] + flat(rows[:5]), zo, zp)


class Around:
    def __init__(self, sides, rows, columns):
        self.sides, self.rows, self.columns = (sides, rows, columns)

    def x_low(self, c):
        return self.sides[0][c]

    def x_high(self, c):
        return self.sides[1][c]

    def low(self, dim, c, x):
        return (self.rows, self.columns)[dim][c][x]

    high = low


def last_kernel(
    u_ref, rate_ref, fast_ref, f1_ref, f2_ref, side_ref, row_ref, eo, zo, ep, zp, next_ref, stat_ref
):
    even = is_even()
    y, z = (Line(0), Line(1))
    f1, f2, rows = (load(f1_ref), load(f2_ref), load(row_ref))
    sides = [[side_ref[w, c] for c in range(13)] for w in range(2)]
    z_other, z_pair = (zo[...], zp[...])
    z_low = jnp.where(even[2], z_other, z_pair)
    z_high = jnp.where(even[2], z_pair, z_other)
    z_outer, z_sign = ends(z)
    y_outer, y_sign = ends(y)

    def column(k):
        low = pltpu.roll(z_low, (NZ - k) % NZ, 1) if k else z_low
        return jnp.where(z.lowest, low, pltpu.roll(z_high, NZ - 1 - k, 1))

    def gaps(outer, beside, own):
        return [jnp.where(outer, b - o, 0.0) for b, o in zip(beside, own)]

    columns = [[column(c * NX + x) for x in range(NX)] for c in range(13)]
    for x in range(NX):
        gap = gaps(z_outer, at(columns, x, 0, 5), at(f1, x, 0, 5))
        for c, value in enumerate(meet(at(f2, x, 0, 8), gap, 2, z_sign)):
            f2[c][x] = value
        for c, value in enumerate(meet(at(columns, x, 5, 8), [-v for v in gap], 2, -z_sign)):
            columns[5 + c][x] = value
    for w, x, sign in ((0, 0, -6.0), (1, NX - 1, 6.0)):
        corner = []
        for c in range(5):
            other, pair = (eo[pl.ds(5 * w + c, 1), :], ep[pl.ds(5 * w + c, 1), :])
            low = jnp.broadcast_to(jnp.where(even[1], other, pair), (NY, NZ))
            high = jnp.broadcast_to(jnp.where(even[1], pair, other), (NY, NZ))
            corner.append(jnp.where(y.lowest, low, high))
        side = sides[w]
        beside = [column(13 * NX + 5 * w + c) for c in range(5)]
        side[5:] = meet(side[5:], gaps(z_outer, beside, side[:5]), 2, z_sign)
        side[5:] = meet(side[5:], gaps(y_outer, corner, side[:5]), 1, y_sign)
        gap = gaps(y_outer, corner, at(rows, x, 0, 5))
        for c, value in enumerate(meet(at(rows, x, 5, 8), gap, 0, sign)):
            rows[5 + c][x] = value
    for x in range(NX):
        beside = [column(13 * NX + 10 + c * NX + x) for c in range(5)]
        gap = gaps(z_outer & y_outer, beside, at(rows, x, 0, 5))
        for c, value in enumerate(meet(at(rows, x, 5, 8), gap, 2, z_sign)):
            rows[5 + c][x] = value

    around = Around([side[5:] for side in sides], rows[5:], columns[5:])
    source = [u_ref[0, x] - rho_offset for x in range(NX)]
    new, base_rate = advance(f2[:4], around, 0, y, z, source)
    slope, slope_rate = advance(f2[4:], around, 4, y, z, [rate_ref[0, x] for x in range(NX)])
    comps = new + slope
    for c in range(8):
        for x in range(NX):
            next_ref[c, x] = comps[c][x]
    weight = y.by_node(WEIGHTS) * z.by_node(WEIGHTS)

    def total(values):
        by_x = [float(WEIGHTS[x]) * values[x] for x in range(NX)]
        return jnp.sum(((by_x[0] + by_x[1]) + (by_x[2] + by_x[3])) * weight)

    stats = [
        jnp.max(fast_ref[...]),
        total([a * a for a in base_rate]),
        total([a * b for a, b in zip(base_rate, slope_rate)]),
        total([b * b for b in slope_rate]),
        total(base_rate),
        total(slope_rate),
        total(source),
    ]
    lane = lax.broadcasted_iota(jnp.int32, (1, NZ), 1)
    out = jnp.zeros((1, NZ), F32)
    for i, value in enumerate(stats):
        out = jnp.where(lane == i, value, out)
    stat_ref[...] = out


def finish_kernel(weight_total, u_ref, rate_ref, field_ref, stat_ref, grav_ref, source_ref, norm_ref):
    stat = stat_ref[...]
    part = [stat[:, i : i + 1] for i in range(7)]
    step = cfl_euler * elem_width / (7.0 * part[0])
    mean = part[6] * (1.0 / weight_total)
    shift = coupling * mean
    squares = (
        part[1]
        + step * (2.0 * part[2] + step * part[3])
        + shift * (2.0 * (part[4] + step * part[5]) + shift * weight_total)
    )
    norm_ref[...] = jnp.sqrt(jnp.maximum(squares, 0.0) * (1.0 / weight_total))
    raised = (ITERS * pseudo_step) * shift
    for x in range(NX):
        phi = field_ref[0, x] + step * field_ref[4, x] + raised
        grad = [field_ref[c, x] + step * field_ref[4 + c, x] for c in range(1, 4)]
        grav_ref[0, x] = phi
        for c in range(3):
            grav_ref[1 + c, x] = grad[c]
        rho = u_ref[0, x] + step * rate_ref[0, x]
        work = 0.0
        for c in range(3):
            source_ref[c, x] = -rho * grad[c]
            work = work + (u_ref[1 + c, x] + step * rate_ref[1 + c, x]) * grad[c]
        source_ref[3, x] = -work


def call(kernel, out_shape, flops, on_chip=True):
    def run(*args):
        if on_chip:
            args = [pltpu.with_memory_space_constraint(a, pltpu.VMEM) for a in args]
        return pl.pallas_call(
            kernel,
            in_specs=[pl.BlockSpec(memory_space=pltpu.VMEM)] * len(args),
            out_specs=[pl.BlockSpec(memory_space=pltpu.VMEM)] * len(out_shape),
            out_shape=out_shape,
            cost_estimate=pl.CostEstimate(flops=flops, bytes_accessed=400000, transcendentals=0),
        )(*args)

    return run


def pair_of(i, size):
    return i ^ 1


def other_of(i, size):
    return (i + 1 if i % 2 else i - 1) % size


ROUTES = {
    "state": (
        ("gy", other_of),
        (GX, other_of),
        (GZ, other_of),
        ("gy", pair_of),
        (GZ, pair_of),
        (GX, pair_of),
    ),
    "second": ((GX, other_of), ("gy", other_of), ("gy", pair_of), (GX, pair_of)),
    "third": (("gy", other_of), (GZ, other_of), ("gy", pair_of), (GZ, pair_of)),
}


def exchange(messages, stage):
    received = []
    for message, (axis, partner) in zip(messages, ROUTES[stage]):
        size = lax.axis_size(axis)
        received.append(lax.ppermute(message, axis, [(a, partner(a, size)) for a in range(size)]))
    return received


def gather(stat, axis):
    lane = lax.broadcasted_iota(jnp.int32, (1, NZ), 1)
    every = lax.all_gather(stat, axis, tiled=True)
    return jnp.where(
        lane == 0, jnp.max(every, axis=0, keepdims=True), jnp.sum(every, axis=0, keepdims=True)
    )


def spread(stat):
    names = ("gx_0", "gx_1", "gy", "gz_0", "gz_1")
    sizes = [lax.axis_size(name) for name in names]
    ring = sizes[0] * sizes[3]
    pairs = []
    for at in np.ndindex(*sizes):
        a, core, b, c, e = at
        place = (a * sizes[3] + c + core * sizes[4] + e - (sizes[3] // 2 - 1)) % ring
        to = (place // sizes[3], core, b, place % sizes[3], e)
        pairs.append(
            (int(np.ravel_multi_index(at, sizes)), int(np.ravel_multi_index(to, sizes)))
        )
    return lax.ppermute(stat, names, pairs)


def over_all(stat):
    for axis in ("gx_0", "gx_1", "gy", "gz_1"):
        stat = gather(stat, axis)
    stat = spread(stat)
    for axis in ("gx_1", "gz_1"):
        stat = gather(stat, axis)
    return stat


def shape(*dims):
    return pltpu.VMEM(dims, F32)


def local(u, g):
    weight_total = float(
        8.0
        * (u.shape[1] // 4 * lax.axis_size(GX))
        * (u.shape[2] // 4 * lax.axis_size("gy"))
        * (u.shape[3] // 4 * lax.axis_size(GZ))
    )
    full = (NX, NY, NZ)
    tile = shape(NY, NZ)
    planes, rows = (shape(9, NY, NZ), shape(9, NX, NZ))
    u, g, *messages = call(
        pack_kernel,
        [shape(5, *full), shape(4, *full), planes, tile, rows, rows, tile, planes],
        10**5,
        False,
    )(u, g)
    xo, zo, yo, *rest = messages
    yo, xo, zo, *rest = exchange([yo, xo, zo, *rest], "state")
    received = [xo, zo, yo, *rest]
    vol, alpha, fast = call(volume_kernel, [shape(5, *full), tile, tile], 10**7)(u)
    planes, rows = (shape(13, NY, NZ), shape(13, NX, NZ))
    rate, f1, f2, *messages = call(
        face_kernel,
        [shape(5, *full), shape(5, *full), shape(8, *full), planes, rows, rows, planes],
        10**6,
    )(u, g, vol, alpha, *received)
    received = exchange(messages, "second")
    corners = shape(10, NZ)
    f2, sides, rows, *messages = call(
        join_kernel,
        [shape(8, *full), shape(2, 13, NY, NZ), shape(13, *full), corners, tile, corners, tile],
        10**6,
    )(f1, f2, *received)
    received = exchange(messages, "third")
    field, stat = call(last_kernel, [shape(8, *full), shape(1, NZ)], 10**6)(
        u, rate, fast, f1, f2, sides, rows, *received
    )
    stat = over_all(stat)
    gravity, gravity_source, norm = call(
        functools.partial(finish_kernel, weight_total),
        [jax.ShapeDtypeStruct((4, *full), F32)] * 2 + [jax.ShapeDtypeStruct((1, 1), F32)],
        10**5,
    )(u, rate, field, stat)
    return (rate, gravity, gravity_source, norm.reshape(()))


def solution(mesh):
    torus = Mesh(
        mesh.devices.reshape(4, 2, mesh.shape["gy"], 8, 4), ("gx_0", "gx_1", "gy", "gz_0", "gz_1")
    )
    placed = (P(None, GX, "gy", GZ), P(None, GX, "gy", GZ))
    return jax.shard_map(
        local,
        mesh=torus,
        in_specs=placed,
        out_specs=(P(None, GX, "gy", GZ), P(None, GX, "gy", GZ), P(None, GX, "gy", GZ), P()),
        check_vma=False,
    )
```

```python
import functools
import math

import jax
import jax.numpy as jnp
import numpy as np
from jax import lax
from jax.experimental import pallas as pl
from jax.experimental.pallas import tpu as pltpu
from jax.sharding import Mesh
from jax.sharding import PartitionSpec as P


ITERS = 3
GX = ("gx_0", "gx_1")
GZ = ("gz_0", "gz_1")

gamma_gas = 1.4
elem_width = 1.0
cfl_euler = 0.5
alpha_most = 0.5
indicator_level = 0.5 * 10.0 ** (-1.8 * 4.0**0.25)
indicator_slope = math.log((1.0 - 0.0001) / 0.0001) / indicator_level
coupling = 10.0
pseudo_step = 0.3 * elem_width / 7.0
rho_offset = 2.3

NX, NY, NZ = (4, 8, 128)
F32 = jnp.float32


def lgl_tables():
    points = np.array([-1.0, -1.0 / math.sqrt(5.0), 1.0 / math.sqrt(5.0), 1.0])
    weights = np.array([1.0, 5.0, 5.0, 1.0]) / 6.0
    barycentric = np.array(
        [1.0 / np.prod([points[a] - points[b] for b in range(4) if b != a]) for a in range(4)]
    )
    derivative = np.zeros((4, 4))
    for a in range(4):
        for b in range(4):
            if b != a:
                derivative[a, b] = barycentric[b] / barycentric[a] / (points[a] - points[b])
        derivative[a, a] = -np.sum(derivative[a])
    legendre = np.stack(
        [np.ones(4), points, 0.5 * (3.0 * points**2 - 1.0), 0.5 * (5.0 * points**3 - 3.0 * points)],
        axis=1,
    )
    legendre = legendre * np.sqrt((2.0 * np.arange(4) + 1.0) / 2.0)
    gram = np.sum(weights[:, None] * legendre * legendre, axis=0)
    modal_map = (legendre * weights[:, None]).T / gram[:, None]
    return (weights, derivative, modal_map)


WEIGHTS, DERIV, MODAL = lgl_tables()


class Line:
    def __init__(self, dim):
        self.dim = dim
        self.length = (NY, NZ)[dim]
        self.at = lax.broadcasted_iota(jnp.int32, (NY, NZ), dim)
        self.node = self.at % 4
        self.lowest = self.at == 0
        self.highest = self.at == self.length - 1
        self.is0 = self.node == 0
        self.is3 = self.node == 3

    def by_node(self, values):
        v = [float(item) for item in values]
        if v[1] == v[2] and v[0] == v[3]:
            return jnp.where(self.is0 | self.is3, v[0], v[1]).astype(F32)
        return jnp.where(
            self.node < 2,
            jnp.where(self.is0, v[0], v[1]),
            jnp.where(self.is3, v[3], v[2]),
        ).astype(F32)

    def roll(self, value, by):
        return pltpu.roll(value, by % self.length, self.dim)

    def cyc(self, value, k):
        return jnp.where(self.node < 4 - k, self.roll(value, -k), self.roll(value, 4 - k))

    def coef(self, matrix, k, scale=1.0):
        return self.by_node([scale * matrix[i, (i + k) % 4] for i in range(4)])

    def element_sum(self, value):
        value = value + self.cyc(value, 2)
        return value + self.cyc(value, 1)


def load(ref):
    return [[ref[c, x] for x in range(NX)] for c in range(ref.shape[0])]


def is_even():
    return [lax.axis_index(axis) % 2 == 0 for axis in ("gx_1", "gy", "gz_1")]


def pack_x(comps, other, pair):
    even = is_even()[0]
    for c, comp in enumerate(comps):
        other[c] = jnp.where(even, comp[0], comp[NX - 1])
        pair[c] = jnp.where(even, comp[NX - 1], comp[0])


def pack_y(comps, other, pair):
    even = is_even()[1]
    for c, comp in enumerate(comps):
        for x, tile in enumerate(comp):
            low, high = (tile[0:1, :], tile[NY - 1 : NY, :])
            other[c, pl.ds(x, 1), :] = jnp.where(even, low, high)
            pair[c, pl.ds(x, 1), :] = jnp.where(even, high, low)


def pack_z(tiles, other, pair):
    even = is_even()[2]
    lane = lax.broadcasted_iota(jnp.int32, (NY, NZ), 1)
    first = jnp.zeros((NY, NZ), F32)
    last = jnp.zeros((NY, NZ), F32)
    for k, tile in enumerate(tiles):
        here = lane == k
        first = jnp.where(here, pltpu.roll(tile, k, 1) if k else tile, first)
        last = jnp.where(here, pltpu.roll(tile, k + 1, 1), last)
    other[...] = jnp.where(even, first, last)
    pair[...] = jnp.where(even, last, first)


def flat(comps):
    return [tile for comp in comps for tile in comp]


class Halo:
    def __init__(self, refs):
        self.even = is_even()
        self.refs = refs
        zo, zp = (refs[1][...], refs[4][...])
        self.zlo = jnp.where(self.even[2], zo, zp)
        self.zhi = jnp.where(self.even[2], zp, zo)

    def x_low(self, c):
        return jnp.where(self.even[0], self.refs[0][c], self.refs[5][c])

    def x_high(self, c):
        return jnp.where(self.even[0], self.refs[5][c], self.refs[0][c])

    def row(self, c, x, pair, other):
        line = jnp.where(self.even[1], self.refs[pair][c, pl.ds(x, 1), :], self.refs[other][c, pl.ds(x, 1), :])
        return jnp.broadcast_to(line, (NY, NZ))

    def low(self, dim, c, x):
        if dim == 0:
            return self.row(c, x, 2, 3)
        k = c * NX + x
        return pltpu.roll(self.zlo, (NZ - k) % NZ, 1) if k else self.zlo

    def high(self, dim, c, x):
        if dim == 0:
            return self.row(c, x, 3, 2)
        k = c * NX + x
        return pltpu.roll(self.zhi, NZ - 1 - k, 1)


def log_mean(left, right):
    total = left + right
    gap = right - left
    slope = gap / total
    ratio_sq = slope * slope
    is_close = ratio_sq < 0.0001
    series = 2.0 + ratio_sq * (2.0 / 3.0 + ratio_sq * (2.0 / 5.0 + ratio_sq * (2.0 / 7.0)))
    top = jnp.where(is_close, total, gap)
    low = jnp.where(is_close, series, jnp.log(right / left))
    return top / low


def two_point(left, right, d):
    rho_mean = log_mean(left[0], right[0])
    inv_mean = left[4] * right[4] / log_mean(left[0] * right[4], right[0] * left[4])
    vel = [0.5 * (left[1 + i] + right[1 + i]) for i in range(3)]
    product = left[1] * right[1] + left[2] * right[2] + left[3] * right[3]
    mass = rho_mean * vel[d]
    flux = [mass] + [mass * vel[i] for i in range(3)]
    flux[1 + d] = flux[1 + d] + 0.5 * (left[4] + right[4])
    energy = mass * (0.5 * product + inv_mean * (1.0 / (gamma_gas - 1.0))) + 0.5 * (
        left[4] * right[1 + d] + right[4] * left[1 + d]
    )
    return flux + [energy]


def primitive(u):
    inv = 1.0 / u[0]
    vel = [u[1 + i] * inv for i in range(3)]
    kinetic = u[1] * vel[0] + u[2] * vel[1] + u[3] * vel[2]
    pressure = (gamma_gas - 1.0) * (u[4] - 0.5 * kinetic)
    return (vel, pressure, jnp.sqrt(gamma_gas * pressure * inv))


def face_data(u, d, known=None):
    vel, pressure, sound = known or primitive(u)
    normal = vel[d]
    flux = [u[1 + d]] + [u[1 + i] * normal for i in range(3)] + [(u[4] + pressure) * normal]
    flux[1 + d] = flux[1 + d] + pressure
    return (u, flux, jnp.abs(normal) + sound)


def interface(left, right):
    speed = jnp.maximum(left[2], right[2])
    return [
        0.5 * ((left[1][c] + right[1][c]) - speed * (right[0][c] - left[0][c])) for c in range(5)
    ]


def volume_kernel(u_ref, vol_ref, alpha_ref, fast_ref):
    y, z = (Line(0), Line(1))
    u = load(u_ref)
    known = [primitive([u[c][x] for c in range(5)]) for x in range(NX)]
    nodes = [[u[0][x]] + known[x][0] + [known[x][1]] for x in range(NX)]
    speed = [
        jnp.abs(known[x][0][0]) + jnp.abs(known[x][0][1]) + jnp.abs(known[x][0][2]) + 3.0 * known[x][2]
        for x in range(NX)
    ]
    fast_ref[...] = jnp.maximum(jnp.maximum(speed[0], speed[1]), jnp.maximum(speed[2], speed[3]))

    product = [u[0][x] * known[x][1] for x in range(NX)]
    coeffs = [sum(float(MODAL[a, i]) * product[i] for i in range(4)) for a in range(4)]
    for line in (y, z):
        modal = [line.coef(MODAL, k) for k in range(4)]
        coeffs = [
            modal[0] * value + sum(modal[k] * line.cyc(value, k) for k in range(1, 4))
            for value in coeffs
        ]
    energy = [value * value for value in coeffs]
    total = (energy[0] + energy[1]) + (energy[2] + energy[3])
    low = (energy[0] + energy[1]) + energy[2]
    high = energy[3] + jnp.where(y.is3 | z.is3, low, 0.0)
    share = z.element_sum(y.element_sum(high)) / z.element_sum(y.element_sum(total))
    alpha = alpha_most / (1.0 + jnp.exp(-indicator_slope * (share - indicator_level)))
    alpha_ref[...] = alpha

    volume = [[None] * NX for _ in range(5)]
    for i in range(NX):
        for j in range(i + 1, NX):
            flux = two_point(nodes[i], nodes[j], 0)
            for c in range(5):
                for at, other in ((i, j), (j, i)):
                    term = (2.0 * DERIV[at, other]).astype(np.float32) * flux[c]
                    volume[c][at] = term if volume[c][at] is None else volume[c][at] + term
    for d, line in ((1, y), (2, z)):
        up, across, down = [line.coef(DERIV, k, 2.0) for k in (1, 2, 3)]
        for x in range(NX):
            near = two_point(nodes[x], [line.cyc(a, 1) for a in nodes[x]], d)
            far = two_point(nodes[x], [line.cyc(a, 2) for a in nodes[x]], d)
            for c in range(5):
                volume[c][x] = volume[c][x] + (
                    up * near[c] + down * line.cyc(near[c], 3) + across * far[c]
                )
    keep = 1.0 - alpha
    for c in range(5):
        for x in range(NX):
            vol_ref[c, x] = keep * volume[c][x]


def gravity_parts(field, halo, base, y, z):
    total = [[0.0] * NX for _ in range(4)]
    have = [c for c in range(4) if field[c] is not None]
    where = {c: base + i for i, c in enumerate(have)}

    for c, partner in ((0, 1), (1, 0)):
        if field[partner] is not None:
            for i in range(NX):
                terms = [float(2.0 * DERIV[i, j]) * field[partner][j] for j in range(NX) if DERIV[i, j] != 0.0]
                total[c][i] = total[c][i] + sum(terms[1:], terms[0])
    jumps = {}
    for c in have if halo is not None else ():
        jumps[c] = (halo.x_low(where[c]) - field[c][0], halo.x_high(where[c]) - field[c][NX - 1])
        for side, x in ((0, 0), (1, NX - 1)):
            total[c][x] = total[c][x] + 6.0 * jumps[c][side]
    for c, partner in ((0, 1), (1, 0)):
        if partner in jumps:
            total[c][0] = total[c][0] - 6.0 * jumps[partner][0]
            total[c][NX - 1] = total[c][NX - 1] + 6.0 * jumps[partner][1]
    for d, line in ((1, y), (2, z)):
        comp = 1 + d
        diag = line.coef(DERIV, 0, 2.0)
        coefs = [line.coef(DERIV, k, 2.0) for k in range(1, 4)]
        sign = line.by_node([-6.0, 0.0, 0.0, 6.0])
        for x in range(NX):
            for c, partner in ((0, comp), (comp, 0)):
                if field[partner] is not None:
                    value = field[partner][x]
                    term = diag * value
                    for k in range(1, 4):
                        term = term + coefs[k - 1] * line.cyc(value, k)
                    total[c][x] = total[c][x] + term
            gaps = {}
            for c in have:
                value = field[c][x]
                low, high = (value, value)
                if halo is not None:
                    low = halo.low(line.dim, where[c], x)
                    high = halo.high(line.dim, where[c], x)
                prev = jnp.where(line.lowest, low, line.roll(value, 1))
                after = jnp.where(line.highest, high, line.roll(value, -1))
                beside = jnp.where(line.is0, prev, jnp.where(line.is3, after, value))
                gaps[c] = beside - value
                total[c][x] = total[c][x] + 6.0 * gaps[c]
            for c, partner in ((0, comp), (comp, 0)):
                if partner in gaps:
                    total[c][x] = total[c][x] + sign * gaps[partner]
    return total


def advance(field, halo, base, y, z, source):
    total = gravity_parts(field, halo, base, y, z)
    phi_rate = [total[0][x] - coupling * source[x] for x in range(NX)]
    new = [[None] * NX for _ in range(4)]
    for x in range(NX):
        change = pseudo_step * phi_rate[x]
        new[0][x] = change if field[0] is None else field[0][x] + change
        for c in range(1, 4):
            if field[c] is None:
                new[c][x] = pseudo_step * total[c][x]
            else:
                new[c][x] = field[c][x] + pseudo_step * (total[c][x] - field[c][x])
    return (new, phi_rate)


def pack_kernel(u_ref, g_ref, u_out, g_out, *outs):
    u_out[...] = u_ref[...]
    g_out[...] = g_ref[...]
    comps = load(u_ref) + load(g_ref)
    xo, zo, yo, yp, zp, xp = outs
    pack_x(comps, xo, xp)
    pack_y(comps, yo, yp)
    pack_z(flat(comps), zo, zp)


def face_kernel(u_ref, g_ref, vol_ref, alpha_ref, *refs):
    halo = Halo(refs[:6])
    rate_ref, f1_ref, f2_ref, xo, yo, yp, xp = refs[6:]
    y, z = (Line(0), Line(1))
    u = load(u_ref)
    g = load(g_ref)
    alpha = alpha_ref[...]
    keep = 1.0 - alpha
    known = [primitive([u[c][x] for c in range(5)]) for x in range(NX)]
    total = load(vol_ref)

    own = [face_data([u[c][x] for c in range(5)], 0, known[x]) for x in range(NX)]
    below = face_data([halo.x_low(c) for c in range(5)], 0)
    above = face_data([halo.x_high(c) for c in range(5)], 0)
    chain = [below] + own + [above]
    faces = [interface(chain[i], chain[i + 1]) for i in range(NX + 1)]
    for x in range(NX):
        inner = alpha * float(1.0 / WEIGHTS[x])
        edge = inner + keep * 6.0
        low_coef = edge if x == 0 else inner
        high_coef = edge if x == NX - 1 else inner
        for c in range(5):
            total[c][x] = total[c][x] + (high_coef * faces[x + 1][c] - low_coef * faces[x][c])
    for d, line in ((1, y), (2, z)):
        inner = alpha * line.by_node(1.0 / WEIGHTS)
        low_coef = inner + keep * line.by_node([6.0, 0.0, 0.0, 0.0])
        high_coef = inner + keep * line.by_node([0.0, 0.0, 0.0, 6.0])
        for x in range(NX):
            mine = face_data([u[c][x] for c in range(5)], d, known[x])
            prev = face_data(
                [
                    jnp.where(line.lowest, halo.low(line.dim, c, x), line.roll(u[c][x], 1))
                    for c in range(5)
                ],
                d,
            )
            after = face_data(
                [jnp.where(line.highest, halo.high(line.dim, c, x), u[c][x]) for c in range(5)], d
            )
            face = interface(prev, mine)
            end = interface(mine, after)
            for c in range(5):
                following = jnp.where(line.highest, end[c], line.roll(face[c], -1))
                total[c][x] = total[c][x] + (high_coef * following - low_coef * face[c])
    rate = [[-2.0 * total[c][x] for x in range(NX)] for c in range(5)]
    for x in range(NX):
        for i in range(3):
            rate[1 + i][x] = rate[1 + i][x] - u[0][x] * g[1 + i][x]
        rate[4][x] = rate[4][x] - (
            u[1][x] * g[1][x] + u[2][x] * g[2][x] + u[3][x] * g[3][x]
        )
        for c in range(5):
            rate_ref[c, x] = rate[c][x]

    source = [u[0][x] - rho_offset for x in range(NX)]
    new, _ = advance(g, halo, 5, y, z, source)
    slope = [(-pseudo_step * coupling) * rate[0][x] for x in range(NX)]
    partial, _ = advance(new, None, 0, y, z, source)
    partial_slope, _ = advance([slope, None, None, None], None, 0, y, z, rate[0])
    f1 = new + [slope]
    f2 = partial + partial_slope
    for x in range(NX):
        for c in range(5):
            f1_ref[c, x] = f1[c][x]
        for c in range(8):
            f2_ref[c, x] = f2[c][x]
    pack_x(f1 + f2, xo, xp)
    pack_y(f1 + f2, yo, yp)


def face_terms(gap, d, sign):
    terms = [None if value is None else 6.0 * value for value in gap]
    for c, partner in ((0, 1 + d), (1 + d, 0)):
        if gap[partner] is not None:
            extra = sign * gap[partner]
            terms[c] = extra if terms[c] is None else terms[c] + extra
    return terms


def meet(field, gap, d, sign):
    terms = face_terms(gap[:4], d, sign) + face_terms([gap[4], None, None, None], d, sign)
    return [
        value if term is None else value + pseudo_step * term for value, term in zip(field, terms)
    ]


def ends(line):
    outer = line.lowest | line.highest
    sign = jnp.where(line.lowest, -6.0, jnp.where(line.highest, 6.0, 0.0)).astype(F32)
    return (outer, sign)


def at(field, x, first, count):
    return [field[first + c][x] for c in range(count)]


def side_kernel(f1_ref, f2_ref, xo, xp, f2_out, side_ref, eo, ep):
    even = is_even()
    f1, f2 = (load(f1_ref), load(f2_ref))
    sides = []
    for low, x, sign in ((True, 0, -6.0), (False, NX - 1, 6.0)):
        near, away = (xo, xp) if low else (xp, xo)
        side = [jnp.where(even[0], near[c], away[c]) for c in range(13)]
        gap = [side[c] - f1[c][x] for c in range(5)]
        for c, value in enumerate(meet(at(f2, x, 0, 8), gap, 0, sign)):
            f2[c][x] = value
        side[5:] = meet(side[5:], [-value for value in gap], 0, -sign)
        sides.append(side)
    for x in range(NX):
        for c in range(8):
            f2_out[c, x] = f2[c][x]
    for w, side in enumerate(sides):
        for c in range(13):
            side_ref[w, c] = side[c]
        for c in range(5):
            low, high = (side[c][0:1, :], side[c][NY - 1 : NY, :])
            eo[pl.ds(5 * w + c, 1), :] = jnp.where(even[1], low, high)
            ep[pl.ds(5 * w + c, 1), :] = jnp.where(even[1], high, low)


def join_kernel(f1_ref, f2_ref, side_ref, yo, yp, f2_out, row_ref, zo, zp):
    even = is_even()
    y = Line(0)
    f1, f2 = (load(f1_ref), load(f2_ref))
    outer, sign = ends(y)
    rows = [[None] * NX for _ in range(13)]
    for x in range(NX):
        for c in range(13):
            other, pair = (yo[c, pl.ds(x, 1), :], yp[c, pl.ds(x, 1), :])
            low = jnp.broadcast_to(jnp.where(even[1], other, pair), (NY, NZ))
            high = jnp.broadcast_to(jnp.where(even[1], pair, other), (NY, NZ))
            rows[c][x] = jnp.where(y.lowest, low, jnp.where(y.highest, high, 0.0))
        gap = [jnp.where(outer, rows[c][x] - f1[c][x], 0.0) for c in range(5)]
        for c, value in enumerate(meet(at(f2, x, 0, 8), gap, 1, sign)):
            f2[c][x] = value
        for c, value in enumerate(meet(at(rows, x, 5, 8), [-v for v in gap], 1, -sign)):
            rows[5 + c][x] = value
    for x in range(NX):
        for c in range(8):
            f2_out[c, x] = f2[c][x]
        for c in range(13):
            row_ref[c, x] = rows[c][x]
    sides = [side_ref[w, c] for w in range(2) for c in range(5)]
    pack_z(flat(f1 + f2) + sides + flat(rows[:5]), zo, zp)


class Around:
    def __init__(self, sides, rows, columns):
        self.sides, self.rows, self.columns = (sides, rows, columns)

    def x_low(self, c):
        return self.sides[0][c]

    def x_high(self, c):
        return self.sides[1][c]

    def low(self, dim, c, x):
        return (self.rows, self.columns)[dim][c][x]

    high = low


def last_kernel(
    u_ref, rate_ref, fast_ref, f1_ref, f2_ref, side_ref, row_ref, eo, ep, zo, zp, next_ref, stat_ref
):
    even = is_even()
    y, z = (Line(0), Line(1))
    f1, f2, rows = (load(f1_ref), load(f2_ref), load(row_ref))
    sides = [[side_ref[w, c] for c in range(13)] for w in range(2)]
    z_other, z_pair = (zo[...], zp[...])
    z_low = jnp.where(even[2], z_other, z_pair)
    z_high = jnp.where(even[2], z_pair, z_other)
    z_outer, z_sign = ends(z)
    y_outer, y_sign = ends(y)

    def column(k):
        low = pltpu.roll(z_low, (NZ - k) % NZ, 1) if k else z_low
        return jnp.where(z.lowest, low, pltpu.roll(z_high, NZ - 1 - k, 1))

    def gaps(outer, beside, own):
        return [jnp.where(outer, b - o, 0.0) for b, o in zip(beside, own)]

    columns = [[column(c * NX + x) for x in range(NX)] for c in range(13)]
    for x in range(NX):
        gap = gaps(z_outer, at(columns, x, 0, 5), at(f1, x, 0, 5))
        for c, value in enumerate(meet(at(f2, x, 0, 8), gap, 2, z_sign)):
            f2[c][x] = value
        for c, value in enumerate(meet(at(columns, x, 5, 8), [-v for v in gap], 2, -z_sign)):
            columns[5 + c][x] = value
    for w, x, sign in ((0, 0, -6.0), (1, NX - 1, 6.0)):
        corner = []
        for c in range(5):
            other, pair = (eo[pl.ds(5 * w + c, 1), :], ep[pl.ds(5 * w + c, 1), :])
            low = jnp.broadcast_to(jnp.where(even[1], other, pair), (NY, NZ))
            high = jnp.broadcast_to(jnp.where(even[1], pair, other), (NY, NZ))
            corner.append(jnp.where(y.lowest, low, high))
        side = sides[w]
        beside = [column(13 * NX + 5 * w + c) for c in range(5)]
        side[5:] = meet(side[5:], gaps(z_outer, beside, side[:5]), 2, z_sign)
        side[5:] = meet(side[5:], gaps(y_outer, corner, side[:5]), 1, y_sign)
        gap = gaps(y_outer, corner, at(rows, x, 0, 5))
        for c, value in enumerate(meet(at(rows, x, 5, 8), gap, 0, sign)):
            rows[5 + c][x] = value
    for x in range(NX):
        beside = [column(13 * NX + 10 + c * NX + x) for c in range(5)]
        gap = gaps(z_outer & y_outer, beside, at(rows, x, 0, 5))
        for c, value in enumerate(meet(at(rows, x, 5, 8), gap, 2, z_sign)):
            rows[5 + c][x] = value

    around = Around([side[5:] for side in sides], rows[5:], columns[5:])
    source = [u_ref[0, x] - rho_offset for x in range(NX)]
    new, base_rate = advance(f2[:4], around, 0, y, z, source)
    slope, slope_rate = advance(f2[4:], around, 4, y, z, [rate_ref[0, x] for x in range(NX)])
    comps = new + slope
    for c in range(8):
        for x in range(NX):
            next_ref[c, x] = comps[c][x]
    weight = y.by_node(WEIGHTS) * z.by_node(WEIGHTS)

    def total(values):
        by_x = [float(WEIGHTS[x]) * values[x] for x in range(NX)]
        return jnp.sum(((by_x[0] + by_x[1]) + (by_x[2] + by_x[3])) * weight)

    stats = [
        jnp.max(fast_ref[...]),
        total([a * a for a in base_rate]),
        total([a * b for a, b in zip(base_rate, slope_rate)]),
        total([b * b for b in slope_rate]),
        total(base_rate),
        total(slope_rate),
        total(source),
    ]
    lane = lax.broadcasted_iota(jnp.int32, (1, NZ), 1)
    out = jnp.zeros((1, NZ), F32)
    for i, value in enumerate(stats):
        out = jnp.where(lane == i, value, out)
    stat_ref[...] = out


def finish_kernel(weight_total, u_ref, rate_ref, field_ref, stat_ref, grav_ref, source_ref, norm_ref):
    stat = stat_ref[...]
    part = [stat[:, i : i + 1] for i in range(7)]
    step = cfl_euler * elem_width / (7.0 * part[0])
    mean = part[6] * (1.0 / weight_total)
    shift = coupling * mean
    squares = (
        part[1]
        + step * (2.0 * part[2] + step * part[3])
        + shift * (2.0 * (part[4] + step * part[5]) + shift * weight_total)
    )
    norm_ref[...] = jnp.sqrt(jnp.maximum(squares, 0.0) * (1.0 / weight_total))
    raised = (ITERS * pseudo_step) * shift
    for x in range(NX):
        phi = field_ref[0, x] + step * field_ref[4, x] + raised
        grad = [field_ref[c, x] + step * field_ref[4 + c, x] for c in range(1, 4)]
        grav_ref[0, x] = phi
        for c in range(3):
            grav_ref[1 + c, x] = grad[c]
        rho = u_ref[0, x] + step * rate_ref[0, x]
        work = 0.0
        for c in range(3):
            source_ref[c, x] = -rho * grad[c]
            work = work + (u_ref[1 + c, x] + step * rate_ref[1 + c, x]) * grad[c]
        source_ref[3, x] = -work


def call(kernel, out_shape, flops, on_chip=True):
    def run(*args):
        if on_chip:
            args = [pltpu.with_memory_space_constraint(a, pltpu.VMEM) for a in args]
        return pl.pallas_call(
            kernel,
            in_specs=[pl.BlockSpec(memory_space=pltpu.VMEM)] * len(args),
            out_specs=[pl.BlockSpec(memory_space=pltpu.VMEM)] * len(out_shape),
            out_shape=out_shape,
            cost_estimate=pl.CostEstimate(flops=flops, bytes_accessed=400000, transcendentals=0),
        )(*args)

    return run


def pair_of(i, size):
    return i ^ 1


def other_of(i, size):
    return (i + 1 if i % 2 else i - 1) % size


ROUTES = {
    "state": (
        (GX, other_of),
        (GZ, other_of),
        ("gy", other_of),
        ("gy", pair_of),
        (GZ, pair_of),
        (GX, pair_of),
    ),
    "second": ((GX, other_of), ("gy", other_of), ("gy", pair_of), (GX, pair_of)),
    "corner": (("gy", other_of), ("gy", pair_of)),
    "third": ((GZ, other_of), (GZ, pair_of)),
}


def exchange(messages, stage):
    received = []
    for message, (axis, partner) in zip(messages, ROUTES[stage]):
        size = lax.axis_size(axis)
        received.append(lax.ppermute(message, axis, [(a, partner(a, size)) for a in range(size)]))
    return received


def gather(stat, axis):
    lane = lax.broadcasted_iota(jnp.int32, (1, NZ), 1)
    every = lax.all_gather(stat, axis, tiled=True)
    return jnp.where(
        lane == 0, jnp.max(every, axis=0, keepdims=True), jnp.sum(every, axis=0, keepdims=True)
    )


def spread(stat):
    names = ("gx_0", "gx_1", "gy", "gz_0", "gz_1")
    sizes = [lax.axis_size(name) for name in names]
    ring = sizes[0] * sizes[3]
    pairs = []
    for at in np.ndindex(*sizes):
        a, core, b, c, e = at
        place = (a * sizes[3] + c + core * sizes[4] + e - (sizes[3] // 2 - 1)) % ring
        to = (place // sizes[3], core, b, place % sizes[3], e)
        pairs.append(
            (int(np.ravel_multi_index(at, sizes)), int(np.ravel_multi_index(to, sizes)))
        )
    return lax.ppermute(stat, names, pairs)


def over_all(stat):
    for axis in ("gx_0", "gx_1", "gy", "gz_1"):
        stat = gather(stat, axis)
    stat = spread(stat)
    for axis in ("gx_1", "gz_1"):
        stat = gather(stat, axis)
    return stat


def shape(*dims):
    return pltpu.VMEM(dims, F32)


def local(u, g):
    weight_total = float(
        8.0
        * (u.shape[1] // 4 * lax.axis_size(GX))
        * (u.shape[2] // 4 * lax.axis_size("gy"))
        * (u.shape[3] // 4 * lax.axis_size(GZ))
    )
    full = (NX, NY, NZ)
    tile = shape(NY, NZ)
    planes, rows = (shape(9, NY, NZ), shape(9, NX, NZ))
    u, g, *messages = call(
        pack_kernel,
        [shape(5, *full), shape(4, *full), planes, tile, rows, rows, tile, planes],
        10**5,
        False,
    )(u, g)
    received = exchange(messages, "state")
    vol, alpha, fast = call(volume_kernel, [shape(5, *full), tile, tile], 10**7)(u)
    planes, rows = (shape(13, NY, NZ), shape(13, NX, NZ))
    rate, f1, f2, *messages = call(
        face_kernel,
        [shape(5, *full), shape(5, *full), shape(8, *full), planes, rows, rows, planes],
        10**6,
    )(u, g, vol, alpha, *received)
    xo, yo, yp, xp = exchange(messages, "second")
    corners = shape(10, NZ)
    f2, sides, *messages = call(
        side_kernel, [shape(8, *full), shape(2, 13, NY, NZ), corners, corners], 10**6
    )(f1, f2, xo, xp)
    corners = exchange(messages, "corner")
    f2, rows, *messages = call(
        join_kernel, [shape(8, *full), shape(13, *full), tile, tile], 10**6
    )(f1, f2, sides, yo, yp)
    received = exchange(messages, "third")
    field, stat = call(last_kernel, [shape(8, *full), shape(1, NZ)], 10**6)(
        u, rate, fast, f1, f2, sides, rows, *corners, *received
    )
    stat = over_all(stat)
    gravity, gravity_source, norm = call(
        functools.partial(finish_kernel, weight_total),
        [jax.ShapeDtypeStruct((4, *full), F32)] * 2 + [jax.ShapeDtypeStruct((1, 1), F32)],
        10**5,
    )(u, rate, field, stat)
    return (rate, gravity, gravity_source, norm.reshape(()))


def solution(mesh):
    torus = Mesh(
        mesh.devices.reshape(4, 2, mesh.shape["gy"], 8, 4), ("gx_0", "gx_1", "gy", "gz_0", "gz_1")
    )
    placed = (P(None, GX, "gy", GZ), P(None, GX, "gy", GZ))
    return jax.shard_map(
        local,
        mesh=torus,
        in_specs=placed,
        out_specs=(P(None, GX, "gy", GZ), P(None, GX, "gy", GZ), P(None, GX, "gy", GZ), P()),
        check_vma=False,
    )
```
